32 devices in a mesh: gx: 2 (over y), gz: 4 (over x, core), ga: 4 (over z).
Axes of the slice: x: 2, y: 2, z: 4, core: 2. Of those that a mesh axis runs over, the one named last changes fastest.
Arguments:
- right_side: float32 [32, 128, 512], P('gx', 'ga', 'gz'), may hold values from -60 to 60, as said below
- diagonal: float32 [32, 128, 512], P('gx', 'ga', 'gz'), may hold values from 0.02 to 1
- element_features: bfloat16 [256, 4096], P(None, ('gx', 'gz', 'ga')), may hold values from -6 to 6
- sample_bank: bfloat16 [256, 131072], P(None, ('gx', 'gz', 'ga')), may hold values from -6 to 6
- target_bank: bfloat16 [6, 131072], P(None, ('gx', 'gz', 'ga')), may hold values from -6 to 6
- patch_index: int32 [65536], P(('gx', 'gz', 'ga')), may hold values from 0 to 4095
- w_first: bfloat16 [256, 256], replicated, may hold values from -0.375 to 0.375
- w_second: bfloat16 [256, 256], replicated, may hold values from -0.375 to 0.375
- w_third: bfloat16 [6, 256], replicated, may hold values from -0.375 to 0.375
Outputs:
- pressure: float32 [32, 128, 512], P('gx', 'ga', 'gz')
- residual: float32 [32, 128, 512], P('gx', 'ga', 'gz')
- step_first: float32 [256, 256], replicated
- step_second: float32 [256, 256], replicated
- step_third: float32 [6, 256], replicated
The draws below stay inside these ranges and needn't reach their ends.
Inputs may be any that keep to these rules, and one draw needn't show every extreme that they name: `right_side`: grows in magnitude along the first dimension. `patch_index`: each entry names a column of the sample_bank and target_bank block that lies on the same device as the entry.
All inputs are finite; a program needn't handle non-finite values.
Results may differ from the reference program's by a relative error of at most 0.0004.
The reference program's roundings to bfloat16 on the way count: a program that leaves them out, or rounds other values in their place, can miss the bound.
Values sent between devices are 32-bit elements; how exact they have to be, the bound alone decides.
A program may use at most 64 MiB of HBM per device.

```python
import math
import jax
import jax.numpy as jnp
from jax import lax

CX = 16
CY = 32
CZ = 128
EL = 8
CH = 256
STRESS = 6
ITERS = 12
SAMPLES_DEV = 2048
BANK_DEV = 4096
NX = 32
NY = 128
NZ = 512
ELEMS = 4096
BANK = 131072
SAMPLES = 65536
N_GX = 2
N_GZ = 4
N_GA = 4


def draw_right_side(key, part):
    position = jnp.arange(NX, dtype=jnp.float32) / NX
    growth = jnp.power(10.0, position)[:, None, None]
    random_part = jax.random.truncated_normal(key, -6.0, 6.0, (NX, NY, NZ), jnp.float32)
    return random_part * growth


def with_ends(result, key, low, high):
    longest = result.shape.index(max(result.shape))
    spots = []
    for shift in (0, 1):
        where = [jax.random.randint(jax.random.fold_in(key, axis), (), 0, length) for axis, length in enumerate(result.shape)]
        where[longest] = (where[longest] + shift) % result.shape[longest]
        spots.append(tuple(where))
    return result.at[spots[0]].set(low).at[spots[1]].set(high)


def level_of(own_key, dims, split, smallest, top_value):
    def one(axis_at, blocks):
        heights = jax.random.uniform(jax.random.fold_in(jax.random.fold_in(own_key, 6), axis_at), (blocks,), jnp.float32, smallest / len(split), top_value / len(split))
        return jnp.repeat(jnp.exp(heights), dims[axis_at] // blocks).reshape((-1,) + (1,) * (len(dims) - axis_at - 1))

    factor_of = one(*split[0])
    for cut in split[1:]:
        factor_of = factor_of * one(*cut)
    return factor_of


def scatter_about(rng, dims, scale, reach, cuts=(), kind=jnp.bfloat16):
    gain = level_of(rng, dims, cuts, -0.22, 0.18) if cuts else 1.0
    entries = jax.random.normal(rng, dims, jnp.float32) * scale * gain
    return jnp.minimum(jnp.maximum(entries, -reach), reach).astype(kind)


def setup_inputs(seed: int = 0) -> dict:
    arg_keys = jax.random.split(jax.random.key(seed), 10)
    return {
        "right_side": draw_right_side(jax.random.fold_in(arg_keys[9], 71), 0),
        "diagonal": jnp.clip(jnp.exp(math.log(1.0) - 3.912023 * jax.random.uniform(arg_keys[1], (NX, NY, NZ), jnp.float32) ** level_of(arg_keys[1], (NX, NY, NZ), ((0, 2), (1, 4), (2, 4)), -0.2, 0.2)), 0.02, 1.0),
        "element_features": scatter_about(arg_keys[2], (CH, ELEMS), 1.0, 6.0, ((1, 32),)),
        "sample_bank": scatter_about(arg_keys[3], (CH, BANK), 1.0, 6.0, ((1, 32),)),
        "target_bank": scatter_about(arg_keys[4], (STRESS, BANK), 1.0, 6.0, ((1, 32),)),
        "patch_index": with_ends(jax.random.randint(arg_keys[5], (SAMPLES,), 0, BANK_DEV), jax.random.fold_in(arg_keys[5], 1), 0, BANK_DEV - 1).astype(jnp.int32),
        "w_first": scatter_about(arg_keys[6], (CH, CH), CH ** -0.5, 0.375),
        "w_second": scatter_about(arg_keys[7], (CH, CH), CH ** -0.5, 0.375),
        "w_third": scatter_about(arg_keys[8], (STRESS, CH), CH ** -0.5, 0.375),
    }


taps = (1.6, -0.2, 8.0 / 315.0, -1.0 / 560.0)
center = 3.0 * 205.0 / 72.0
epsilon = 1e-06

def neighbours(padded):
    length_x = padded.shape[0] - 8
    length_y = padded.shape[1] - 8
    length_z = padded.shape[2] - 8
    summed = jnp.zeros((length_x, length_y, length_z), padded.dtype)
    for offset in range(1, 5):
        weight = taps[offset - 1]
        along_x = padded[4 + offset:4 + offset + length_x, 4:4 + length_y, 4:4 + length_z] + padded[4 - offset:4 - offset + length_x, 4:4 + length_y, 4:4 + length_z]
        along_y = padded[4:4 + length_x, 4 + offset:4 + offset + length_y, 4:4 + length_z] + padded[4:4 + length_x, 4 - offset:4 - offset + length_y, 4:4 + length_z]
        along_z = padded[4:4 + length_x, 4:4 + length_y, 4 + offset:4 + offset + length_z] + padded[4:4 + length_x, 4:4 + length_y, 4 - offset:4 - offset + length_z]
        summed = summed + weight * (along_x + along_y + along_z)
    return summed

def operate(padded, precond):
    return precond * padded[4:-4, 4:-4, 4:-4] - neighbours(padded)

def closure(w_first, w_second, w_third, inputs):
    linear_first = jnp.dot(w_first, inputs, preferred_element_type=jnp.float32)
    hidden_first = jax.nn.silu(linear_first).astype(jnp.bfloat16)
    linear_second = jnp.dot(w_second, hidden_first, preferred_element_type=jnp.float32)
    hidden_second = jax.nn.silu(linear_second).astype(jnp.bfloat16)
    predicted = jnp.dot(w_third, hidden_second, preferred_element_type=jnp.float32)
    return (linear_first, hidden_first, linear_second, hidden_second, predicted)

def slope(linear):
    sigmoid = jax.nn.sigmoid(linear)
    return sigmoid * (1.0 + linear * (1.0 - sigmoid))

def gradients(w_first, w_second, w_third, inputs, targets):
    linear_first, hidden_first, linear_second, hidden_second, predicted = closure(w_first, w_second, w_third, inputs)
    error = (predicted - targets.astype(jnp.float32)).astype(jnp.bfloat16)
    contract = (((1,), (1,)), ((), ()))
    leading = (((0,), (0,)), ((), ()))
    grad_third = lax.dot_general(error, hidden_second, contract, preferred_element_type=jnp.float32)
    back_second = lax.dot_general(w_third, error, leading, preferred_element_type=jnp.float32)
    delta_second = (back_second * slope(linear_second)).astype(jnp.bfloat16)
    grad_second = lax.dot_general(delta_second, hidden_first, contract, preferred_element_type=jnp.float32)
    back_first = lax.dot_general(w_second, delta_second, leading, preferred_element_type=jnp.float32)
    delta_first = (back_first * slope(linear_first)).astype(jnp.bfloat16)
    grad_first = lax.dot_general(delta_first, inputs, contract, preferred_element_type=jnp.float32)
    return (grad_first, grad_second, grad_third)

def normalize(gradient):
    return gradient * lax.rsqrt(jnp.mean(gradient * gradient) + epsilon)

def reference(right_side, diagonal, element_features, sample_bank, target_bank, patch_index, w_first, w_second, w_third):
    predicted = closure(w_first, w_second, w_third, element_features)[4]
    trace = (predicted[0] + predicted[1] + predicted[2]) / 3.0
    elems_x = CX // EL
    elems_y = CY // EL
    elems_z = CZ // EL
    blocks = trace.reshape(N_GX, N_GZ, N_GA, elems_x, elems_y, elems_z)
    blocks = blocks.transpose(0, 3, 2, 4, 1, 5).reshape(N_GX * elems_x, N_GA * elems_y, N_GZ * elems_z)
    forcing = jnp.repeat(jnp.repeat(jnp.repeat(blocks, EL, 0), EL, 1), EL, 2)
    source = right_side + forcing
    precond = diagonal + center
    pressure = jnp.zeros_like(source)
    residual = source
    scaled = residual / precond
    direction = scaled
    product_now = jnp.sum(residual * scaled)
    for iteration in range(ITERS):
        image_dir = operate(jnp.pad(direction, 4), precond)
        step_len = product_now / jnp.sum(direction * image_dir)
        pressure = pressure + step_len * direction
        residual = residual - step_len * image_dir
        scaled = residual / precond
        product_next = jnp.sum(residual * scaled)
        direction = scaled + product_next / product_now * direction
        product_now = product_next

    def accumulate(device, running):
        sample_start = (device * SAMPLES_DEV).astype(jnp.int32)
        bank_start = (device * BANK_DEV).astype(jnp.int32)
        columns = lax.dynamic_slice_in_dim(patch_index, sample_start, SAMPLES_DEV)
        bank_shard = lax.dynamic_slice_in_dim(sample_bank, bank_start, BANK_DEV, 1)
        goal_shard = lax.dynamic_slice_in_dim(target_bank, bank_start, BANK_DEV, 1)
        inputs = jnp.take(bank_shard, columns, axis=1)
        targets = jnp.take(goal_shard, columns, axis=1)
        partial_value = gradients(w_first, w_second, w_third, inputs, targets)
        return tuple((before + after for before, after in zip(running, partial_value)))
    initial = (jnp.zeros((CH, CH), jnp.float32), jnp.zeros((CH, CH), jnp.float32), jnp.zeros((STRESS, CH), jnp.float32))
    grad_first, grad_second, grad_third = lax.fori_loop(0, N_GX * N_GZ * N_GA, accumulate, initial)
    return (pressure, residual, normalize(grad_first), normalize(grad_second), normalize(grad_third))
```

```python
import functools

import jax
import jax.numpy as jnp
from jax import lax
from jax.experimental import pallas as pl
from jax.experimental.pallas import tpu as pltpu
from jax.sharding import PartitionSpec as P

EL = 8
ITERS = 12
TILE = 512
AXES = ("gx", "gz", "ga")
ONE_PHASE = 64

taps = (1.6, -0.2, 8.0 / 315.0, -1.0 / 560.0)
center = 3.0 * 205.0 / 72.0
epsilon = 1e-06
half = 1.1
MESH = pl.DeviceIdType.MESH
F32 = jnp.float32
BF16 = jnp.bfloat16


def dot(a, b, dims=((1,), (0,)), precision=None):
    return lax.dot_general(a, b, (dims, ((), ())), preferred_element_type=F32, precision=precision)


def sigmoid(v):
    return 1.0 / (1.0 + jnp.exp(-v))


def phases_of(sizes):
    total = 1
    for a in AXES:
        total *= sizes[a]
    return (AXES,) if total <= ONE_PHASE else (("gx",), ("gz", "ga"))


def shift_offsets(sizes):
    combos = [()]
    for n in sizes:
        combos = [c + (k,) for c in combos for k in range(n)]
    return combos[1:]


def krylov_coefficients(mu):
    n = len(mu) // 2
    one = jnp.ones_like(mu[0])
    rho, pi = dict(enumerate(mu)), dict(enumerate(mu))
    r, p, x = [one], [one], []
    for k in range(n):
        last = 2 * n - 2 - k
        tau = {}
        for l in range(k, last + 1):
            tau[l] = pi[l] + 0.5 * (pi[l + 1] + pi[abs(l - 1)])
        alpha = rho[k] / tau[k]
        x = [a + alpha * b for a, b in zip(x, p)] + [alpha * b for b in p[len(x):]]
        moved = list(p) + [jnp.zeros_like(one)]
        for j, b in enumerate(p):
            if j == 0:
                moved[1] = moved[1] + b
            else:
                moved[j - 1] = moved[j - 1] + 0.5 * b
                moved[j + 1] = moved[j + 1] + 0.5 * b
        r = [a - alpha * b for a, b in zip(r + [jnp.zeros_like(one)], moved)]
        if k + 1 < n:
            new = {l: rho[l] - alpha * tau[l] for l in range(k + 1, last + 1)}
            beta = (-alpha if k == 0 else -0.5 * alpha) * new[k + 1] / rho[k]
            p = [a + beta * b for a, b in zip(r, p)] + r[len(p):]
            pi = {l: (new[l] if l > k else 0.0) + beta * pi[l] for l in range(k, last + 1)}
            rho = new
    return [v * (1.0 / half) for v in x], r


def solve_kernel(
    sizes, right, diag, feats, bank, target, index, w1, w2, w3, press, resid, total_grads,
    mp, nb, basis, pre, inv, yp, yr, zp, zr, eta, ar_src, ar_dst,
    bank_v, counts, grads, first, held, second, owned, third, full,
    bank_sem, g_send, g_recv, h_send, h_recv, a_send, a_recv,
):
    lx, ly, lz = right.shape
    ch, columns = bank.shape
    stress = target.shape[0]
    tiles = columns // TILE
    pos = {a: lax.axis_index(a) for a in AXES}
    phases = phases_of(sizes)

    def tile_copy(t):
        return pltpu.make_async_copy(
            bank.at[:, pl.ds(t * TILE, TILE)], bank_v.at[t], bank_sem.at[t]
        )

    for t in range(tiles):
        tile_copy(t).start()

    def coords(axes, offs, sign):
        out = {}
        for a, k in zip(axes, offs):
            n = sizes[a]
            c = pos[a] + (k if sign > 0 else n - k) if k else pos[a]
            out[a] = lax.rem(c, n) if k else c
        return out

    def flat(axes, at):
        value = 0
        for a in axes:
            value = value * sizes[a] + at[a]
        return value

    groups = []
    for axes in phases:
        me = flat(axes, pos)
        peers = []
        for offs in shift_offsets([sizes[a] for a in axes]):
            to = {**pos, **coords(axes, offs, 1)}
            source = flat(axes, coords(axes, offs, -1))
            peers.append((to, source))
        groups.append((me, peers))

    nx, nz, na = sizes["gx"], sizes["gz"], sizes["ga"]
    share = grads.shape[0] // nz
    piece = share // na

    def block_of(iz, ia=None):
        if ia is None:
            return pl.ds(pl.multiple_of(iz * share, 8), share)
        return pl.ds(pl.multiple_of((iz * na + ia) * piece, 8), piece)

    def along(axis, k, sign):
        return coords((axis,), (k,), sign)[axis]

    def gather_copy(number, axis, k, src, dst):
        return pltpu.make_async_remote_copy(
            src_ref=src,
            dst_ref=dst,
            send_sem=g_send.at[number],
            recv_sem=g_recv.at[number],
            device_id={**pos, axis: along(axis, k, 1)},
            device_id_type=MESH,
        )

    def scatter_gz(k):
        return gather_copy(k - 1, "gz", k, grads.at[block_of(along("gz", k, 1))], first.at[k - 1])

    def scatter_ga(k):
        rows = pl.ds(pl.multiple_of(along("ga", k, 1) * piece, 8), piece)
        return gather_copy(nz - 1 + k - 1, "ga", k, held.at[rows], second.at[k - 1])

    def add_gx(k, sign=1):
        slot = pos["gx"] if sign > 0 else along("gx", k, -1)
        return gather_copy(nz + na - 2 + k - 1, "gx", k, owned, third.at[slot])

    def gather_ga(k, sign=1):
        at = pos["ga"] if sign > 0 else along("ga", k, -1)
        rows = block_of(pos["gz"], at)
        return gather_copy(nz + na + nx - 3 + k - 1, "ga", k, full.at[rows], full.at[rows])

    def gather_gz(k, sign=1):
        at = pos["gz"] if sign > 0 else along("gz", k, -1)
        rows = block_of(at)
        return gather_copy(nz + 2 * na + nx - 4 + k - 1, "gz", k, full.at[rows], full.at[rows])

    def gradient_stage(stage):
        if stage == 0:
            for k in range(1, nz):
                scatter_gz(k).start()
        elif stage == 1:
            total = grads[block_of(pos["gz"]), :]
            for k in range(1, nz):
                scatter_gz(k).wait_recv()
                total = total + first[k - 1]
            held[...] = total
            for k in range(1, na):
                scatter_ga(k).start()
        elif stage == 2:
            total = held[pl.ds(pl.multiple_of(pos["ga"] * piece, 8), piece), :]
            for k in range(1, na):
                scatter_ga(k).wait_recv()
                total = total + second[k - 1]
            owned[...] = total
            third[pos["gx"]] = total
            for k in range(1, nx):
                add_gx(k).start()
        elif stage == 3:
            for k in range(1, nx):
                add_gx(k, -1).wait_recv()
            full[block_of(pos["gz"], pos["ga"]), :] = jnp.sum(third[...], axis=0)
            for k in range(1, na):
                gather_ga(k).start()
        elif stage == 4:
            for k in range(1, na):
                gather_ga(k, -1).wait_recv()
            for k in range(1, nz):
                gather_gz(k).start()
        else:
            for k in range(1, nz):
                gather_gz(k, -1).wait_recv()
                scatter_gz(k).wait_send()
                gather_gz(k).wait_send()
            for k in range(1, na):
                scatter_ga(k).wait_send()
                gather_ga(k).wait_send()
            for k in range(1, nx):
                add_gx(k).wait_send()

    def count_samples():
        samples = index.shape[1]
        ids = index[...]
        high = lax.broadcasted_iota(jnp.int32, (columns // 128, samples), 0) == (ids // 128)
        low = lax.broadcasted_iota(jnp.int32, (128, samples), 0) == (ids % 128)
        counts[...] = dot(
            jnp.where(high, 1.0, 0.0).astype(BF16),
            jnp.where(low, 1.0, 0.0).astype(BF16),
            ((1,), (1,)),
        )

    def gradient_tile(t):
        rows = TILE // 128
        tile_copy(t).wait()
        weight = jnp.concatenate([counts[pl.ds(t * rows + j, 1), :] for j in range(rows)], axis=1)
        x = bank_v[t]
        a1, a2, a3 = w1[...], w2[...], w3[...]
        l1 = dot(a1, x)
        s1 = sigmoid(l1)
        h1 = (l1 * s1).astype(BF16)
        l2 = dot(a2, h1)
        s2 = sigmoid(l2)
        h2 = (l2 * s2).astype(BF16)
        goal = target[:, pl.ds(pl.multiple_of(t * TILE, TILE), TILE)]
        error = (dot(a3, h2) - goal.astype(F32)).astype(BF16)

        def weighted(delta, right):
            scaled = delta.astype(F32) * weight
            upper = scaled.astype(BF16)
            lower = (scaled - upper.astype(F32)).astype(BF16)
            return dot(upper, right, ((1,), (1,))) + dot(lower, right, ((1,), (1,)))

        grads[2 * ch : 2 * ch + stress] += weighted(error, h2)
        d2 = (dot(a3, error, ((0,), (0,))) * (s2 * (1.0 + l2 * (1.0 - s2)))).astype(BF16)
        grads[ch : 2 * ch] += weighted(d2, h1)
        d1 = (dot(a2, d2, ((0,), (0,))) * (s1 * (1.0 + l1 * (1.0 - s1)))).astype(BF16)
        grads[:ch] += weighted(d1, x)

    def gradient_work(i):
        pl.when(i < tiles)(lambda: gradient_tile(i))
        for stage in range(ITERS - tiles):
            pl.when(i == tiles + stage)(lambda stage=stage: gradient_stage(stage))

    mp[...] = jnp.zeros_like(mp)
    yr[...] = jnp.zeros_like(yr)
    zr[...] = jnp.zeros_like(zr)

    barrier = pltpu.get_barrier_semaphore()
    total = 0
    for _, peers in groups:
        for to, _ in peers:
            pl.semaphore_signal(barrier, inc=1, device_id=to, device_id_type=MESH)
            total += 1

    lane = lax.broadcasted_iota(jnp.int32, (ly, lz), 1)
    sub8 = lax.broadcasted_iota(jnp.int32, (8, lz), 0)

    def halo_copies(par):
        out = {}

        def add(axis, step, number, src, dst):
            copy = pltpu.make_async_remote_copy(
                src_ref=src,
                dst_ref=dst,
                send_sem=h_send.at[par, number],
                recv_sem=h_recv.at[par, number],
                device_id={**pos, axis: jnp.clip(pos[axis] + step, 0, sizes[axis] - 1)},
                device_id_type=MESH,
            )
            can_send = pos[axis] < sizes[axis] - 1 if step > 0 else pos[axis] > 0
            will_get = pos[axis] > 0 if step > 0 else pos[axis] < sizes[axis] - 1
            out.setdefault(axis, []).append((copy, can_send, will_get))

        rows = pl.ds(8, ly)
        if sizes["gx"] > 1:
            add("gx", 1, 0, mp.at[par, pl.ds(lx, 4), rows], mp.at[par, pl.ds(0, 4), rows])
            add("gx", -1, 1, mp.at[par, pl.ds(4, 4), rows], mp.at[par, pl.ds(lx + 4, 4), rows])
        if sizes["ga"] > 1:
            add("ga", 1, 2, yp.at[par, 0], yr.at[par, 0])
            add("ga", -1, 3, yp.at[par, 1], yr.at[par, 1])
        if sizes["gz"] > 1:
            add("gz", 1, 4, zp.at[par], zr.at[par, 0])
            add("gz", -1, 5, zp.at[par], zr.at[par, 1])
        return out

    def halo_start(par, *axes):
        copies = halo_copies(par)
        for axis in axes:
            for copy, can_send, _ in copies.get(axis, []):
                pl.when(can_send)(copy.start)

    def halo_wait(par):
        for copies in halo_copies(par).values():
            for copy, _, will_get in copies:
                pl.when(will_get)(copy.wait_recv)

    def halo_sent(par):
        for copies in halo_copies(par).values():
            for copy, can_send, _ in copies:
                pl.when(can_send)(copy.wait_send)

    bases = []
    base = 0
    for axes in phases:
        bases.append(base)
        n = 1
        for a in axes:
            n *= sizes[a]
        base += n

    def sum_copies(phase):
        me, peers = groups[phase]
        out = []
        for k, (to, source) in enumerate(peers):
            slot = bases[phase]
            send = pltpu.make_async_remote_copy(
                src_ref=ar_src.at[phase],
                dst_ref=ar_dst.at[slot + me],
                send_sem=a_send.at[slot + k],
                recv_sem=a_recv.at[slot + me],
                device_id=to,
                device_id_type=MESH,
            )
            receive = pltpu.make_async_remote_copy(
                src_ref=ar_src.at[phase],
                dst_ref=ar_dst.at[slot + source],
                send_sem=a_send.at[slot + k],
                recv_sem=a_recv.at[slot + source],
                device_id=to,
                device_id_type=MESH,
            )
            out.append((send, receive))
        return out

    def sum_start(phase, row):
        ar_src[phase] = row
        ar_dst[bases[phase] + groups[phase][0]] = row
        for send, _ in sum_copies(phase):
            send.start()

    def sum_wait(phase):
        count = len(groups[phase][1]) + 1
        for _, receive in sum_copies(phase):
            receive.wait_recv()
        return jnp.sum(ar_dst[pl.ds(bases[phase], count)], axis=0)

    def sums_sent():
        for phase in range(len(phases)):
            for send, _ in sum_copies(phase):
                send.wait_send()

    def stencil_local(par):
        for x in range(lx):
            v = mp[par, 4 + x, pl.ds(8, ly)]
            acc = None
            for k in range(1, 5):
                t = mp[par, 4 + x, pl.ds(8 + k, ly)] + mp[par, 4 + x, pl.ds(8 - k, ly)]
                if x + k < lx:
                    t = t + mp[par, 4 + x + k, pl.ds(8, ly)]
                if x - k >= 0:
                    t = t + mp[par, 4 + x - k, pl.ds(8, ly)]
                t = t + jnp.where(lane >= k, pltpu.roll(v, k, 1), 0.0)
                t = t + jnp.where(lane < lz - k, pltpu.roll(v, lz - k, 1), 0.0)
                t = taps[k - 1] * t
                acc = t if acc is None else acc + t
            nb[x] = acc

    def z_correction(par):
        h = jnp.where(lane % 8 < 4, zr[par, 0], zr[par, 1])
        acc = jnp.zeros((ly, lz), F32)
        place = lane % 8
        for k in range(1, 5):
            ahead = jnp.where((place >= 4) & (place - 4 < k), pltpu.roll(h, k, 1), 0.0)
            behind = jnp.where((place < 4) & (place >= 4 - k), pltpu.roll(h, lz - k, 1), 0.0)
            acc = acc + taps[k - 1] * (ahead + behind)
        return acc

    def corrected(par, x, zc):
        acc = nb[x]
        for k in range(1, 5):
            if x - k < 0:
                acc = acc + taps[k - 1] * mp[par, 4 + x - k, pl.ds(8, ly)]
            if x + k >= lx:
                acc = acc + taps[k - 1] * mp[par, 4 + x + k, pl.ds(8, ly)]
        z = pltpu.roll(zc, (2 * lz - 8 * x - 4) % lz, 1)
        acc = acc + jnp.where((lane < 4) | (lane >= lz - 4), z, 0.0)
        if x % 2 == 0:
            h = jnp.where(sub8 < 4, yr[par, 1, x // 2], yr[par, 0, x // 2])
        else:
            h = pltpu.roll(jnp.where(sub8 < 4, yr[par, 0, x // 2], yr[par, 1, x // 2]), 4, 0)
        low = jnp.zeros((8, lz), F32)
        high = jnp.zeros((8, lz), F32)
        for k in range(1, 5):
            low = low + taps[k - 1] * jnp.where(sub8 < k, pltpu.roll(h, k, 0), 0.0)
            high = high + taps[k - 1] * jnp.where(sub8 >= 8 - k, pltpu.roll(h, 8 - k, 0), 0.0)
        parts = [acc[:8] + low] + ([acc[8:-8]] if ly > 16 else []) + [acc[-8:] + high]
        return jnp.concatenate(parts, axis=0)

    def publish(par, x, m, packed, edges):
        mp[par, 4 + x, pl.ds(8, ly)] = m
        if x % 2 == 0:
            edges = (m[:8], m[-8:])
        else:
            yp[par, 0, x // 2] = jnp.where(sub8 < 4, pltpu.roll(m[-8:], 4, 0), edges[1])
            yp[par, 1, x // 2] = jnp.where(sub8 < 4, edges[0], pltpu.roll(m[:8], 4, 0))
        turned = pltpu.roll(m, (8 * x + 4) % lz, 1)
        return jnp.where((lane >= 8 * x) & (lane < 8 * x + 8), turned, packed), edges

    order = list(range(4)) + list(range(lx - 4, lx)) + list(range(4, lx - 4))

    hidden = dot(w1[...], feats[...])
    hidden = (hidden * sigmoid(hidden)).astype(BF16)
    hidden = dot(w2[...], hidden)
    hidden = (hidden * sigmoid(hidden)).astype(BF16)
    predicted = dot(w3[...], hidden)
    trace = (predicted[0:1] + predicted[1:2] + predicted[2:3]) / 3.0
    ex, ey, ez = lx // EL, ly // EL, lz // EL
    spread = jnp.where(
        lax.broadcasted_iota(jnp.int32, (lz, lz), 0) == lax.broadcasted_iota(jnp.int32, (lz, lz), 1) // EL,
        1.0,
        0.0,
    )
    lines = jnp.concatenate(
        [trace if e == 0 else pltpu.roll(trace, (lz - e * ez) % lz, 1) for e in range(ex * ey)], axis=0
    )
    forcing = dot(lines, spread, precision=lax.Precision.HIGHEST)
    pl.semaphore_wait(barrier, total)
    packed = jnp.zeros((ly, lz), F32)
    edges = None
    for n, x in enumerate(order):
        line = forcing[(x // EL) * ey : (x // EL) * ey + ey]
        block = jnp.concatenate([jnp.broadcast_to(line[j : j + 1], (EL, lz)) for j in range(ey)], axis=0)
        whole = diag[x] + center
        scale = 1.0 / whole
        pre[x] = whole
        inv[x] = scale * (2.0 / half)
        first_vector = (right[x] + block) * scale
        basis[0, x] = first_vector
        packed, edges = publish(0, x, first_vector, packed, edges)
        if n == 7:
            halo_start(0, "gx")
    zp[0] = packed
    halo_start(0, "ga", "gz")
    grads[...] = jnp.zeros_like(grads)
    count_samples()

    def iteration(i, carry):
        par = lax.rem(i, 2)
        later = 1 - par
        stencil_local(par)
        gradient_work(i)
        halo_wait(par)
        zc = z_correction(par)
        start = jnp.where(i == 0, 0.5, 1.0)
        back = jnp.where(i == 0, 0.0, 1.0)
        keep = start * (2.0 / half - 2.0)
        more = i < ITERS - 1
        packed = jnp.zeros((ly, lz), F32)
        even = jnp.zeros((ly, lz), F32)
        odd = jnp.zeros((ly, lz), F32)
        edges = None
        older = jnp.maximum(i - 1, 0)
        for n, x in enumerate(order):
            v = mp[par, 4 + x, pl.ds(8, ly)]
            m = keep * v - start * (inv[x] * corrected(par, x, zc)) - back * basis[older, x]
            basis[i + 1, x] = m
            weighed = pre[x] * v
            even = even + weighed * v
            odd = odd + weighed * m
            packed, edges = publish(later, x, m, packed, edges)
            if n == 7:
                pl.when(more)(lambda: halo_start(later, "gx"))
        zp[later] = packed
        pl.when(more)(lambda: halo_start(later, "ga", "gz"))
        eta[2 * i] = jnp.sum(even.reshape(ly // 8, 8, lz), axis=0)
        eta[2 * i + 1] = jnp.sum(odd.reshape(ly // 8, 8, lz), axis=0)
        halo_sent(par)
        return carry

    lax.fori_loop(0, ITERS, iteration, 0)

    count = 2 * ITERS
    sums = jnp.sum(jnp.sum(eta[...], axis=1), axis=1, keepdims=True)
    mine = lax.broadcasted_iota(jnp.int32, (count, lz), 0) == lax.broadcasted_iota(jnp.int32, (count, lz), 1)
    row = jnp.sum(jnp.where(mine, sums, 0.0), axis=0, keepdims=True)
    sum_start(0, row)
    for stage in range(ITERS - tiles, 5):
        gradient_stage(stage)
    for phase in range(1, len(phases)):
        sum_start(phase, sum_wait(phase - 1))
    row = sum_wait(len(phases) - 1)
    spread_row = jnp.sum(jnp.where(mine, row, 0.0), axis=1, keepdims=True)
    moment = [jnp.broadcast_to(spread_row[j : j + 1], (1, lz)) for j in range(count)]
    mu = moment[:2] + [2.0 * moment[j] - moment[j % 2] for j in range(2, count)]
    along_x, along_r = krylov_coefficients(mu)
    for x in range(lx):
        p = along_x[0] * basis[0, x]
        r = along_r[0] * basis[0, x]
        for j in range(1, ITERS):
            v = basis[j, x]
            p = p + along_x[j] * v
            r = r + along_r[j] * v
        press[x] = p
        resid[x] = pre[x] * (r + along_r[ITERS] * basis[ITERS, x])
    gradient_stage(5)
    total_grads[...] = full[...]
    sums_sent()


def pressure_solve(right_side, diagonal, feats, bank, target, index, w1, w2, w3):
    sizes = {a: lax.axis_size(a) for a in AXES}
    lx, ly, lz = right_side.shape
    ch, columns = bank.shape
    slots = 0
    phases = phases_of(sizes)
    for axes in phases:
        n = 1
        for a in axes:
            n *= sizes[a]
        slots += n
    nx, nz, na = (sizes[a] for a in ("gx", "gz", "ga"))
    unit = 8 * nz * na
    rows = w1.shape[0] + w2.shape[0] + w3.shape[0]
    rows = (rows + unit - 1) // unit * unit
    share = rows // nz
    piece = share // na
    tiles = columns // TILE
    copies = max(2 * (nz - 1) + 2 * (na - 1) + nx - 1, 1)
    field = pltpu.VMEM((lx, ly, lz), F32)
    vmem = pl.BlockSpec(memory_space=pltpu.VMEM)
    return pl.pallas_call(
        functools.partial(solve_kernel, sizes),
        out_shape=[jax.ShapeDtypeStruct((lx, ly, lz), F32)] * 2 + [jax.ShapeDtypeStruct((rows, ch), F32)],
        in_specs=[vmem] * 3 + [pl.BlockSpec(memory_space=pl.ANY)] + [vmem] * 5,
        out_specs=[vmem] * 3,
        scratch_shapes=[
            pltpu.VMEM((2, lx + 8, ly + 16, lz), F32),
            field,
            pltpu.VMEM((ITERS + 1, lx, ly, lz), F32),
            field, field,
            pltpu.VMEM((2, 2, lx // 2, 8, lz), F32),
            pltpu.VMEM((2, 2, lx // 2, 8, lz), F32),
            pltpu.VMEM((2, ly, lz), F32),
            pltpu.VMEM((2, 2, ly, lz), F32),
            pltpu.VMEM((2 * ITERS, 8, lz), F32),
            pltpu.VMEM((len(phases), 1, lz), F32),
            pltpu.VMEM((slots, 1, lz), F32),
            pltpu.VMEM((tiles, ch, TILE), BF16),
            pltpu.VMEM((columns // 128, 128), F32),
            pltpu.VMEM((rows, ch), F32),
            pltpu.VMEM((max(nz - 1, 1), share, ch), F32),
            pltpu.VMEM((share, ch), F32),
            pltpu.VMEM((max(na - 1, 1), piece, ch), F32),
            pltpu.VMEM((piece, ch), F32),
            pltpu.VMEM((nx, piece, ch), F32),
            pltpu.VMEM((rows, ch), F32),
            pltpu.SemaphoreType.DMA((tiles,)),
            pltpu.SemaphoreType.DMA((copies,)),
            pltpu.SemaphoreType.DMA((copies,)),
            pltpu.SemaphoreType.DMA((2, 6)),
            pltpu.SemaphoreType.DMA((2, 6)),
            pltpu.SemaphoreType.DMA((slots,)),
            pltpu.SemaphoreType.DMA((slots,)),
        ],
        compiler_params=pltpu.CompilerParams(collective_id=0, has_side_effects=True),
        cost_estimate=pl.CostEstimate(
            flops=60_000_000, bytes_accessed=200_000_000, transcendentals=0
        ),
    )(right_side, diagonal, feats, bank, target, index.reshape(1, -1), w1, w2, w3)


def finish_kernel(press_in, resid_in, grads, press, resid, step1, step2, step3):
    press[...] = press_in[...]
    resid[...] = resid_in[...]
    ch = step1.shape[0]
    start = 0
    for out in (step1, step2, step3):
        count = out.shape[0]
        value = grads[start : start + count]
        squares = jnp.sum(jnp.sum(value * value, axis=0, keepdims=True), axis=1, keepdims=True)
        out[...] = value * lax.rsqrt(squares / (count * ch) + epsilon)
        start += count


def finish(press, resid, grads, weights):
    vmem = pl.BlockSpec(memory_space=pltpu.VMEM)
    return pl.pallas_call(
        finish_kernel,
        out_shape=[jax.ShapeDtypeStruct(press.shape, F32)] * 2
        + [jax.ShapeDtypeStruct(w.shape, F32) for w in weights],
        in_specs=[vmem] * 3,
        out_specs=[vmem] * 5,
        cost_estimate=pl.CostEstimate(flops=1_000_000, bytes_accessed=2_000_000, transcendentals=0),
    )(press, resid, grads)


def body(
    right_side, diagonal, element_features, sample_bank, target_bank, patch_index, w_first, w_second, w_third
):
    weights = (w_first, w_second, w_third)
    solved = pressure_solve(
        right_side, diagonal, element_features, sample_bank, target_bank, patch_index, *weights
    )
    return tuple(finish(*solved, weights))


def solution(mesh):
    return jax.shard_map(
        body,
        mesh=mesh,
        in_specs=(
            P("gx", "ga", "gz"),
            P("gx", "ga", "gz"),
            P(None, ("gx", "gz", "ga")),
            P(None, ("gx", "gz", "ga")),
            P(None, ("gx", "gz", "ga")),
            P(("gx", "gz", "ga")),
            P(),
            P(),
            P(),
        ),
        out_specs=(P("gx", "ga", "gz"), P("gx", "ga", "gz"), P(), P(), P()),
        check_vma=False,
    )
```

```python
import functools

import jax
import jax.numpy as jnp
from jax import lax
from jax.experimental import pallas as pl
from jax.experimental.pallas import tpu as pltpu
from jax.sharding import PartitionSpec as P

EL = 8
ITERS = 12
TILE = 256
TILES_AT_ONCE = 3
AXES = ("gx", "gz", "ga")
ONE_PHASE = 64
STAGES = 7

taps = (1.6, -0.2, 8.0 / 315.0, -1.0 / 560.0)
center = 3.0 * 205.0 / 72.0
epsilon = 1e-06
half = 1.1
MESH = pl.DeviceIdType.MESH
F32 = jnp.float32
BF16 = jnp.bfloat16


def dot(a, b, dims=((1,), (0,)), precision=None):
    return lax.dot_general(a, b, (dims, ((), ())), preferred_element_type=F32, precision=precision)


def sigmoid(v):
    return 1.0 / (1.0 + jnp.exp(-v))


def phases_of(sizes):
    total = 1
    for a in AXES:
        total *= sizes[a]
    return (AXES,) if total <= ONE_PHASE else (("gx",), ("gz", "ga"))


def shift_offsets(sizes):
    combos = [()]
    for n in sizes:
        combos = [c + (k,) for c in combos for k in range(n)]
    return combos[1:]


def krylov_coefficients(mu):
    n = len(mu) // 2
    one = jnp.ones_like(mu[0])
    rho, pi = dict(enumerate(mu)), dict(enumerate(mu))
    r, p, x = [one], [one], []
    for k in range(n):
        last = 2 * n - 2 - k
        tau = {}
        for l in range(k, last + 1):
            tau[l] = pi[l] + 0.5 * (pi[l + 1] + pi[abs(l - 1)])
        alpha = rho[k] / tau[k]
        x = [a + alpha * b for a, b in zip(x, p)] + [alpha * b for b in p[len(x):]]
        moved = list(p) + [jnp.zeros_like(one)]
        for j, b in enumerate(p):
            if j == 0:
                moved[1] = moved[1] + b
            else:
                moved[j - 1] = moved[j - 1] + 0.5 * b
                moved[j + 1] = moved[j + 1] + 0.5 * b
        r = [a - alpha * b for a, b in zip(r + [jnp.zeros_like(one)], moved)]
        if k + 1 < n:
            new = {l: rho[l] - alpha * tau[l] for l in range(k + 1, last + 1)}
            beta = (-alpha if k == 0 else -0.5 * alpha) * new[k + 1] / rho[k]
            p = [a + beta * b for a, b in zip(r, p)] + r[len(p):]
            pi = {l: (new[l] if l > k else 0.0) + beta * pi[l] for l in range(k, last + 1)}
            rho = new
    return [v * (1.0 / half) for v in x], r


def solve_kernel(
    sizes, right, diag, feats, bank, target, index, w1, w2, w3, press, resid, total_grads,
    mp, nb, basis, pre, inv, yp, yr, zp, zr, eta, ar_src, ar_dst,
    bank_v, counts, grads, swapped, halved, first, held, second, owned, third, full,
    small, small_in, small_third,
    bank_sem, g_send, g_recv, h_send, h_recv, a_send, a_recv,
):
    lx, ly, lz = right.shape
    ch, columns = bank.shape
    stress = target.shape[0]
    tiles = columns // TILE
    pos = {a: lax.axis_index(a) for a in AXES}
    phases = phases_of(sizes)

    def tile_copy(t):
        return pltpu.make_async_copy(
            bank.at[:, pl.ds(t * TILE, TILE)], bank_v.at[t], bank_sem.at[t]
        )

    for t in range(tiles):
        tile_copy(t).start()

    def coords(axes, offs, sign):
        out = {}
        for a, k in zip(axes, offs):
            n = sizes[a]
            c = pos[a] + (k if sign > 0 else n - k) if k else pos[a]
            out[a] = lax.rem(c, n) if k else c
        return out

    def flat(axes, at):
        value = 0
        for a in axes:
            value = value * sizes[a] + at[a]
        return value

    groups = []
    for axes in phases:
        me = flat(axes, pos)
        peers = []
        for offs in shift_offsets([sizes[a] for a in axes]):
            to = {**pos, **coords(axes, offs, 1)}
            source = flat(axes, coords(axes, offs, -1))
            peers.append((to, source))
        groups.append((me, peers))

    nx, nz, na = sizes["gx"], sizes["gz"], sizes["ga"]
    pair = 2 if nz % 2 == 0 else 1
    nh = nz // pair
    side, spot = lax.rem(pos["gz"], pair), lax.div(pos["gz"], pair)
    half_rows = grads.shape[0] // pair
    share = half_rows // nh
    piece = share // na

    def half_of(b):
        return pl.ds(pl.multiple_of(b * half_rows, 8), half_rows)

    def share_of(h):
        return pl.ds(pl.multiple_of(h * share, 8), share)

    def block_of(h, ia=None):
        start = side * half_rows + h * share
        if ia is None:
            return pl.ds(pl.multiple_of(start, 8), share)
        return pl.ds(pl.multiple_of(start + ia * piece, 8), piece)

    def along(axis, k, sign):
        return coords((axis,), (k,), sign)[axis]

    def spot_along(k, sign):
        return lax.rem(spot + (k if sign > 0 else nh - k), nh)

    numbers = {}

    def gradient_copy(kind, k, src, dst, to):
        number = numbers.setdefault((kind, k), len(numbers))
        return pltpu.make_async_remote_copy(
            src_ref=src,
            dst_ref=dst,
            send_sem=g_send.at[number],
            recv_sem=g_recv.at[number],
            device_id={**pos, **to},
            device_id_type=MESH,
        )

    def to_pair():
        return {"gz": spot * pair + (pair - 1 - side)}

    def to_spot(k):
        return {"gz": spot_along(k, 1) * pair + side}

    def swap_pair():
        other = half_of(pair - 1 - side)
        return [
            gradient_copy("swap", 0, grads.at[other], swapped, to_pair()),
            gradient_copy("swap", 1, small.at[0], small_in.at[0], to_pair()),
        ]

    def scatter_gz(k):
        return [
            gradient_copy("gz", k, halved.at[share_of(spot_along(k, 1))], first.at[k - 1], to_spot(k)),
            gradient_copy("small gz", k, small.at[1], small_in.at[k], to_spot(k)),
        ]

    def scatter_ga(k):
        rows = pl.ds(pl.multiple_of(along("ga", k, 1) * piece, 8), piece)
        to = {"ga": along("ga", k, 1)}
        return [
            gradient_copy("ga", k, held.at[rows], second.at[k - 1], to),
            gradient_copy("small ga", k, small.at[2], small_in.at[nh + k - 1], to),
        ]

    def add_gx(k, sign=1):
        slot = pos["gx"] if sign > 0 else along("gx", k, -1)
        to = {"gx": along("gx", k, 1)}
        return [
            gradient_copy("gx", k, owned, third.at[slot], to),
            gradient_copy("small gx", k, small.at[3], small_third.at[slot], to),
        ]

    def gather_ga(k, sign=1):
        at = pos["ga"] if sign > 0 else along("ga", k, -1)
        rows = block_of(spot, at)
        return [gradient_copy("all ga", k, full.at[rows], full.at[rows], {"ga": along("ga", k, 1)})]

    def gather_gz(k, sign=1):
        rows = block_of(spot if sign > 0 else spot_along(k, -1))
        return [gradient_copy("all gz", k, full.at[rows], full.at[rows], to_spot(k))]

    def gather_pair(sign=1):
        rows = half_of(side if sign > 0 else pair - 1 - side)
        return [gradient_copy("all pair", 0, full.at[rows], full.at[rows], to_pair())]

    def start(copies):
        for copy in copies:
            copy.start()

    def arrived(copies):
        for copy in copies:
            copy.wait_recv()

    def sent(copies):
        for copy in copies:
            copy.wait_send()

    def gradient_stage(stage):
        if stage == 0:
            if pair > 1:
                start(swap_pair())
        elif stage == 1:
            total, few = grads[half_of(side), :], small[0]
            if pair > 1:
                arrived(swap_pair())
                total, few = total + swapped[...], few + small_in[0]
            halved[...] = total
            small[1] = few
            for k in range(1, nh):
                start(scatter_gz(k))
        elif stage == 2:
            total, few = halved[share_of(spot), :], small[1]
            for k in range(1, nh):
                arrived(scatter_gz(k))
                total, few = total + first[k - 1], few + small_in[k]
            held[...] = total
            small[2] = few
            for k in range(1, na):
                start(scatter_ga(k))
        elif stage == 3:
            total, few = held[pl.ds(pl.multiple_of(pos["ga"] * piece, 8), piece), :], small[2]
            for k in range(1, na):
                arrived(scatter_ga(k))
                total, few = total + second[k - 1], few + small_in[nh + k - 1]
            owned[...] = total
            third[pos["gx"]] = total
            small[3] = few
            small_third[pos["gx"]] = few
            for k in range(1, nx):
                start(add_gx(k))
        elif stage == 4:
            for k in range(1, nx):
                arrived(add_gx(k, -1))
            full[block_of(spot, pos["ga"]), :] = jnp.sum(third[...], axis=0)
            for k in range(1, na):
                start(gather_ga(k))
        elif stage == 5:
            for k in range(1, na):
                arrived(gather_ga(k, -1))
            for k in range(1, nh):
                start(gather_gz(k))
        elif stage == 6:
            for k in range(1, nh):
                arrived(gather_gz(k, -1))
            if pair > 1:
                start(gather_pair())
        else:
            if pair > 1:
                arrived(gather_pair(-1))
                sent(swap_pair() + gather_pair())
            for k in range(1, nh):
                sent(scatter_gz(k) + gather_gz(k))
            for k in range(1, na):
                sent(scatter_ga(k) + gather_ga(k))
            for k in range(1, nx):
                sent(add_gx(k))

    def count_samples():
        samples = index.shape[1]
        ids = index[...]
        high = lax.broadcasted_iota(jnp.int32, (columns // 128, samples), 0) == (ids // 128)
        low = lax.broadcasted_iota(jnp.int32, (128, samples), 0) == (ids % 128)
        counts[...] = dot(
            jnp.where(high, 1.0, 0.0).astype(BF16),
            jnp.where(low, 1.0, 0.0).astype(BF16),
            ((1,), (1,)),
        )

    def gradient_tile(t):
        rows = TILE // 128
        tile_copy(t).wait()
        weight = jnp.concatenate([counts[pl.ds(t * rows + j, 1), :] for j in range(rows)], axis=1)
        x = bank_v[t]
        a1, a2, a3 = w1[...], w2[...], w3[...]
        l1 = dot(a1, x)
        s1 = sigmoid(l1)
        h1 = (l1 * s1).astype(BF16)
        l2 = dot(a2, h1)
        s2 = sigmoid(l2)
        h2 = (l2 * s2).astype(BF16)
        goal = target[:, pl.ds(pl.multiple_of(t * TILE, TILE), TILE)]
        error = (dot(a3, h2) - goal.astype(F32)).astype(BF16)

        def weighted(delta, right):
            scaled = delta.astype(F32) * weight
            upper = scaled.astype(BF16)
            lower = (scaled - upper.astype(F32)).astype(BF16)
            return dot(upper, right, ((1,), (1,))) + dot(lower, right, ((1,), (1,)))

        small[0, :stress] += weighted(error, h2)
        d2 = (dot(a3, error, ((0,), (0,))) * (s2 * (1.0 + l2 * (1.0 - s2)))).astype(BF16)
        grads[ch : 2 * ch] += weighted(d2, h1)
        d1 = (dot(a2, d2, ((0,), (0,))) * (s1 * (1.0 + l1 * (1.0 - s1)))).astype(BF16)
        grads[:ch] += weighted(d1, x)

    loops = -(-tiles // TILES_AT_ONCE)

    def gradient_work(i):
        def one(t, carry):
            gradient_tile(t)
            return carry

        lax.fori_loop(
            jnp.minimum(i * TILES_AT_ONCE, tiles), jnp.minimum((i + 1) * TILES_AT_ONCE, tiles), one, 0
        )
        for stage in range(STAGES):
            pl.when(i == min(loops - 1 + stage, ITERS - 1))(lambda stage=stage: gradient_stage(stage))

    mp[...] = jnp.zeros_like(mp)
    yr[...] = jnp.zeros_like(yr)
    zr[...] = jnp.zeros_like(zr)

    barrier = pltpu.get_barrier_semaphore()
    total = 0
    for _, peers in groups:
        for to, _ in peers:
            pl.semaphore_signal(barrier, inc=1, device_id=to, device_id_type=MESH)
            total += 1

    lane = lax.broadcasted_iota(jnp.int32, (ly, lz), 1)
    sub8 = lax.broadcasted_iota(jnp.int32, (8, lz), 0)

    def halo_copies(par):
        out = {}

        def add(axis, step, number, src, dst, part=None):
            copy = pltpu.make_async_remote_copy(
                src_ref=src,
                dst_ref=dst,
                send_sem=h_send.at[par, number],
                recv_sem=h_recv.at[par, number],
                device_id={**pos, axis: jnp.clip(pos[axis] + step, 0, sizes[axis] - 1)},
                device_id_type=MESH,
            )
            can_send = pos[axis] < sizes[axis] - 1 if step > 0 else pos[axis] > 0
            will_get = pos[axis] > 0 if step > 0 else pos[axis] < sizes[axis] - 1
            out.setdefault(part or axis, []).append((copy, can_send, will_get))

        rows = pl.ds(8, ly)
        if sizes["gx"] > 1:
            add("gx", 1, 0, mp.at[par, pl.ds(lx + 2, 2), rows], mp.at[par, pl.ds(2, 2), rows], "high outer")
            add("gx", -1, 1, mp.at[par, pl.ds(4, 2), rows], mp.at[par, pl.ds(lx + 4, 2), rows], "low outer")
            add("gx", 1, 6, mp.at[par, pl.ds(lx, 2), rows], mp.at[par, pl.ds(0, 2), rows], "high inner")
            add("gx", -1, 7, mp.at[par, pl.ds(6, 2), rows], mp.at[par, pl.ds(lx + 6, 2), rows], "low inner")
        if sizes["ga"] > 1:
            add("ga", 1, 2, yp.at[par, 0], yr.at[par, 0])
            add("ga", -1, 3, yp.at[par, 1], yr.at[par, 1])
        if sizes["gz"] > 1:
            add("gz", 1, 4, zp.at[par], zr.at[par, 0])
            add("gz", -1, 5, zp.at[par], zr.at[par, 1])
        return out

    def halo_start(par, *axes):
        copies = halo_copies(par)
        for axis in axes:
            for copy, can_send, _ in copies.get(axis, []):
                pl.when(can_send)(copy.start)

    def halo_wait(par):
        for copies in halo_copies(par).values():
            for copy, _, will_get in copies:
                pl.when(will_get)(copy.wait_recv)

    def halo_sent(par):
        for copies in halo_copies(par).values():
            for copy, can_send, _ in copies:
                pl.when(can_send)(copy.wait_send)

    bases = []
    base = 0
    for axes in phases:
        bases.append(base)
        n = 1
        for a in axes:
            n *= sizes[a]
        base += n

    def sum_copies(phase):
        me, peers = groups[phase]
        out = []
        for k, (to, source) in enumerate(peers):
            slot = bases[phase]
            send = pltpu.make_async_remote_copy(
                src_ref=ar_src.at[phase],
                dst_ref=ar_dst.at[slot + me],
                send_sem=a_send.at[slot + k],
                recv_sem=a_recv.at[slot + me],
                device_id=to,
                device_id_type=MESH,
            )
            receive = pltpu.make_async_remote_copy(
                src_ref=ar_src.at[phase],
                dst_ref=ar_dst.at[slot + source],
                send_sem=a_send.at[slot + k],
                recv_sem=a_recv.at[slot + source],
                device_id=to,
                device_id_type=MESH,
            )
            out.append((send, receive))
        return out

    def sum_start(phase, row):
        ar_src[phase] = row
        ar_dst[bases[phase] + groups[phase][0]] = row
        for send, _ in sum_copies(phase):
            send.start()

    def sum_wait(phase):
        count = len(groups[phase][1]) + 1
        for _, receive in sum_copies(phase):
            receive.wait_recv()
        return jnp.sum(ar_dst[pl.ds(bases[phase], count)], axis=0)

    def sums_sent():
        for phase in range(len(phases)):
            for send, _ in sum_copies(phase):
                send.wait_send()

    def stencil_local(par):
        for x in range(lx):
            v = mp[par, 4 + x, pl.ds(8, ly)]
            acc = None
            for k in range(1, 5):
                t = mp[par, 4 + x, pl.ds(8 + k, ly)] + mp[par, 4 + x, pl.ds(8 - k, ly)]
                if x + k < lx:
                    t = t + mp[par, 4 + x + k, pl.ds(8, ly)]
                if x - k >= 0:
                    t = t + mp[par, 4 + x - k, pl.ds(8, ly)]
                t = t + jnp.where(lane >= k, pltpu.roll(v, k, 1), 0.0)
                t = t + jnp.where(lane < lz - k, pltpu.roll(v, lz - k, 1), 0.0)
                t = taps[k - 1] * t
                acc = t if acc is None else acc + t
            nb[x] = acc

    def z_correction(par):
        h = jnp.where(lane % 8 < 4, zr[par, 0], zr[par, 1])
        acc = jnp.zeros((ly, lz), F32)
        place = lane % 8
        for k in range(1, 5):
            ahead = jnp.where((place >= 4) & (place - 4 < k), pltpu.roll(h, k, 1), 0.0)
            behind = jnp.where((place < 4) & (place >= 4 - k), pltpu.roll(h, lz - k, 1), 0.0)
            acc = acc + taps[k - 1] * (ahead + behind)
        return acc

    def corrected(par, x, zc):
        acc = nb[x]
        for k in range(1, 5):
            if x - k < 0:
                acc = acc + taps[k - 1] * mp[par, 4 + x - k, pl.ds(8, ly)]
            if x + k >= lx:
                acc = acc + taps[k - 1] * mp[par, 4 + x + k, pl.ds(8, ly)]
        z = pltpu.roll(zc, (2 * lz - 8 * x - 4) % lz, 1)
        acc = acc + jnp.where((lane < 4) | (lane >= lz - 4), z, 0.0)
        if x % 2 == 0:
            h = jnp.where(sub8 < 4, yr[par, 1, x // 2], yr[par, 0, x // 2])
        else:
            h = pltpu.roll(jnp.where(sub8 < 4, yr[par, 0, x // 2], yr[par, 1, x // 2]), 4, 0)
        low = jnp.zeros((8, lz), F32)
        high = jnp.zeros((8, lz), F32)
        for k in range(1, 5):
            low = low + taps[k - 1] * jnp.where(sub8 < k, pltpu.roll(h, k, 0), 0.0)
            high = high + taps[k - 1] * jnp.where(sub8 >= 8 - k, pltpu.roll(h, 8 - k, 0), 0.0)
        parts = [acc[:8] + low] + ([acc[8:-8]] if ly > 16 else []) + [acc[-8:] + high]
        return jnp.concatenate(parts, axis=0)

    def publish(par, x, m, packed, edges):
        mp[par, 4 + x, pl.ds(8, ly)] = m
        if x % 2 == 0:
            edges = (m[:8], m[-8:])
        else:
            yp[par, 0, x // 2] = jnp.where(sub8 < 4, pltpu.roll(m[-8:], 4, 0), edges[1])
            yp[par, 1, x // 2] = jnp.where(sub8 < 4, edges[0], pltpu.roll(m[:8], 4, 0))
        turned = pltpu.roll(m, (8 * x + 4) % lz, 1)
        return jnp.where((lane >= 8 * x) & (lane < 8 * x + 8), turned, packed), edges

    order = [lx - 2, lx - 1, 0, 1, lx - 4, lx - 3, 2, 3] + list(range(4, lx - 4))
    leave = {1: "high outer", 3: "low outer", 5: "high inner", 7: "low inner"}

    hidden = dot(w1[...], feats[...])
    hidden = (hidden * sigmoid(hidden)).astype(BF16)
    hidden = dot(w2[...], hidden)
    hidden = (hidden * sigmoid(hidden)).astype(BF16)
    predicted = dot(w3[...], hidden)
    trace = (predicted[0:1] + predicted[1:2] + predicted[2:3]) / 3.0
    ex, ey, ez = lx // EL, ly // EL, lz // EL
    spread = jnp.where(
        lax.broadcasted_iota(jnp.int32, (lz, lz), 0) == lax.broadcasted_iota(jnp.int32, (lz, lz), 1) // EL,
        1.0,
        0.0,
    )
    lines = jnp.concatenate(
        [trace if e == 0 else pltpu.roll(trace, (lz - e * ez) % lz, 1) for e in range(ex * ey)], axis=0
    )
    forcing = dot(lines, spread, precision=lax.Precision.HIGHEST)
    pl.semaphore_wait(barrier, total)
    packed = jnp.zeros((ly, lz), F32)
    edges = None
    for n, x in enumerate(order):
        line = forcing[(x // EL) * ey : (x // EL) * ey + ey]
        block = jnp.concatenate([jnp.broadcast_to(line[j : j + 1], (EL, lz)) for j in range(ey)], axis=0)
        whole = diag[x] + center
        scale = 1.0 / whole
        pre[x] = whole
        inv[x] = scale * (2.0 / half)
        first_vector = (right[x] + block) * scale
        basis[0, x] = first_vector
        packed, edges = publish(0, x, first_vector, packed, edges)
        if n in leave:
            halo_start(0, leave[n])
    zp[0] = packed
    halo_start(0, "ga", "gz")
    grads[...] = jnp.zeros_like(grads)
    small[...] = jnp.zeros_like(small)
    count_samples()

    def iteration(i, carry):
        par = lax.rem(i, 2)
        later = 1 - par
        stencil_local(par)
        gradient_work(i)
        halo_wait(par)
        zc = z_correction(par)
        start = jnp.where(i == 0, 0.5, 1.0)
        back = jnp.where(i == 0, 0.0, 1.0)
        keep = start * (2.0 / half - 2.0)
        more = i < ITERS - 1
        packed = jnp.zeros((ly, lz), F32)
        even = jnp.zeros((ly, lz), F32)
        odd = jnp.zeros((ly, lz), F32)
        edges = None
        older = jnp.maximum(i - 1, 0)
        for n, x in enumerate(order):
            v = mp[par, 4 + x, pl.ds(8, ly)]
            m = keep * v - start * (inv[x] * corrected(par, x, zc)) - back * basis[older, x]
            basis[i + 1, x] = m
            weighed = pre[x] * v
            even = even + weighed * v
            odd = odd + weighed * m
            packed, edges = publish(later, x, m, packed, edges)
            if n in leave:
                pl.when(more)(lambda: halo_start(later, leave[n]))
        zp[later] = packed
        pl.when(more)(lambda: halo_start(later, "ga", "gz"))
        eta[2 * i] = jnp.sum(even.reshape(ly // 8, 8, lz), axis=0)
        eta[2 * i + 1] = jnp.sum(odd.reshape(ly // 8, 8, lz), axis=0)
        halo_sent(par)
        return carry

    lax.fori_loop(0, ITERS, iteration, 0)

    count = 2 * ITERS
    sums = jnp.sum(jnp.sum(eta[...], axis=1), axis=1, keepdims=True)
    mine = lax.broadcasted_iota(jnp.int32, (count, lz), 0) == lax.broadcasted_iota(jnp.int32, (count, lz), 1)
    row = jnp.sum(jnp.where(mine, sums, 0.0), axis=0, keepdims=True)
    sum_start(0, row)
    for phase in range(1, len(phases)):
        sum_start(phase, sum_wait(phase - 1))
    row = sum_wait(len(phases) - 1)
    spread_row = jnp.sum(jnp.where(mine, row, 0.0), axis=1, keepdims=True)
    moment = [jnp.broadcast_to(spread_row[j : j + 1], (1, lz)) for j in range(count)]
    mu = moment[:2] + [2.0 * moment[j] - moment[j % 2] for j in range(2, count)]
    along_x, along_r = krylov_coefficients(mu)
    for x in range(lx):
        p = along_x[0] * basis[0, x]
        r = along_r[0] * basis[0, x]
        for j in range(1, ITERS):
            v = basis[j, x]
            p = p + along_x[j] * v
            r = r + along_r[j] * v
        press[x] = p
        resid[x] = pre[x] * (r + along_r[ITERS] * basis[ITERS, x])
    gradient_stage(STAGES)
    total_grads[: 2 * ch] = full[...]
    total_grads[2 * ch :] = jnp.sum(small_third[...], axis=0)
    sums_sent()


def pressure_solve(right_side, diagonal, feats, bank, target, index, w1, w2, w3):
    sizes = {a: lax.axis_size(a) for a in AXES}
    lx, ly, lz = right_side.shape
    ch, columns = bank.shape
    slots = 0
    phases = phases_of(sizes)
    for axes in phases:
        n = 1
        for a in axes:
            n *= sizes[a]
        slots += n
    nx, nz, na = (sizes[a] for a in ("gx", "gz", "ga"))
    rows = w1.shape[0] + w2.shape[0]
    few = (w3.shape[0] + 7) // 8 * 8
    pair = 2 if nz % 2 == 0 else 1
    nh = nz // pair
    share = rows // nz
    piece = share // na
    tiles = columns // TILE
    copies = 3 + 3 * (nh - 1) + 3 * (na - 1) + 2 * (nx - 1)
    field = pltpu.VMEM((lx, ly, lz), F32)
    vmem = pl.BlockSpec(memory_space=pltpu.VMEM)
    return pl.pallas_call(
        functools.partial(solve_kernel, sizes),
        out_shape=[jax.ShapeDtypeStruct((lx, ly, lz), F32)] * 2 + [jax.ShapeDtypeStruct((rows + few, ch), F32)],
        in_specs=[vmem] * 3 + [pl.BlockSpec(memory_space=pl.ANY)] + [vmem] * 5,
        out_specs=[vmem] * 3,
        scratch_shapes=[
            pltpu.VMEM((2, lx + 8, ly + 16, lz), F32),
            field,
            pltpu.VMEM((ITERS + 1, lx, ly, lz), F32),
            field, field,
            pltpu.VMEM((2, 2, lx // 2, 8, lz), F32),
            pltpu.VMEM((2, 2, lx // 2, 8, lz), F32),
            pltpu.VMEM((2, ly, lz), F32),
            pltpu.VMEM((2, 2, ly, lz), F32),
            pltpu.VMEM((2 * ITERS, 8, lz), F32),
            pltpu.VMEM((len(phases), 1, lz), F32),
            pltpu.VMEM((slots, 1, lz), F32),
            pltpu.VMEM((tiles, ch, TILE), BF16),
            pltpu.VMEM((columns // 128, 128), F32),
            pltpu.VMEM((rows, ch), F32),
            pltpu.VMEM((rows // pair, ch), F32),
            pltpu.VMEM((rows // pair, ch), F32),
            pltpu.VMEM((max(nh - 1, 1), share, ch), F32),
            pltpu.VMEM((share, ch), F32),
            pltpu.VMEM((max(na - 1, 1), piece, ch), F32),
            pltpu.VMEM((piece, ch), F32),
            pltpu.VMEM((nx, piece, ch), F32),
            pltpu.VMEM((rows, ch), F32),
            pltpu.VMEM((4, few, ch), F32),
            pltpu.VMEM((nh + na - 1, few, ch), F32),
            pltpu.VMEM((nx, few, ch), F32),
            pltpu.SemaphoreType.DMA((tiles,)),
            pltpu.SemaphoreType.DMA((copies,)),
            pltpu.SemaphoreType.DMA((copies,)),
            pltpu.SemaphoreType.DMA((2, 8)),
            pltpu.SemaphoreType.DMA((2, 8)),
            pltpu.SemaphoreType.DMA((slots,)),
            pltpu.SemaphoreType.DMA((slots,)),
        ],
        compiler_params=pltpu.CompilerParams(collective_id=0, has_side_effects=True),
        cost_estimate=pl.CostEstimate(
            flops=60_000_000, bytes_accessed=200_000_000, transcendentals=0
        ),
    )(right_side, diagonal, feats, bank, target, index.reshape(1, -1), w1, w2, w3)


def finish_kernel(press_in, resid_in, grads, press, resid, step1, step2, step3):
    press[...] = press_in[...]
    resid[...] = resid_in[...]
    ch = step1.shape[0]
    start = 0
    for out in (step1, step2, step3):
        count = out.shape[0]
        value = grads[start : start + count]
        squares = jnp.sum(jnp.sum(value * value, axis=0, keepdims=True), axis=1, keepdims=True)
        out[...] = value * lax.rsqrt(squares / (count * ch) + epsilon)
        start += count


def finish(press, resid, grads, weights):
    vmem = pl.BlockSpec(memory_space=pltpu.VMEM)
    return pl.pallas_call(
        finish_kernel,
        out_shape=[jax.ShapeDtypeStruct(press.shape, F32)] * 2
        + [jax.ShapeDtypeStruct(w.shape, F32) for w in weights],
        in_specs=[vmem] * 3,
        out_specs=[vmem] * 5,
        cost_estimate=pl.CostEstimate(flops=1_000_000, bytes_accessed=2_000_000, transcendentals=0),
    )(press, resid, grads)


def body(
    right_side, diagonal, element_features, sample_bank, target_bank, patch_index, w_first, w_second, w_third
):
    weights = (w_first, w_second, w_third)
    solved = pressure_solve(
        right_side, diagonal, element_features, sample_bank, target_bank, patch_index, *weights
    )
    return tuple(finish(*solved, weights))


def solution(mesh):
    return jax.shard_map(
        body,
        mesh=mesh,
        in_specs=(
            P("gx", "ga", "gz"),
            P("gx", "ga", "gz"),
            P(None, ("gx", "gz", "ga")),
            P(None, ("gx", "gz", "ga")),
            P(None, ("gx", "gz", "ga")),
            P(("gx", "gz", "ga")),
            P(),
            P(),
            P(),
        ),
        out_specs=(P("gx", "ga", "gz"), P("gx", "ga", "gz"), P(), P(), P()),
        check_vma=False,
    )
```

```python
import functools

import jax
import jax.numpy as jnp
from jax import lax
from jax.experimental import pallas as pl
from jax.experimental.pallas import tpu as pltpu
from jax.sharding import PartitionSpec as P

EL = 8
ITERS = 12
TILE = 1024
AXES = ("gx", "gz", "ga")
ONE_PHASE = 64
STAGE_STEPS = (0, 1, 3, 5, 6, 8)

taps = (1.6, -0.2, 8.0 / 315.0, -1.0 / 560.0)
center = 3.0 * 205.0 / 72.0
epsilon = 1e-06
half = 1.1
MESH = pl.DeviceIdType.MESH
F32 = jnp.float32
BF16 = jnp.bfloat16


def dot(a, b, dims=((1,), (0,)), precision=None):
    return lax.dot_general(a, b, (dims, ((), ())), preferred_element_type=F32, precision=precision)


def sigmoid(v):
    return 1.0 / (1.0 + jnp.exp(-v))


def phases_of(sizes):
    total = 1
    for a in AXES:
        total *= sizes[a]
    return (AXES,) if total <= ONE_PHASE else (("gx",), ("gz", "ga"))


def shift_offsets(sizes):
    combos = [()]
    for n in sizes:
        combos = [c + (k,) for c in combos for k in range(n)]
    return combos[1:]


def renormalized(s, e):
    r = s + e
    return r, e - (r - s)


def two_sum(a, b):
    s = a + b
    t = s - a
    return s, (a - (s - t)) + (b - t)


def pair_add(a, b):
    s, e = two_sum(a[0], b[0])
    return renormalized(s, e + (a[1] + b[1]))


def pair_scale(a, c):
    return a[0] * c, a[1] * c


def halves(v):
    t = v * 4097.0
    high = t - (t - v)
    return high, v - high


def pair_mul(a, b):
    p = a[0] * b[0]
    (ah, al), (bh, bl) = halves(a[0]), halves(b[0])
    e = ((ah * bh - p) + ah * bl + al * bh) + al * bl
    return renormalized(p, e + (a[0] * b[1] + a[1] * b[0]))


def pair_div(a, b):
    q = a[0] / b[0]
    rest = pair_add(a, pair_scale(pair_mul((q, jnp.zeros_like(q)), b), -1.0))
    return renormalized(q, rest[0] / b[0])


def krylov_coefficients(eta):
    count, lanes = eta[0].shape
    n = count // 2
    size = (n + 2 + 7) // 8 * 8
    row = lax.broadcasted_iota(jnp.int32, (count, lanes), 0)
    place = lax.broadcasted_iota(jnp.int32, (size, lanes), 0)

    def at(v, j):
        return tuple(jnp.broadcast_to(part[j : j + 1], (1, lanes)) for part in v)

    def wide(v):
        return tuple(jnp.broadcast_to(part, (count, lanes)) for part in v)

    low = tuple(jnp.where(row % 2 == 0, e, o) for e, o in zip(wide(at(eta, 0)), wide(at(eta, 1))))
    moments = pair_add(pair_scale(eta, 2.0), pair_scale(low, -1.0))
    rho = tuple(jnp.where(row < 2, e, m) for e, m in zip(eta, moments))
    pi = rho
    r = jnp.where(place == 0, 1.0, 0.0)
    p, x = r, jnp.zeros_like(r)
    for k in range(n):
        above = tuple(pltpu.roll(v, count - 1, 0) for v in pi)
        below = tuple(pltpu.roll(v, 1, 0) for v in pi)
        if k < 2:
            below = tuple(jnp.where(row == 0, u, v) for u, v in zip(above, below))
        tau = pair_add(pi, pair_scale(pair_add(above, below), 0.5))
        alpha = pair_div(at(rho, k), at(tau, k))
        step = jnp.broadcast_to(alpha[0], (size, lanes))
        x = x + step * p
        ahead = jnp.where(place < size - 1, pltpu.roll(p, size - 1, 0), 0.0)
        r = r - step * (p + 0.5 * (ahead + pltpu.roll(jnp.where(place == 0, 2.0 * p, p), 1, 0)))
        if k + 1 < n:
            new = pair_add(rho, pair_scale(pair_mul(wide(alpha), tau), -1.0))
            gain = pair_scale(pair_div(at(new, k + 1), at(rho, k)), -1.0 if k == 0 else -0.5)
            beta = pair_mul(alpha, gain)
            p = r + jnp.broadcast_to(beta[0], (size, lanes)) * p
            pi = pair_add(new, pair_mul(wide(beta), pi))
            rho = new
    return x * (1.0 / half), r


def solve_kernel(
    sizes, right, diag, feats, bank, target, index, w1, w2, w3, press, resid, total_grads,
    mp, nb, basis, pre, inv, yp, yr, zp, zr, eta, ar_src, ar_dst,
    bank_v, counts, grads, swapped, halved, first, held, second, owned, third, full,
    small, small_in, small_third,
    bank_sem, g_send, g_recv, h_send, h_recv, a_send, a_recv,
):
    lx, ly, lz = right.shape
    ch, columns = bank.shape
    stress = target.shape[0]
    tiles = columns // TILE
    pos = {a: lax.axis_index(a) for a in AXES}
    phases = phases_of(sizes)

    def tile_copy(t):
        return pltpu.make_async_copy(
            bank.at[:, pl.ds(t * TILE, TILE)], bank_v.at[t], bank_sem.at[t]
        )

    for t in range(tiles):
        tile_copy(t).start()

    def coords(axes, offs, sign):
        out = {}
        for a, k in zip(axes, offs):
            n = sizes[a]
            c = pos[a] + (k if sign > 0 else n - k) if k else pos[a]
            out[a] = lax.rem(c, n) if k else c
        return out

    def flat(axes, at):
        value = 0
        for a in axes:
            value = value * sizes[a] + at[a]
        return value

    groups = []
    for axes in phases:
        me = flat(axes, pos)
        peers = []
        for offs in shift_offsets([sizes[a] for a in axes]):
            to = {**pos, **coords(axes, offs, 1)}
            source = flat(axes, coords(axes, offs, -1))
            far = sum(min(k, sizes[a] - k) for a, k in zip(axes, offs))
            peers.append((far, to, source))
        peers = [(to, source) for far, to, source in sorted(peers, key=lambda peer: -peer[0])]
        groups.append((me, peers))

    nx, nz, na = sizes["gx"], sizes["gz"], sizes["ga"]
    pair = 2 if nz % 2 == 0 else 1
    nh = nz // pair
    side, spot = lax.rem(pos["gz"], pair), lax.div(pos["gz"], pair)
    half_rows = grads.shape[0] // pair
    share = half_rows // nh
    piece = share // na

    def half_of(b):
        return pl.ds(pl.multiple_of(b * half_rows, 8), half_rows)

    def share_of(h):
        return pl.ds(pl.multiple_of(h * share, 8), share)

    def block_of(h, ia=None):
        start = side * half_rows + h * share
        if ia is None:
            return pl.ds(pl.multiple_of(start, 8), share)
        return pl.ds(pl.multiple_of(start + ia * piece, 8), piece)

    def along(axis, k, sign):
        return coords((axis,), (k,), sign)[axis]

    def spot_along(k, sign):
        return lax.rem(spot + (k if sign > 0 else nh - k), nh)

    numbers = {}

    def gradient_copy(kind, k, src, dst, to):
        number = numbers.setdefault((kind, k), len(numbers))
        return pltpu.make_async_remote_copy(
            src_ref=src,
            dst_ref=dst,
            send_sem=g_send.at[number],
            recv_sem=g_recv.at[number],
            device_id={**pos, **to},
            device_id_type=MESH,
        )

    def to_pair():
        return {"gz": spot * pair + (pair - 1 - side)}

    def to_spot(k):
        return {"gz": spot_along(k, 1) * pair + side}

    def swap_pair():
        other = half_of(pair - 1 - side)
        return [
            gradient_copy("swap", 0, grads.at[other], swapped, to_pair()),
            gradient_copy("swap", 1, small.at[0], small_in.at[0], to_pair()),
        ]

    def scatter_gz(k):
        return [
            gradient_copy("gz", k, halved.at[share_of(spot_along(k, 1))], first.at[k - 1], to_spot(k)),
            gradient_copy("small gz", k, small.at[1], small_in.at[k], to_spot(k)),
        ]

    def scatter_ga(k):
        rows = pl.ds(pl.multiple_of(along("ga", k, 1) * piece, 8), piece)
        to = {"ga": along("ga", k, 1)}
        return [
            gradient_copy("ga", k, held.at[rows], second.at[k - 1], to),
            gradient_copy("small ga", k, small.at[2], small_in.at[nh + k - 1], to),
        ]

    def add_gx(k, sign=1):
        slot = pos["gx"] if sign > 0 else along("gx", k, -1)
        to = {"gx": along("gx", k, 1)}
        return [
            gradient_copy("gx", k, owned, third.at[slot], to),
            gradient_copy("small gx", k, small.at[3], small_third.at[slot], to),
        ]

    def gather_ga(k, sign=1):
        at = pos["ga"] if sign > 0 else along("ga", k, -1)
        rows = block_of(spot, at)
        return [gradient_copy("all ga", k, full.at[rows], full.at[rows], {"ga": along("ga", k, 1)})]

    def gather_gz(k, sign=1):
        rows = block_of(spot if sign > 0 else spot_along(k, -1))
        return [gradient_copy("all gz", k, full.at[rows], full.at[rows], to_spot(k))]

    def gather_pair(sign=1):
        rows = half_of(side if sign > 0 else pair - 1 - side)
        return [gradient_copy("all pair", 0, full.at[rows], full.at[rows], to_pair())]

    def start(copies):
        for copy in copies:
            copy.start()

    def arrived(copies):
        for copy in copies:
            copy.wait_recv()

    def sent(copies):
        for copy in copies:
            copy.wait_send()

    def gradient_stage(stage):
        if stage == 0:
            if pair > 1:
                start(swap_pair())
        elif stage == 1:
            total, few = grads[half_of(side), :], small[0]
            if pair > 1:
                arrived(swap_pair())
                total, few = total + swapped[...], few + small_in[0]
            halved[...] = total
            small[1] = few
            for k in range(1, nh):
                start(scatter_gz(k))
        elif stage == 2:
            total, few = halved[share_of(spot), :], small[1]
            for k in range(1, nh):
                arrived(scatter_gz(k))
                total, few = total + first[k - 1], few + small_in[k]
            held[...] = total
            small[2] = few
            for k in range(1, na):
                start(scatter_ga(k))
        elif stage == 3:
            total, few = held[pl.ds(pl.multiple_of(pos["ga"] * piece, 8), piece), :], small[2]
            for k in range(1, na):
                arrived(scatter_ga(k))
                total, few = total + second[k - 1], few + small_in[nh + k - 1]
            owned[...] = total
            third[pos["gx"]] = total
            small[3] = few
            small_third[pos["gx"]] = few
            for k in range(1, nx):
                start(add_gx(k))
        elif stage == 4:
            for k in range(1, nx):
                arrived(add_gx(k, -1))
            full[block_of(spot, pos["ga"]), :] = jnp.sum(third[...], axis=0)
            for k in range(1, na):
                start(gather_ga(k))
        elif stage == 5:
            for k in range(1, na):
                arrived(gather_ga(k, -1))
            for k in range(1, nh):
                start(gather_gz(k))
        elif stage == 6:
            for k in range(1, nh):
                arrived(gather_gz(k, -1))
            if pair > 1:
                start(gather_pair())
        else:
            if pair > 1:
                arrived(gather_pair(-1))
                sent(swap_pair() + gather_pair())
            for k in range(1, nh):
                sent(scatter_gz(k) + gather_gz(k))
            for k in range(1, na):
                sent(scatter_ga(k) + gather_ga(k))
            for k in range(1, nx):
                sent(add_gx(k))

    def count_samples():
        samples = index.shape[1]
        ids = index[...]
        high = lax.broadcasted_iota(jnp.int32, (columns // 128, samples), 0) == (ids // 128)
        low = lax.broadcasted_iota(jnp.int32, (128, samples), 0) == (ids % 128)
        counts[...] = dot(
            jnp.where(high, 1.0, 0.0).astype(BF16),
            jnp.where(low, 1.0, 0.0).astype(BF16),
            ((1,), (1,)),
        )

    def gradient_tile(t):
        rows = TILE // 128
        tile_copy(t).wait()
        weight = jnp.concatenate([counts[pl.ds(t * rows + j, 1), :] for j in range(rows)], axis=1)
        x = bank_v[t]
        a1, a2, a3 = w1[...], w2[...], w3[...]
        l1 = dot(a1, x)
        s1 = sigmoid(l1)
        h1 = (l1 * s1).astype(BF16)
        l2 = dot(a2, h1)
        s2 = sigmoid(l2)
        h2 = (l2 * s2).astype(BF16)
        goal = target[:, pl.ds(pl.multiple_of(t * TILE, TILE), TILE)]
        error = (dot(a3, h2) - goal.astype(F32)).astype(BF16)

        def weighted(delta, right):
            scaled = delta.astype(F32) * weight
            upper = scaled.astype(BF16)
            lower = (scaled - upper.astype(F32)).astype(BF16)
            return dot(upper, right, ((1,), (1,))) + dot(lower, right, ((1,), (1,)))

        small[0, :stress] += weighted(error, h2)
        d2 = (dot(a3, error, ((0,), (0,))) * (s2 * (1.0 + l2 * (1.0 - s2)))).astype(BF16)
        grads[ch : 2 * ch] += weighted(d2, h1)
        d1 = (dot(a2, d2, ((0,), (0,))) * (s1 * (1.0 + l1 * (1.0 - s1)))).astype(BF16)
        grads[:ch] += weighted(d1, x)

    def gradient_work(i):
        pl.when(i < tiles)(lambda: gradient_tile(i))
        for stage, step in enumerate(STAGE_STEPS):
            pl.when(i == tiles - 1 + step)(lambda stage=stage: gradient_stage(stage))

    mp[...] = jnp.zeros_like(mp)
    yr[...] = jnp.zeros_like(yr)
    zr[...] = jnp.zeros_like(zr)

    barrier = pltpu.get_barrier_semaphore()
    total = 0
    for _, peers in groups:
        for to, _ in peers:
            pl.semaphore_signal(barrier, inc=1, device_id=to, device_id_type=MESH)
            total += 1

    lane = lax.broadcasted_iota(jnp.int32, (ly, lz), 1)
    sub8 = lax.broadcasted_iota(jnp.int32, (8, lz), 0)

    def halo_copies(par):
        out = {}

        def add(axis, step, number, src, dst):
            copy = pltpu.make_async_remote_copy(
                src_ref=src,
                dst_ref=dst,
                send_sem=h_send.at[par, number],
                recv_sem=h_recv.at[par, number],
                device_id={**pos, axis: jnp.clip(pos[axis] + step, 0, sizes[axis] - 1)},
                device_id_type=MESH,
            )
            can_send = pos[axis] < sizes[axis] - 1 if step > 0 else pos[axis] > 0
            will_get = pos[axis] > 0 if step > 0 else pos[axis] < sizes[axis] - 1
            out.setdefault(axis, []).append((copy, can_send, will_get))

        rows = pl.ds(8, ly)
        if sizes["gx"] > 1:
            add("gx", 1, 0, mp.at[par, pl.ds(lx, 4), rows], mp.at[par, pl.ds(0, 4), rows])
            add("gx", -1, 1, mp.at[par, pl.ds(4, 4), rows], mp.at[par, pl.ds(lx + 4, 4), rows])
        if sizes["ga"] > 1:
            add("ga", 1, 2, yp.at[par, 0], yr.at[par, 0])
            add("ga", -1, 3, yp.at[par, 1], yr.at[par, 1])
        if sizes["gz"] > 1:
            add("gz", 1, 4, zp.at[par], zr.at[par, 0])
            add("gz", -1, 5, zp.at[par], zr.at[par, 1])
        return out

    def halo_start(par, *axes):
        copies = halo_copies(par)
        for axis in axes:
            for copy, can_send, _ in copies.get(axis, []):
                pl.when(can_send)(copy.start)

    def halo_wait(par):
        for copies in halo_copies(par).values():
            for copy, _, will_get in copies:
                pl.when(will_get)(copy.wait_recv)

    def halo_sent(par):
        for copies in halo_copies(par).values():
            for copy, can_send, _ in copies:
                pl.when(can_send)(copy.wait_send)

    bases = []
    base = 0
    for axes in phases:
        bases.append(base)
        n = 1
        for a in axes:
            n *= sizes[a]
        base += n

    def sum_copies(phase):
        me, peers = groups[phase]
        out = []
        for k, (to, source) in enumerate(peers):
            slot = bases[phase]
            send = pltpu.make_async_remote_copy(
                src_ref=ar_src.at[phase],
                dst_ref=ar_dst.at[slot + me],
                send_sem=a_send.at[slot + k],
                recv_sem=a_recv.at[slot + me],
                device_id=to,
                device_id_type=MESH,
            )
            receive = pltpu.make_async_remote_copy(
                src_ref=ar_src.at[phase],
                dst_ref=ar_dst.at[slot + source],
                send_sem=a_send.at[slot + k],
                recv_sem=a_recv.at[slot + source],
                device_id=to,
                device_id_type=MESH,
            )
            out.append((send, receive))
        return out

    def sum_start(phase, row):
        ar_src[phase] = row
        ar_dst[bases[phase] + groups[phase][0]] = row
        for send, _ in sum_copies(phase):
            send.start()

    def sum_wait(phase):
        count = len(groups[phase][1]) + 1
        for _, receive in sum_copies(phase):
            receive.wait_recv()
        parts = [ar_dst[bases[phase] + j] for j in range(count)]
        parts = [(v, jnp.zeros_like(v)) for v in parts]
        while len(parts) > 1:
            joined = [pair_add(a, b) for a, b in zip(parts[::2], parts[1::2])]
            parts = joined + parts[2 * len(joined) :]
        return pair_add(parts[0], tuple(pltpu.roll(v, lz // 2, 1) for v in parts[0]))

    def packed_pair(v):
        first_half = lax.broadcasted_iota(jnp.int32, (1, lz), 1) < lz // 2
        return jnp.where(first_half, v[0], pltpu.roll(v[1], lz // 2, 1))

    def sums_sent():
        for phase in range(len(phases)):
            for send, _ in sum_copies(phase):
                send.wait_send()

    def stencil_local(par, keep, start, back, older):
        even = jnp.zeros((ly, lz), F32)
        for x in range(lx):
            v = mp[par, 4 + x, pl.ds(8, ly)]
            acc = None
            for k in range(1, 5):
                t = mp[par, 4 + x, pl.ds(8 + k, ly)] + mp[par, 4 + x, pl.ds(8 - k, ly)]
                if x + k < lx:
                    t = t + mp[par, 4 + x + k, pl.ds(8, ly)]
                if x - k >= 0:
                    t = t + mp[par, 4 + x - k, pl.ds(8, ly)]
                t = t + jnp.where(lane >= k, pltpu.roll(v, k, 1), 0.0)
                t = t + jnp.where(lane < lz - k, pltpu.roll(v, lz - k, 1), 0.0)
                t = taps[k - 1] * t
                acc = t if acc is None else acc + t
            nb[x] = keep * v - start * (inv[x] * acc) - back * basis[older, x]
            even = even + pre[x] * v * v
        return even

    def z_correction(par):
        h = jnp.where(lane % 8 < 4, zr[par, 0], zr[par, 1])
        acc = jnp.zeros((ly, lz), F32)
        place = lane % 8
        for k in range(1, 5):
            ahead = jnp.where((place >= 4) & (place - 4 < k), pltpu.roll(h, k, 1), 0.0)
            behind = jnp.where((place < 4) & (place >= 4 - k), pltpu.roll(h, lz - k, 1), 0.0)
            acc = acc + taps[k - 1] * (ahead + behind)
        return acc

    def outer_part(par, x, zc):
        z = pltpu.roll(zc, (2 * lz - 8 * x - 4) % lz, 1)
        acc = jnp.where((lane < 4) | (lane >= lz - 4), z, 0.0)
        for k in range(1, 5):
            if x - k < 0:
                acc = acc + taps[k - 1] * mp[par, 4 + x - k, pl.ds(8, ly)]
            if x + k >= lx:
                acc = acc + taps[k - 1] * mp[par, 4 + x + k, pl.ds(8, ly)]
        if x % 2 == 0:
            h = jnp.where(sub8 < 4, yr[par, 1, x // 2], yr[par, 0, x // 2])
        else:
            h = pltpu.roll(jnp.where(sub8 < 4, yr[par, 0, x // 2], yr[par, 1, x // 2]), 4, 0)
        low = jnp.zeros((8, lz), F32)
        high = jnp.zeros((8, lz), F32)
        for k in range(1, 5):
            low = low + taps[k - 1] * jnp.where(sub8 < k, pltpu.roll(h, k, 0), 0.0)
            high = high + taps[k - 1] * jnp.where(sub8 >= 8 - k, pltpu.roll(h, 8 - k, 0), 0.0)
        parts = [acc[:8] + low] + ([acc[8:-8]] if ly > 16 else []) + [acc[-8:] + high]
        return jnp.concatenate(parts, axis=0)

    def publish(par, x, m, packed, edges):
        mp[par, 4 + x, pl.ds(8, ly)] = m
        if x % 2 == 0:
            edges = (m[:8], m[-8:])
        else:
            yp[par, 0, x // 2] = jnp.where(sub8 < 4, pltpu.roll(m[-8:], 4, 0), edges[1])
            yp[par, 1, x // 2] = jnp.where(sub8 < 4, edges[0], pltpu.roll(m[:8], 4, 0))
        turned = pltpu.roll(m, (8 * x + 4) % lz, 1)
        return jnp.where((lane >= 8 * x) & (lane < 8 * x + 8), turned, packed), edges

    order = list(range(4)) + list(range(lx - 4, lx)) + list(range(4, lx - 4))

    hidden = dot(w1[...], feats[...])
    hidden = (hidden * sigmoid(hidden)).astype(BF16)
    hidden = dot(w2[...], hidden)
    hidden = (hidden * sigmoid(hidden)).astype(BF16)
    predicted = dot(w3[...], hidden)
    trace = (predicted[0:1] + predicted[1:2] + predicted[2:3]) / 3.0
    ex, ey, ez = lx // EL, ly // EL, lz // EL
    spread = jnp.where(
        lax.broadcasted_iota(jnp.int32, (lz, lz), 0) == lax.broadcasted_iota(jnp.int32, (lz, lz), 1) // EL,
        1.0,
        0.0,
    )
    lines = jnp.concatenate(
        [trace if e == 0 else pltpu.roll(trace, (lz - e * ez) % lz, 1) for e in range(ex * ey)], axis=0
    )
    forcing = dot(lines, spread, precision=lax.Precision.HIGHEST)
    pl.semaphore_wait(barrier, total)
    packed = jnp.zeros((ly, lz), F32)
    edges = None
    for n, x in enumerate(order):
        line = forcing[(x // EL) * ey : (x // EL) * ey + ey]
        block = jnp.concatenate([jnp.broadcast_to(line[j : j + 1], (EL, lz)) for j in range(ey)], axis=0)
        whole = diag[x] + center
        scale = 1.0 / whole
        pre[x] = whole
        inv[x] = scale * (2.0 / half)
        first_vector = (right[x] + block) * scale
        basis[0, x] = first_vector
        packed, edges = publish(0, x, first_vector, packed, edges)
        if n == 7:
            halo_start(0, "gx")
    zp[0] = packed
    halo_start(0, "ga", "gz")
    grads[...] = jnp.zeros_like(grads)
    small[...] = jnp.zeros_like(small)
    count_samples()

    def iteration(i, carry):
        par = lax.rem(i, 2)
        later = 1 - par
        start = jnp.where(i == 0, 0.5, 1.0)
        back = jnp.where(i == 0, 0.0, 1.0)
        keep = start * (2.0 / half - 2.0)
        even = stencil_local(par, keep, start, back, jnp.maximum(i - 1, 0))
        eta[2 * i] = jnp.sum(even.reshape(ly // 8, 8, lz), axis=0)
        gradient_work(i)
        halo_wait(par)
        zc = z_correction(par)
        more = i < ITERS - 1
        packed = jnp.zeros((ly, lz), F32)
        odd = jnp.zeros((ly, lz), F32)
        edges = None
        for n, x in enumerate(order):
            m = nb[x] - start * (inv[x] * outer_part(par, x, zc))
            basis[i + 1, x] = m
            odd = odd + pre[x] * mp[par, 4 + x, pl.ds(8, ly)] * m
            packed, edges = publish(later, x, m, packed, edges)
            if n == 7:
                pl.when(more)(lambda: halo_start(later, "gx"))
        zp[later] = packed
        pl.when(more)(lambda: halo_start(later, "ga", "gz"))
        eta[2 * i + 1] = jnp.sum(odd.reshape(ly // 8, 8, lz), axis=0)
        halo_sent(par)
        return carry

    lax.fori_loop(0, ITERS, iteration, 0)

    count = 2 * ITERS
    lanes = jnp.sum(eta[...], axis=1)
    coarse = jnp.max(jnp.abs(lanes), axis=1, keepdims=True) * (2.0 * lz)
    upper = (lanes + coarse) - coarse
    mine = lax.broadcasted_iota(jnp.int32, (count, lz), 0) == lax.broadcasted_iota(jnp.int32, (count, lz), 1)
    row = packed_pair(
        [
            jnp.sum(jnp.where(mine, jnp.sum(v, axis=1, keepdims=True), 0.0), axis=0, keepdims=True)
            for v in (upper, lanes - upper)
        ]
    )
    sum_start(0, row)
    for phase in range(1, len(phases)):
        sum_start(phase, packed_pair(sum_wait(phase - 1)))
    sums = sum_wait(len(phases) - 1)
    gradient_stage(6)
    sums = tuple(
        jnp.broadcast_to(jnp.sum(jnp.where(mine, v, 0.0), axis=1, keepdims=True), (count, lz)) for v in sums
    )
    in_x, in_r = krylov_coefficients(sums)
    along_x = [jnp.broadcast_to(in_x[j : j + 1], (ly, lz)) for j in range(ITERS)]
    along_r = [jnp.broadcast_to(in_r[j : j + 1], (ly, lz)) for j in range(ITERS + 1)]
    for x in range(lx):
        p = along_x[0] * basis[0, x]
        r = along_r[0] * basis[0, x]
        for j in range(1, ITERS):
            v = basis[j, x]
            p = p + along_x[j] * v
            r = r + along_r[j] * v
        press[x] = p
        resid[x] = pre[x] * (r + along_r[ITERS] * basis[ITERS, x])
    gradient_stage(7)
    total_grads[: 2 * ch] = full[...]
    total_grads[2 * ch :] = jnp.sum(small_third[...], axis=0)
    sums_sent()


def pressure_solve(right_side, diagonal, feats, bank, target, index, w1, w2, w3):
    sizes = {a: lax.axis_size(a) for a in AXES}
    lx, ly, lz = right_side.shape
    ch, columns = bank.shape
    slots = 0
    phases = phases_of(sizes)
    for axes in phases:
        n = 1
        for a in axes:
            n *= sizes[a]
        slots += n
    nx, nz, na = (sizes[a] for a in ("gx", "gz", "ga"))
    rows = w1.shape[0] + w2.shape[0]
    few = (w3.shape[0] + 7) // 8 * 8
    pair = 2 if nz % 2 == 0 else 1
    nh = nz // pair
    share = rows // nz
    piece = share // na
    tiles = columns // TILE
    copies = 3 + 3 * (nh - 1) + 3 * (na - 1) + 2 * (nx - 1)
    field = pltpu.VMEM((lx, ly, lz), F32)
    vmem = pl.BlockSpec(memory_space=pltpu.VMEM)
    return pl.pallas_call(
        functools.partial(solve_kernel, sizes),
        out_shape=[pltpu.VMEM((lx, ly, lz), F32)] * 2 + [pltpu.VMEM((rows + few, ch), F32)],
        in_specs=[vmem] * 3 + [pl.BlockSpec(memory_space=pl.ANY)] + [vmem] * 5,
        out_specs=[vmem] * 3,
        scratch_shapes=[
            pltpu.VMEM((2, lx + 8, ly + 16, lz), F32),
            field,
            pltpu.VMEM((ITERS + 1, lx, ly, lz), F32),
            field, field,
            pltpu.VMEM((2, 2, lx // 2, 8, lz), F32),
            pltpu.VMEM((2, 2, lx // 2, 8, lz), F32),
            pltpu.VMEM((2, ly, lz), F32),
            pltpu.VMEM((2, 2, ly, lz), F32),
            pltpu.VMEM((2 * ITERS, 8, lz), F32),
            pltpu.VMEM((len(phases), 1, lz), F32),
            pltpu.VMEM((slots, 1, lz), F32),
            pltpu.VMEM((tiles, ch, TILE), BF16),
            pltpu.VMEM((columns // 128, 128), F32),
            pltpu.VMEM((rows, ch), F32),
            pltpu.VMEM((rows // pair, ch), F32),
            pltpu.VMEM((rows // pair, ch), F32),
            pltpu.VMEM((max(nh - 1, 1), share, ch), F32),
            pltpu.VMEM((share, ch), F32),
            pltpu.VMEM((max(na - 1, 1), piece, ch), F32),
            pltpu.VMEM((piece, ch), F32),
            pltpu.VMEM((nx, piece, ch), F32),
            pltpu.VMEM((rows, ch), F32),
            pltpu.VMEM((4, few, ch), F32),
            pltpu.VMEM((nh + na - 1, few, ch), F32),
            pltpu.VMEM((nx, few, ch), F32),
            pltpu.SemaphoreType.DMA((tiles,)),
            pltpu.SemaphoreType.DMA((copies,)),
            pltpu.SemaphoreType.DMA((copies,)),
            pltpu.SemaphoreType.DMA((2, 6)),
            pltpu.SemaphoreType.DMA((2, 6)),
            pltpu.SemaphoreType.DMA((slots,)),
            pltpu.SemaphoreType.DMA((slots,)),
        ],
        compiler_params=pltpu.CompilerParams(collective_id=0, has_side_effects=True),
        cost_estimate=pl.CostEstimate(
            flops=60_000_000, bytes_accessed=200_000_000, transcendentals=0
        ),
    )(right_side, diagonal, feats, bank, target, index.reshape(1, -1), w1, w2, w3)


def finish_kernel(press_in, resid_in, grads, press, resid, step1, step2, step3):
    press[...] = press_in[...]
    resid[...] = resid_in[...]
    ch = step1.shape[0]
    start = 0
    for out in (step1, step2, step3):
        count = out.shape[0]
        value = grads[start : start + count]
        squares = jnp.sum(jnp.sum(value * value, axis=0, keepdims=True), axis=1, keepdims=True)
        out[...] = value * lax.rsqrt(squares / (count * ch) + epsilon)
        start += count


def finish(press, resid, grads, weights):
    vmem = pl.BlockSpec(memory_space=pltpu.VMEM)
    return pl.pallas_call(
        finish_kernel,
        out_shape=[jax.ShapeDtypeStruct(press.shape, F32)] * 2
        + [jax.ShapeDtypeStruct(w.shape, F32) for w in weights],
        in_specs=[vmem] * 3,
        out_specs=[vmem] * 5,
        cost_estimate=pl.CostEstimate(flops=1_000_000, bytes_accessed=2_000_000, transcendentals=0),
    )(*(pltpu.with_memory_space_constraint(v, pltpu.VMEM) for v in (press, resid, grads)))


def body(
    right_side, diagonal, element_features, sample_bank, target_bank, patch_index, w_first, w_second, w_third
):
    weights = (w_first, w_second, w_third)
    solved = pressure_solve(
        right_side, diagonal, element_features, sample_bank, target_bank, patch_index, *weights
    )
    return tuple(finish(*solved, weights))


def solution(mesh):
    return jax.shard_map(
        body,
        mesh=mesh,
        in_specs=(
            P("gx", "ga", "gz"),
            P("gx", "ga", "gz"),
            P(None, ("gx", "gz", "ga")),
            P(None, ("gx", "gz", "ga")),
            P(None, ("gx", "gz", "ga")),
            P(("gx", "gz", "ga")),
            P(),
            P(),
            P(),
        ),
        out_specs=(P("gx", "ga", "gz"), P("gx", "ga", "gz"), P(), P(), P()),
        check_vma=False,
    )
```

```python
import functools

import jax
import jax.numpy as jnp
from jax import lax
from jax.experimental import pallas as pl
from jax.experimental.pallas import tpu as pltpu
from jax.sharding import PartitionSpec as P

EL = 8
ITERS = 12
TILE = 1024
AXES = ("gx", "gz", "ga")
ONE_PHASE = 64
STAGE_STEPS = (1, 2, 4, 6, 7, 8)

taps = (1.6, -0.2, 8.0 / 315.0, -1.0 / 560.0)
center = 3.0 * 205.0 / 72.0
epsilon = 1e-06
half = 1.1
MESH = pl.DeviceIdType.MESH
F32 = jnp.float32
BF16 = jnp.bfloat16


def dot(a, b, dims=((1,), (0,)), precision=None):
    return lax.dot_general(a, b, (dims, ((), ())), preferred_element_type=F32, precision=precision)


def sigmoid(v):
    return 1.0 / (1.0 + jnp.exp(-v))


def phases_of(sizes):
    total = 1
    for a in AXES:
        total *= sizes[a]
    return (AXES,) if total <= ONE_PHASE else (("gx",), ("gz", "ga"))


def shift_offsets(sizes):
    combos = [()]
    for n in sizes:
        combos = [c + (k,) for c in combos for k in range(n)]
    return combos[1:]


def renormalized(s, e):
    r = s + e
    return r, e - (r - s)


def two_sum(a, b):
    s = a + b
    t = s - a
    return s, (a - (s - t)) + (b - t)


def pair_add(a, b):
    s, e = two_sum(a[0], b[0])
    return renormalized(s, e + (a[1] + b[1]))


def pair_scale(a, c):
    return a[0] * c, a[1] * c


def halves(v):
    t = v * 4097.0
    high = t - (t - v)
    return high, v - high


def product(a, b, parts):
    p = a * b
    (ah, al), (bh, bl) = parts, halves(b)
    return p, ((ah * bh - p) + ah * bl + al * bh) + al * bl


def pair_div(a, b, inverse):
    q = a[0] * inverse
    p, e = product(q, b[0], halves(q))
    return renormalized(q, (((a[0] - p) - e) + (a[1] - q * b[1])) * inverse)


def krylov_coefficients(eta):
    count, lanes = eta[0].shape
    n = count // 2
    size = (n + 2 + 7) // 8 * 8
    row = lax.broadcasted_iota(jnp.int32, (count, lanes), 0)
    place = lax.broadcasted_iota(jnp.int32, (size, lanes), 0)

    def at(v, j):
        return tuple(jnp.broadcast_to(part[j : j + 1], (1, lanes)) for part in v)

    def wide(v):
        return tuple(jnp.broadcast_to(part, (count, lanes)) for part in v)

    def plus_product(a, c, v):
        c0, c1 = wide(c)
        p, e = product(c0, v[0], wide(halves(c[0])))
        value, error = two_sum(a[0], p)
        return renormalized(value, error + (a[1] + (e + (c0 * v[1] + c1 * v[0]))))

    low = tuple(jnp.where(row % 2 == 0, e, o) for e, o in zip(wide(at(eta, 0)), wide(at(eta, 1))))
    moments = pair_add(pair_scale(eta, 2.0), pair_scale(low, -1.0))
    rho = tuple(jnp.where(row < 2, e, m) for e, m in zip(eta, moments))
    pi = rho
    r = jnp.where(place == 0, 1.0, 0.0)
    p, x = r, jnp.zeros_like(r)
    for k in range(n):
        above = tuple(pltpu.roll(v, count - 1, 0) for v in pi)
        below = tuple(pltpu.roll(v, 1, 0) for v in pi)
        if k < 2:
            below = tuple(jnp.where(row == 0, u, v) for u, v in zip(above, below))
        near, rest = two_sum(above[0], below[0])
        value, error = two_sum(pi[0], 0.5 * near)
        tau = value, error + (pi[1] + 0.5 * (rest + (above[1] + below[1])))
        pivot = at(tau, k)
        inverse = 1.0 / pivot[0]
        alpha = pair_div(at(rho, k), pivot, inverse)
        step = jnp.broadcast_to(alpha[0], (size, lanes))
        x = x + step * p
        ahead = jnp.where(place < size - 1, pltpu.roll(p, size - 1, 0), 0.0)
        r = r - step * (p + 0.5 * (ahead + pltpu.roll(jnp.where(place == 0, 2.0 * p, p), 1, 0)))
        if k + 1 < n:
            new = plus_product(rho, pair_scale(alpha, -1.0), tau)
            beta = pair_scale(pair_div(at(new, k + 1), pivot, inverse), -1.0 if k == 0 else -0.5)
            p = r + jnp.broadcast_to(beta[0], (size, lanes)) * p
            pi = plus_product(new, beta, pi)
            rho = new
    return x * (1.0 / half), r


def solve_kernel(
    sizes, right_in, diag_in, feats_in, bank, target_in, index_in, w1_in, w2_in, w3_in, press, resid, total_grads,
    right, diag, feats, target, index, w1, w2, w3, in_sem,
    mp, nb, basis, pre, inv, yp, yr, zp, zr, eta, ar_src, ar_dst,
    bank_v, counts, grads, swapped, halved, first, held, second, owned, third, full,
    small, small_in, small_third,
    bank_sem, g_send, g_recv, h_send, h_recv, a_send, a_recv,
):
    given = ((feats_in, feats), (w1_in, w1), (w2_in, w2), (w3_in, w3), (diag_in, diag), (right_in, right),
             (index_in, index), (target_in, target))
    given = [pltpu.make_async_copy(src, dst, in_sem.at[n]) for n, (src, dst) in enumerate(given)]
    for copy in given:
        copy.start()

    lx, ly, lz = right.shape
    ch, columns = bank.shape
    stress = target.shape[0]
    tiles = columns // TILE
    pos = {a: lax.axis_index(a) for a in AXES}
    phases = phases_of(sizes)

    def tile_copy(t):
        return pltpu.make_async_copy(
            bank.at[:, pl.ds(t * TILE, TILE)], bank_v.at[t], bank_sem.at[t]
        )

    for t in range(tiles):
        tile_copy(t).start()

    def coords(axes, offs, sign):
        out = {}
        for a, k in zip(axes, offs):
            n = sizes[a]
            c = pos[a] + (k if sign > 0 else n - k) if k else pos[a]
            out[a] = lax.rem(c, n) if k else c
        return out

    def flat(axes, at):
        value = 0
        for a in axes:
            value = value * sizes[a] + at[a]
        return value

    groups = []
    for axes in phases:
        me = flat(axes, pos)
        peers = []
        for offs in shift_offsets([sizes[a] for a in axes]):
            to = {**pos, **coords(axes, offs, 1)}
            source = flat(axes, coords(axes, offs, -1))
            far = sum(min(k, sizes[a] - k) for a, k in zip(axes, offs))
            peers.append((far, to, source))
        peers = [(to, source) for far, to, source in sorted(peers, key=lambda peer: -peer[0])]
        groups.append((me, peers))

    nx, nz, na = sizes["gx"], sizes["gz"], sizes["ga"]
    pair = 2 if nz % 2 == 0 else 1
    nh = nz // pair
    side, spot = lax.rem(pos["gz"], pair), lax.div(pos["gz"], pair)
    half_rows = grads.shape[0] // pair
    share = half_rows // nh
    piece = share // na

    def half_of(b):
        return pl.ds(pl.multiple_of(b * half_rows, 8), half_rows)

    def share_of(h):
        return pl.ds(pl.multiple_of(h * share, 8), share)

    def block_of(h, ia=None):
        start = side * half_rows + h * share
        if ia is None:
            return pl.ds(pl.multiple_of(start, 8), share)
        return pl.ds(pl.multiple_of(start + ia * piece, 8), piece)

    def along(axis, k, sign):
        return coords((axis,), (k,), sign)[axis]

    def spot_along(k, sign):
        return lax.rem(spot + (k if sign > 0 else nh - k), nh)

    numbers = {}

    def gradient_copy(kind, k, src, dst, to):
        number = numbers.setdefault((kind, k), len(numbers))
        return pltpu.make_async_remote_copy(
            src_ref=src,
            dst_ref=dst,
            send_sem=g_send.at[number],
            recv_sem=g_recv.at[number],
            device_id={**pos, **to},
            device_id_type=MESH,
        )

    def to_pair():
        return {"gz": spot * pair + (pair - 1 - side)}

    def to_spot(k):
        return {"gz": spot_along(k, 1) * pair + side}

    def swap_pair():
        other = half_of(pair - 1 - side)
        return [
            gradient_copy("swap", 0, grads.at[other], swapped, to_pair()),
            gradient_copy("swap", 1, small.at[0], small_in.at[0], to_pair()),
        ]

    def scatter_gz(k):
        return [
            gradient_copy("gz", k, halved.at[share_of(spot_along(k, 1))], first.at[k - 1], to_spot(k)),
            gradient_copy("small gz", k, small.at[1], small_in.at[k], to_spot(k)),
        ]

    def scatter_ga(k):
        rows = pl.ds(pl.multiple_of(along("ga", k, 1) * piece, 8), piece)
        to = {"ga": along("ga", k, 1)}
        return [
            gradient_copy("ga", k, held.at[rows], second.at[k - 1], to),
            gradient_copy("small ga", k, small.at[2], small_in.at[nh + k - 1], to),
        ]

    def add_gx(k, sign=1):
        slot = pos["gx"] if sign > 0 else along("gx", k, -1)
        to = {"gx": along("gx", k, 1)}
        return [
            gradient_copy("gx", k, owned, third.at[slot], to),
            gradient_copy("small gx", k, small.at[3], small_third.at[slot], to),
        ]

    def gather_ga(k, sign=1):
        at = pos["ga"] if sign > 0 else along("ga", k, -1)
        rows = block_of(spot, at)
        return [gradient_copy("all ga", k, full.at[rows], full.at[rows], {"ga": along("ga", k, 1)})]

    def gather_gz(k, sign=1):
        rows = block_of(spot if sign > 0 else spot_along(k, -1))
        return [gradient_copy("all gz", k, full.at[rows], full.at[rows], to_spot(k))]

    def gather_pair(sign=1):
        rows = half_of(side if sign > 0 else pair - 1 - side)
        return [gradient_copy("all pair", 0, full.at[rows], full.at[rows], to_pair())]

    def start(copies):
        for copy in copies:
            copy.start()

    def arrived(copies):
        for copy in copies:
            copy.wait_recv()

    def sent(copies):
        for copy in copies:
            copy.wait_send()

    def gradient_stage(stage):
        if stage == 0:
            if pair > 1:
                start(swap_pair())
        elif stage == 1:
            total, few = grads[half_of(side), :], small[0]
            if pair > 1:
                arrived(swap_pair())
                total, few = total + swapped[...], few + small_in[0]
            halved[...] = total
            small[1] = few
            for k in range(1, nh):
                start(scatter_gz(k))
        elif stage == 2:
            total, few = halved[share_of(spot), :], small[1]
            for k in range(1, nh):
                arrived(scatter_gz(k))
                total, few = total + first[k - 1], few + small_in[k]
            held[...] = total
            small[2] = few
            for k in range(1, na):
                start(scatter_ga(k))
        elif stage == 3:
            total, few = held[pl.ds(pl.multiple_of(pos["ga"] * piece, 8), piece), :], small[2]
            for k in range(1, na):
                arrived(scatter_ga(k))
                total, few = total + second[k - 1], few + small_in[nh + k - 1]
            owned[...] = total
            third[pos["gx"]] = total
            small[3] = few
            small_third[pos["gx"]] = few
            for k in range(1, nx):
                start(add_gx(k))
        elif stage == 4:
            for k in range(1, nx):
                arrived(add_gx(k, -1))
            full[block_of(spot, pos["ga"]), :] = jnp.sum(third[...], axis=0)
            for k in range(1, na):
                start(gather_ga(k))
        elif stage == 5:
            for k in range(1, na):
                arrived(gather_ga(k, -1))
            for k in range(1, nh):
                start(gather_gz(k))
        elif stage == 6:
            for k in range(1, nh):
                arrived(gather_gz(k, -1))
            if pair > 1:
                start(gather_pair())
        else:
            if pair > 1:
                arrived(gather_pair(-1))
                sent(swap_pair() + gather_pair())
            for k in range(1, nh):
                sent(scatter_gz(k) + gather_gz(k))
            for k in range(1, na):
                sent(scatter_ga(k) + gather_ga(k))
            for k in range(1, nx):
                sent(add_gx(k))

    def count_samples():
        samples = index.shape[1]
        ids = index[...]
        high = lax.broadcasted_iota(jnp.int32, (columns // 128, samples), 0) == (ids // 128)
        low = lax.broadcasted_iota(jnp.int32, (128, samples), 0) == (ids % 128)
        counts[...] = dot(
            jnp.where(high, 1.0, 0.0).astype(BF16),
            jnp.where(low, 1.0, 0.0).astype(BF16),
            ((1,), (1,)),
        )

    def gradient_tile(t):
        rows = TILE // 128
        tile_copy(t).wait()
        weight = jnp.concatenate([counts[pl.ds(t * rows + j, 1), :] for j in range(rows)], axis=1)
        x = bank_v[t]
        a1, a2, a3 = w1[...], w2[...], w3[...]
        l1 = dot(a1, x)
        s1 = sigmoid(l1)
        h1 = (l1 * s1).astype(BF16)
        l2 = dot(a2, h1)
        s2 = sigmoid(l2)
        h2 = (l2 * s2).astype(BF16)
        goal = target[:, pl.ds(pl.multiple_of(t * TILE, TILE), TILE)]
        error = (dot(a3, h2) - goal.astype(F32)).astype(BF16)

        def weighted(delta, right):
            scaled = delta.astype(F32) * weight
            upper = scaled.astype(BF16)
            lower = (scaled - upper.astype(F32)).astype(BF16)
            return dot(upper, right, ((1,), (1,))) + dot(lower, right, ((1,), (1,)))

        small[0, :stress] += weighted(error, h2)
        d2 = (dot(a3, error, ((0,), (0,))) * (s2 * (1.0 + l2 * (1.0 - s2)))).astype(BF16)
        grads[ch : 2 * ch] += weighted(d2, h1)
        d1 = (dot(a2, d2, ((0,), (0,))) * (s1 * (1.0 + l1 * (1.0 - s1)))).astype(BF16)
        grads[:ch] += weighted(d1, x)

    def gradient_work(i):
        pl.when(i < tiles)(lambda: gradient_tile(i))
        for stage, step in enumerate(STAGE_STEPS):
            pl.when(i == tiles - 1 + step)(lambda stage=stage: gradient_stage(stage))

    mp[...] = jnp.zeros_like(mp)
    yr[...] = jnp.zeros_like(yr)
    zr[...] = jnp.zeros_like(zr)

    barrier = pltpu.get_barrier_semaphore()
    total = 0
    for _, peers in groups:
        for to, _ in peers:
            pl.semaphore_signal(barrier, inc=1, device_id=to, device_id_type=MESH)
            total += 1

    lane = lax.broadcasted_iota(jnp.int32, (ly, lz), 1)
    sub8 = lax.broadcasted_iota(jnp.int32, (8, lz), 0)

    def halo_copies(par):
        out = {}

        def add(axis, step, number, src, dst):
            copy = pltpu.make_async_remote_copy(
                src_ref=src,
                dst_ref=dst,
                send_sem=h_send.at[par, number],
                recv_sem=h_recv.at[par, number],
                device_id={**pos, axis: jnp.clip(pos[axis] + step, 0, sizes[axis] - 1)},
                device_id_type=MESH,
            )
            can_send = pos[axis] < sizes[axis] - 1 if step > 0 else pos[axis] > 0
            will_get = pos[axis] > 0 if step > 0 else pos[axis] < sizes[axis] - 1
            out.setdefault(axis, []).append((copy, can_send, will_get))

        rows = pl.ds(8, ly)
        if sizes["gx"] > 1:
            add("gx", 1, 0, mp.at[par, pl.ds(lx, 4), rows], mp.at[par, pl.ds(0, 4), rows])
            add("gx", -1, 1, mp.at[par, pl.ds(4, 4), rows], mp.at[par, pl.ds(lx + 4, 4), rows])
        if sizes["ga"] > 1:
            add("ga", 1, 2, yp.at[par, 0], yr.at[par, 0])
            add("ga", -1, 3, yp.at[par, 1], yr.at[par, 1])
        if sizes["gz"] > 1:
            add("gz", 1, 4, zp.at[par], zr.at[par, 0])
            add("gz", -1, 5, zp.at[par], zr.at[par, 1])
        return out

    def halo_start(par, *axes):
        copies = halo_copies(par)
        for axis in axes:
            for copy, can_send, _ in copies.get(axis, []):
                pl.when(can_send)(copy.start)

    def halo_wait(par, *axes):
        copies = halo_copies(par)
        for axis in axes:
            for copy, _, will_get in copies.get(axis, []):
                pl.when(will_get)(copy.wait_recv)

    def halo_sent(par):
        for copies in halo_copies(par).values():
            for copy, can_send, _ in copies:
                pl.when(can_send)(copy.wait_send)

    bases = []
    base = 0
    for axes in phases:
        bases.append(base)
        n = 1
        for a in axes:
            n *= sizes[a]
        base += n

    def sum_copies(phase):
        me, peers = groups[phase]
        out = []
        for k, (to, source) in enumerate(peers):
            slot = bases[phase]
            send = pltpu.make_async_remote_copy(
                src_ref=ar_src.at[phase],
                dst_ref=ar_dst.at[slot + me],
                send_sem=a_send.at[slot + k],
                recv_sem=a_recv.at[slot + me],
                device_id=to,
                device_id_type=MESH,
            )
            receive = pltpu.make_async_remote_copy(
                src_ref=ar_src.at[phase],
                dst_ref=ar_dst.at[slot + source],
                send_sem=a_send.at[slot + k],
                recv_sem=a_recv.at[slot + source],
                device_id=to,
                device_id_type=MESH,
            )
            out.append((send, receive))
        return out

    def sum_start(phase, row):
        ar_src[phase] = row
        ar_dst[bases[phase] + groups[phase][0]] = row
        for send, _ in sum_copies(phase):
            send.start()

    def sum_wait(phase):
        count = len(groups[phase][1]) + 1
        for _, receive in sum_copies(phase):
            receive.wait_recv()
        parts = [ar_dst[bases[phase] + j] for j in range(count)]
        parts = [(v, jnp.zeros_like(v)) for v in parts]
        while len(parts) > 1:
            joined = [pair_add(a, b) for a, b in zip(parts[::2], parts[1::2])]
            parts = joined + parts[2 * len(joined) :]
        return pair_add(parts[0], tuple(pltpu.roll(v, lz // 2, 1) for v in parts[0]))

    def packed_pair(v):
        first_half = lax.broadcasted_iota(jnp.int32, (1, lz), 1) < lz // 2
        return jnp.where(first_half, v[0], pltpu.roll(v[1], lz // 2, 1))

    def sums_sent():
        for phase in range(len(phases)):
            for send, _ in sum_copies(phase):
                send.wait_send()

    def stencil_local(par, keep, start, back, older):
        even = jnp.zeros((ly, lz), F32)
        for x in range(lx):
            v = mp[par, 4 + x, pl.ds(8, ly)]
            acc = None
            for k in range(1, 5):
                t = mp[par, 4 + x, pl.ds(8 + k, ly)] + mp[par, 4 + x, pl.ds(8 - k, ly)]
                if x + k < lx:
                    t = t + mp[par, 4 + x + k, pl.ds(8, ly)]
                if x - k >= 0:
                    t = t + mp[par, 4 + x - k, pl.ds(8, ly)]
                t = t + jnp.where(lane >= k, pltpu.roll(v, k, 1), 0.0)
                t = t + jnp.where(lane < lz - k, pltpu.roll(v, lz - k, 1), 0.0)
                t = taps[k - 1] * t
                acc = t if acc is None else acc + t
            nb[x] = keep * v - start * (inv[x] * acc) - back * basis[older, x]
            even = even + pre[x] * v * v
        return even

    def z_correction(par):
        h = jnp.where(lane % 8 < 4, zr[par, 0], zr[par, 1])
        acc = jnp.zeros((ly, lz), F32)
        place = lane % 8
        for k in range(1, 5):
            ahead = jnp.where((place >= 4) & (place - 4 < k), pltpu.roll(h, k, 1), 0.0)
            behind = jnp.where((place < 4) & (place >= 4 - k), pltpu.roll(h, lz - k, 1), 0.0)
            acc = acc + taps[k - 1] * (ahead + behind)
        return acc

    def side_part(par, x, zc):
        z = pltpu.roll(zc, (2 * lz - 8 * x - 4) % lz, 1)
        acc = jnp.where((lane < 4) | (lane >= lz - 4), z, 0.0)
        if x % 2 == 0:
            h = jnp.where(sub8 < 4, yr[par, 1, x // 2], yr[par, 0, x // 2])
        else:
            h = pltpu.roll(jnp.where(sub8 < 4, yr[par, 0, x // 2], yr[par, 1, x // 2]), 4, 0)
        low = jnp.zeros((8, lz), F32)
        high = jnp.zeros((8, lz), F32)
        for k in range(1, 5):
            low = low + taps[k - 1] * jnp.where(sub8 < k, pltpu.roll(h, k, 0), 0.0)
            high = high + taps[k - 1] * jnp.where(sub8 >= 8 - k, pltpu.roll(h, 8 - k, 0), 0.0)
        parts = [acc[:8] + low] + ([acc[8:-8]] if ly > 16 else []) + [acc[-8:] + high]
        return jnp.concatenate(parts, axis=0)

    def end_part(par, x):
        acc = None
        for k in range(1, 5):
            for at in (4 + x - k, 4 + x + k):
                if at < 4 or at >= lx + 4:
                    t = taps[k - 1] * mp[par, at, pl.ds(8, ly)]
                    acc = t if acc is None else acc + t
        return acc

    def publish(par, x, m, packed, edges):
        mp[par, 4 + x, pl.ds(8, ly)] = m
        if x % 2 == 0:
            edges = (m[:8], m[-8:])
        else:
            yp[par, 0, x // 2] = jnp.where(sub8 < 4, pltpu.roll(m[-8:], 4, 0), edges[1])
            yp[par, 1, x // 2] = jnp.where(sub8 < 4, edges[0], pltpu.roll(m[:8], 4, 0))
        turned = pltpu.roll(m, (8 * x + 4) % lz, 1)
        return jnp.where((lane >= 8 * x) & (lane < 8 * x + 8), turned, packed), edges

    ends = list(range(4)) + list(range(lx - 4, lx))
    inner = list(range(4, lx - 4))

    for copy in given[:4]:
        copy.wait()
    hidden = dot(w1[...], feats[...])
    hidden = (hidden * sigmoid(hidden)).astype(BF16)
    hidden = dot(w2[...], hidden)
    hidden = (hidden * sigmoid(hidden)).astype(BF16)
    predicted = dot(w3[...], hidden)
    trace = (predicted[0:1] + predicted[1:2] + predicted[2:3]) / 3.0
    ex, ey, ez = lx // EL, ly // EL, lz // EL
    spread = jnp.where(
        lax.broadcasted_iota(jnp.int32, (lz, lz), 0) == lax.broadcasted_iota(jnp.int32, (lz, lz), 1) // EL,
        1.0,
        0.0,
    )
    lines = jnp.concatenate(
        [trace if e == 0 else pltpu.roll(trace, (lz - e * ez) % lz, 1) for e in range(ex * ey)], axis=0
    )
    forcing = dot(lines, spread, precision=lax.Precision.HIGHEST)
    for copy in given[4:6]:
        copy.wait()
    pl.semaphore_wait(barrier, total)
    packed = jnp.zeros((ly, lz), F32)
    edges = None
    for n, x in enumerate(ends + inner):
        line = forcing[(x // EL) * ey : (x // EL) * ey + ey]
        block = jnp.concatenate([jnp.broadcast_to(line[j : j + 1], (EL, lz)) for j in range(ey)], axis=0)
        whole = diag[x] + center
        scale = 1.0 / whole
        pre[x] = whole
        inv[x] = scale * (2.0 / half)
        first_vector = (right[x] + block) * scale
        basis[0, x] = first_vector
        packed, edges = publish(0, x, first_vector, packed, edges)
        if n == 7:
            halo_start(0, "gx")
    zp[0] = packed
    halo_start(0, "ga", "gz")
    grads[...] = jnp.zeros_like(grads)
    small[...] = jnp.zeros_like(small)
    for copy in given[6:]:
        copy.wait()
    count_samples()

    def iteration(i, carry):
        par = lax.rem(i, 2)
        later = 1 - par
        start = jnp.where(i == 0, 0.5, 1.0)
        back = jnp.where(i == 0, 0.0, 1.0)
        keep = start * (2.0 / half - 2.0)
        even = stencil_local(par, keep, start, back, jnp.maximum(i - 1, 0))
        eta[2 * i] = jnp.sum(even.reshape(ly // 8, 8, lz), axis=0)
        gradient_work(i)
        halo_wait(par, "ga", "gz")
        zc = z_correction(par)
        more = i < ITERS - 1
        packed = jnp.zeros((ly, lz), F32)
        odd = jnp.zeros((ly, lz), F32)
        edges = None
        for x in ends:
            nb[x] = nb[x] - start * (inv[x] * side_part(par, x, zc))
        for x in inner:
            m = nb[x] - start * (inv[x] * side_part(par, x, zc))
            basis[i + 1, x] = m
            odd = odd + pre[x] * mp[par, 4 + x, pl.ds(8, ly)] * m
            packed, edges = publish(later, x, m, packed, edges)
        halo_wait(par, "gx")
        for x in ends:
            m = nb[x] - start * (inv[x] * end_part(par, x))
            basis[i + 1, x] = m
            odd = odd + pre[x] * mp[par, 4 + x, pl.ds(8, ly)] * m
            packed, edges = publish(later, x, m, packed, edges)
        pl.when(more)(lambda: halo_start(later, "gx"))
        zp[later] = packed
        pl.when(more)(lambda: halo_start(later, "ga", "gz"))
        eta[2 * i + 1] = jnp.sum(odd.reshape(ly // 8, 8, lz), axis=0)
        halo_sent(par)
        return carry

    lax.fori_loop(0, ITERS, iteration, 0)

    count = 2 * ITERS
    lanes = jnp.sum(eta[...], axis=1)
    coarse = jnp.max(jnp.abs(lanes), axis=1, keepdims=True) * (2.0 * lz)
    upper = (lanes + coarse) - coarse
    mine = lax.broadcasted_iota(jnp.int32, (count, lz), 0) == lax.broadcasted_iota(jnp.int32, (count, lz), 1)
    row = packed_pair(
        [
            jnp.sum(jnp.where(mine, jnp.sum(v, axis=1, keepdims=True), 0.0), axis=0, keepdims=True)
            for v in (upper, lanes - upper)
        ]
    )
    sum_start(0, row)
    for phase in range(1, len(phases)):
        sum_start(phase, packed_pair(sum_wait(phase - 1)))
    sums = sum_wait(len(phases) - 1)
    gradient_stage(6)
    sums = tuple(
        jnp.broadcast_to(jnp.sum(jnp.where(mine, v, 0.0), axis=1, keepdims=True), (count, lz)) for v in sums
    )
    in_x, in_r = krylov_coefficients(sums)
    along_x = [jnp.broadcast_to(in_x[j : j + 1], (ly, lz)) for j in range(ITERS)]
    along_r = [jnp.broadcast_to(in_r[j : j + 1], (ly, lz)) for j in range(ITERS + 1)]
    for x in range(lx):
        p = along_x[0] * basis[0, x]
        r = along_r[0] * basis[0, x]
        for j in range(1, ITERS):
            v = basis[j, x]
            p = p + along_x[j] * v
            r = r + along_r[j] * v
        press[x] = p
        resid[x] = pre[x] * (r + along_r[ITERS] * basis[ITERS, x])
    gradient_stage(7)
    total_grads[: 2 * ch] = full[...]
    total_grads[2 * ch :] = jnp.sum(small_third[...], axis=0)
    sums_sent()


def pressure_solve(right_side, diagonal, feats, bank, target, index, w1, w2, w3):
    sizes = {a: lax.axis_size(a) for a in AXES}
    lx, ly, lz = right_side.shape
    ch, columns = bank.shape
    slots = 0
    phases = phases_of(sizes)
    for axes in phases:
        n = 1
        for a in axes:
            n *= sizes[a]
        slots += n
    nx, nz, na = (sizes[a] for a in ("gx", "gz", "ga"))
    rows = w1.shape[0] + w2.shape[0]
    few = (w3.shape[0] + 7) // 8 * 8
    pair = 2 if nz % 2 == 0 else 1
    nh = nz // pair
    share = rows // nz
    piece = share // na
    tiles = columns // TILE
    copies = 3 + 3 * (nh - 1) + 3 * (na - 1) + 2 * (nx - 1)
    inputs = (right_side, diagonal, feats, bank, target, index.reshape(1, -1), w1, w2, w3)
    field = pltpu.VMEM((lx, ly, lz), F32)
    vmem = pl.BlockSpec(memory_space=pltpu.VMEM)
    return pl.pallas_call(
        functools.partial(solve_kernel, sizes),
        out_shape=[pltpu.VMEM((lx, ly, lz), F32)] * 2 + [pltpu.VMEM((rows + few, ch), F32)],
        in_specs=[pl.BlockSpec(memory_space=pl.ANY)] * 9,
        out_specs=[vmem] * 3,
        scratch_shapes=[pltpu.VMEM(v.shape, v.dtype) for v in inputs if v is not bank]
        + [
            pltpu.SemaphoreType.DMA((len(inputs) - 1,)),
            pltpu.VMEM((2, lx + 8, ly + 16, lz), F32),
            field,
            pltpu.VMEM((ITERS + 1, lx, ly, lz), F32),
            field, field,
            pltpu.VMEM((2, 2, lx // 2, 8, lz), F32),
            pltpu.VMEM((2, 2, lx // 2, 8, lz), F32),
            pltpu.VMEM((2, ly, lz), F32),
            pltpu.VMEM((2, 2, ly, lz), F32),
            pltpu.VMEM((2 * ITERS, 8, lz), F32),
            pltpu.VMEM((len(phases), 1, lz), F32),
            pltpu.VMEM((slots, 1, lz), F32),
            pltpu.VMEM((tiles, ch, TILE), BF16),
            pltpu.VMEM((columns // 128, 128), F32),
            pltpu.VMEM((rows, ch), F32),
            pltpu.VMEM((rows // pair, ch), F32),
            pltpu.VMEM((rows // pair, ch), F32),
            pltpu.VMEM((max(nh - 1, 1), share, ch), F32),
            pltpu.VMEM((share, ch), F32),
            pltpu.VMEM((max(na - 1, 1), piece, ch), F32),
            pltpu.VMEM((piece, ch), F32),
            pltpu.VMEM((nx, piece, ch), F32),
            pltpu.VMEM((rows, ch), F32),
            pltpu.VMEM((4, few, ch), F32),
            pltpu.VMEM((nh + na - 1, few, ch), F32),
            pltpu.VMEM((nx, few, ch), F32),
            pltpu.SemaphoreType.DMA((tiles,)),
            pltpu.SemaphoreType.DMA((copies,)),
            pltpu.SemaphoreType.DMA((copies,)),
            pltpu.SemaphoreType.DMA((2, 6)),
            pltpu.SemaphoreType.DMA((2, 6)),
            pltpu.SemaphoreType.DMA((slots,)),
            pltpu.SemaphoreType.DMA((slots,)),
        ],
        compiler_params=pltpu.CompilerParams(collective_id=0, has_side_effects=True),
        cost_estimate=pl.CostEstimate(
            flops=60_000_000, bytes_accessed=200_000_000, transcendentals=0
        ),
    )(*inputs)


def finish_kernel(press_in, resid_in, grads, press, resid, step1, step2, step3):
    press[...] = press_in[...]
    resid[...] = resid_in[...]
    ch = step1.shape[0]
    start = 0
    for out in (step1, step2, step3):
        count = out.shape[0]
        value = grads[start : start + count]
        squares = jnp.sum(jnp.sum(value * value, axis=0, keepdims=True), axis=1, keepdims=True)
        out[...] = value * lax.rsqrt(squares / (count * ch) + epsilon)
        start += count


def finish(press, resid, grads, weights):
    vmem = pl.BlockSpec(memory_space=pltpu.VMEM)
    return pl.pallas_call(
        finish_kernel,
        out_shape=[jax.ShapeDtypeStruct(press.shape, F32)] * 2
        + [jax.ShapeDtypeStruct(w.shape, F32) for w in weights],
        in_specs=[vmem] * 3,
        out_specs=[vmem] * 5,
        cost_estimate=pl.CostEstimate(flops=1_000_000, bytes_accessed=2_000_000, transcendentals=0),
    )(*(pltpu.with_memory_space_constraint(v, pltpu.VMEM) for v in (press, resid, grads)))


def body(
    right_side, diagonal, element_features, sample_bank, target_bank, patch_index, w_first, w_second, w_third
):
    weights = (w_first, w_second, w_third)
    solved = pressure_solve(
        right_side, diagonal, element_features, sample_bank, target_bank, patch_index, *weights
    )
    return tuple(finish(*solved, weights))


def solution(mesh):
    return jax.shard_map(
        body,
        mesh=mesh,
        in_specs=(
            P("gx", "ga", "gz"),
            P("gx", "ga", "gz"),
            P(None, ("gx", "gz", "ga")),
            P(None, ("gx", "gz", "ga")),
            P(None, ("gx", "gz", "ga")),
            P(("gx", "gz", "ga")),
            P(),
            P(),
            P(),
        ),
        out_specs=(P("gx", "ga", "gz"), P("gx", "ga", "gz"), P(), P(), P()),
        check_vma=False,
    )
```

```python
import functools

import jax
import jax.numpy as jnp
from jax import lax
from jax.experimental import pallas as pl
from jax.experimental.pallas import tpu as pltpu
from jax.sharding import PartitionSpec as P

EL = 8
ITERS = 12
TILE = 1024
AXES = ("gx", "gz", "ga")
ONE_PHASE = 64
STAGE_STEPS = ((1, 1), (2, 3), (3, 4), (4, 5), (5, 6), (6, 7), (7, 8))

taps = (1.6, -0.2, 8.0 / 315.0, -1.0 / 560.0)
center = 3.0 * 205.0 / 72.0
epsilon = 1e-06
half = 1.1
MESH = pl.DeviceIdType.MESH
F32 = jnp.float32
BF16 = jnp.bfloat16


def dot(a, b, dims=((1,), (0,)), precision=None):
    return lax.dot_general(a, b, (dims, ((), ())), preferred_element_type=F32, precision=precision)


def sigmoid(v):
    return 1.0 / (1.0 + jnp.exp(-v))


def phases_of(sizes):
    total = 1
    for a in AXES:
        total *= sizes[a]
    return (AXES,) if total <= ONE_PHASE else (("gx",), ("gz", "ga"))


def shift_offsets(sizes):
    combos = [()]
    for n in sizes:
        combos = [c + (k,) for c in combos for k in range(n)]
    return combos[1:]


def renormalized(s, e):
    r = s + e
    return r, e - (r - s)


def two_sum(a, b):
    s = a + b
    t = s - a
    return s, (a - (s - t)) + (b - t)


def pair_add(a, b):
    s, e = two_sum(a[0], b[0])
    return renormalized(s, e + (a[1] + b[1]))


def pair_scale(a, c):
    return a[0] * c, a[1] * c


def halves(v):
    t = v * 4097.0
    high = t - (t - v)
    return high, v - high


def product(a, b, parts):
    p = a * b
    (ah, al), (bh, bl) = parts, halves(b)
    return p, ((ah * bh - p) + ah * bl + al * bh) + al * bl


def pair_div(a, b, inverse):
    q = a[0] * inverse
    p, e = product(q, b[0], halves(q))
    return renormalized(q, (((a[0] - p) - e) + (a[1] - q * b[1])) * inverse)


def krylov_coefficients(eta):
    count, lanes = eta[0].shape
    n = count // 2
    size = (n + 2 + 7) // 8 * 8
    row = lax.broadcasted_iota(jnp.int32, (count, lanes), 0)
    place = lax.broadcasted_iota(jnp.int32, (size, lanes), 0)

    def at(v, j):
        return tuple(jnp.broadcast_to(part[j : j + 1], (1, lanes)) for part in v)

    def wide(v):
        return tuple(jnp.broadcast_to(part, (count, lanes)) for part in v)

    def plus_product(a, c, v):
        c0, c1 = wide(c)
        p, e = product(c0, v[0], wide(halves(c[0])))
        value, error = two_sum(a[0], p)
        return renormalized(value, error + (a[1] + (e + (c0 * v[1] + c1 * v[0]))))

    low = tuple(jnp.where(row % 2 == 0, e, o) for e, o in zip(wide(at(eta, 0)), wide(at(eta, 1))))
    moments = pair_add(pair_scale(eta, 2.0), pair_scale(low, -1.0))
    rho = tuple(jnp.where(row < 2, e, m) for e, m in zip(eta, moments))
    pi = rho
    r = jnp.where(place == 0, 1.0, 0.0)
    p, x = r, jnp.zeros_like(r)
    for k in range(n):
        above = tuple(pltpu.roll(v, count - 1, 0) for v in pi)
        below = tuple(pltpu.roll(v, 1, 0) for v in pi)
        if k < 2:
            below = tuple(jnp.where(row == 0, u, v) for u, v in zip(above, below))
        near, rest = two_sum(above[0], below[0])
        value, error = two_sum(pi[0], 0.5 * near)
        tau = value, error + (pi[1] + 0.5 * (rest + (above[1] + below[1])))
        pivot = at(tau, k)
        inverse = 1.0 / pivot[0]
        alpha = pair_div(at(rho, k), pivot, inverse)
        step = jnp.broadcast_to(alpha[0], (size, lanes))
        x = x + step * p
        ahead = jnp.where(place < size - 1, pltpu.roll(p, size - 1, 0), 0.0)
        r = r - step * (p + 0.5 * (ahead + pltpu.roll(jnp.where(place == 0, 2.0 * p, p), 1, 0)))
        if k + 1 < n:
            new = plus_product(rho, pair_scale(alpha, -1.0), tau)
            beta = pair_scale(pair_div(at(new, k + 1), pivot, inverse), -1.0 if k == 0 else -0.5)
            p = r + jnp.broadcast_to(beta[0], (size, lanes)) * p
            pi = plus_product(new, beta, pi)
            rho = new
    return x * (1.0 / half), r


def solve_kernel(
    sizes, right_in, diag_in, feats_in, bank, target_in, index_in, w1_in, w2_in, w3_in, press, resid, total_grads,
    right, diag, feats, target, index, w1, w2, w3, in_sem,
    mp, nb, basis, pre, inv, yp, yr, zp, zr, eta, ar_src, ar_dst,
    bank_v, counts, grads, swapped, halved, first, held, second, owned, third, full,
    small, small_in, small_third,
    bank_sem, g_send, g_recv, h_send, h_recv, a_send, a_recv,
):
    given = ((feats_in, feats), (w1_in, w1), (w2_in, w2), (w3_in, w3), (diag_in, diag), (right_in, right),
             (index_in, index), (target_in, target))
    given = [pltpu.make_async_copy(src, dst, in_sem.at[n]) for n, (src, dst) in enumerate(given)]
    for copy in given:
        copy.start()

    lx, ly, lz = right.shape
    ch, columns = bank.shape
    stress = target.shape[0]
    tiles = columns // TILE
    pos = {a: lax.axis_index(a) for a in AXES}
    phases = phases_of(sizes)

    def tile_copy(t):
        return pltpu.make_async_copy(
            bank.at[:, pl.ds(t * TILE, TILE)], bank_v.at[t], bank_sem.at[t]
        )

    for t in range(tiles):
        tile_copy(t).start()

    def coords(axes, offs, sign):
        out = {}
        for a, k in zip(axes, offs):
            n = sizes[a]
            c = pos[a] + (k if sign > 0 else n - k) if k else pos[a]
            out[a] = lax.rem(c, n) if k else c
        return out

    def flat(axes, at):
        value = 0
        for a in axes:
            value = value * sizes[a] + at[a]
        return value

    groups = []
    for axes in phases:
        me = flat(axes, pos)
        peers = []
        for offs in shift_offsets([sizes[a] for a in axes]):
            to = {**pos, **coords(axes, offs, 1)}
            source = flat(axes, coords(axes, offs, -1))
            far = sum(min(k, sizes[a] - k) for a, k in zip(axes, offs))
            peers.append((far, to, source))
        peers = [(to, source) for far, to, source in sorted(peers, key=lambda peer: -peer[0])]
        groups.append((me, peers))

    nx, nz, na = sizes["gx"], sizes["gz"], sizes["ga"]
    pair = 2 if nz % 2 == 0 else 1
    nh = nz // pair
    side, spot = lax.rem(pos["gz"], pair), lax.div(pos["gz"], pair)
    half_rows = grads.shape[0] // pair
    share = half_rows // nh
    piece = share // na

    def half_of(b):
        return pl.ds(pl.multiple_of(b * half_rows, 8), half_rows)

    def share_of(h):
        return pl.ds(pl.multiple_of(h * share, 8), share)

    def block_of(h, ia=None):
        start = side * half_rows + h * share
        if ia is None:
            return pl.ds(pl.multiple_of(start, 8), share)
        return pl.ds(pl.multiple_of(start + ia * piece, 8), piece)

    def along(axis, k, sign):
        return coords((axis,), (k,), sign)[axis]

    def spot_along(k, sign):
        return lax.rem(spot + (k if sign > 0 else nh - k), nh)

    numbers = {}

    def gradient_copy(kind, k, src, dst, to):
        number = numbers.setdefault((kind, k), len(numbers))
        return pltpu.make_async_remote_copy(
            src_ref=src,
            dst_ref=dst,
            send_sem=g_send.at[number],
            recv_sem=g_recv.at[number],
            device_id={**pos, **to},
            device_id_type=MESH,
        )

    def to_pair():
        return {"gz": spot * pair + (pair - 1 - side)}

    def to_spot(k):
        return {"gz": spot_along(k, 1) * pair + side}

    def swap_pair():
        other = half_of(pair - 1 - side)
        return [
            gradient_copy("swap", 0, grads.at[other], swapped, to_pair()),
            gradient_copy("swap", 1, small.at[0], small_in.at[0], to_pair()),
        ]

    def scatter_gz(k):
        return [
            gradient_copy("gz", k, halved.at[share_of(spot_along(k, 1))], first.at[k - 1], to_spot(k)),
            gradient_copy("small gz", k, small.at[1], small_in.at[k], to_spot(k)),
        ]

    def scatter_ga(k):
        rows = pl.ds(pl.multiple_of(along("ga", k, 1) * piece, 8), piece)
        to = {"ga": along("ga", k, 1)}
        return [
            gradient_copy("ga", k, held.at[rows], second.at[k - 1], to),
            gradient_copy("small ga", k, small.at[2], small_in.at[nh + k - 1], to),
        ]

    def add_gx(k, sign=1):
        slot = pos["gx"] if sign > 0 else along("gx", k, -1)
        to = {"gx": along("gx", k, 1)}
        return [
            gradient_copy("gx", k, owned, third.at[slot], to),
            gradient_copy("small gx", k, small.at[3], small_third.at[slot], to),
        ]

    def gather_ga(k, sign=1):
        at = pos["ga"] if sign > 0 else along("ga", k, -1)
        rows = block_of(spot, at)
        return [gradient_copy("all ga", k, full.at[rows], full.at[rows], {"ga": along("ga", k, 1)})]

    def gather_gz(k, sign=1):
        rows = block_of(spot if sign > 0 else spot_along(k, -1))
        return [gradient_copy("all gz", k, full.at[rows], full.at[rows], to_spot(k))]

    def gather_pair(sign=1):
        rows = half_of(side if sign > 0 else pair - 1 - side)
        return [gradient_copy("all pair", 0, full.at[rows], full.at[rows], to_pair())]

    def start(copies):
        for copy in copies:
            copy.start()

    def arrived(copies):
        for copy in copies:
            copy.wait_recv()

    def sent(copies):
        for copy in copies:
            copy.wait_send()

    def gradient_stage(stage):
        if stage == 0:
            if pair > 1:
                start(swap_pair())
        elif stage == 1:
            total, few = grads[half_of(side), :], small[0]
            if pair > 1:
                arrived(swap_pair())
                total, few = total + swapped[...], few + small_in[0]
            halved[...] = total
            small[1] = few
            for k in range(1, nh):
                start(scatter_gz(k))
        elif stage == 2:
            total, few = halved[share_of(spot), :], small[1]
            for k in range(1, nh):
                arrived(scatter_gz(k))
                total, few = total + first[k - 1], few + small_in[k]
            held[...] = total
            small[2] = few
            for k in range(1, na, 2):
                start(scatter_ga(k))
        elif stage == 3:
            for k in range(2, na, 2):
                start(scatter_ga(k))
        elif stage == 4:
            total, few = held[pl.ds(pl.multiple_of(pos["ga"] * piece, 8), piece), :], small[2]
            for k in range(1, na):
                arrived(scatter_ga(k))
                total, few = total + second[k - 1], few + small_in[nh + k - 1]
            owned[...] = total
            third[pos["gx"]] = total
            small[3] = few
            small_third[pos["gx"]] = few
            for k in range(1, nx):
                start(add_gx(k))
        elif stage == 5:
            for k in range(1, nx):
                arrived(add_gx(k, -1))
            full[block_of(spot, pos["ga"]), :] = jnp.sum(third[...], axis=0)
            for k in range(1, na, 2):
                start(gather_ga(k))
        elif stage == 6:
            for k in range(2, na, 2):
                start(gather_ga(k))
        elif stage == 7:
            for k in range(1, na):
                arrived(gather_ga(k, -1))
            for k in range(1, nh):
                start(gather_gz(k))
        elif stage == 8:
            for k in range(1, nh):
                arrived(gather_gz(k, -1))
            if pair > 1:
                start(gather_pair())
        else:
            if pair > 1:
                arrived(gather_pair(-1))
                sent(swap_pair() + gather_pair())
            for k in range(1, nh):
                sent(scatter_gz(k) + gather_gz(k))
            for k in range(1, na):
                sent(scatter_ga(k) + gather_ga(k))
            for k in range(1, nx):
                sent(add_gx(k))

    def count_samples():
        samples = index.shape[1]
        ids = index[...]
        high = lax.broadcasted_iota(jnp.int32, (columns // 128, samples), 0) == (ids // 128)
        low = lax.broadcasted_iota(jnp.int32, (128, samples), 0) == (ids % 128)
        counts[...] = dot(
            jnp.where(high, 1.0, 0.0).astype(BF16),
            jnp.where(low, 1.0, 0.0).astype(BF16),
            ((1,), (1,)),
        )

    def gradient_tile(t):
        rows = TILE // 128
        tile_copy(t).wait()
        weight = jnp.concatenate([counts[pl.ds(t * rows + j, 1), :] for j in range(rows)], axis=1)
        x = bank_v[t]
        a1, a2, a3 = w1[...], w2[...], w3[...]
        l1 = dot(a1, x)
        s1 = sigmoid(l1)
        h1 = (l1 * s1).astype(BF16)
        l2 = dot(a2, h1)
        s2 = sigmoid(l2)
        h2 = (l2 * s2).astype(BF16)
        goal = target[:, pl.ds(pl.multiple_of(t * TILE, TILE), TILE)]
        error = (dot(a3, h2) - goal.astype(F32)).astype(BF16)

        def weighted(delta, right):
            scaled = delta.astype(F32) * weight
            upper = scaled.astype(BF16)
            lower = (scaled - upper.astype(F32)).astype(BF16)
            return dot(upper, right, ((1,), (1,))) + dot(lower, right, ((1,), (1,)))

        small[0, :stress] += weighted(error, h2)
        d2 = (dot(a3, error, ((0,), (0,))) * (s2 * (1.0 + l2 * (1.0 - s2)))).astype(BF16)
        grads[ch : 2 * ch] += weighted(d2, h1)
        d1 = (dot(a2, d2, ((0,), (0,))) * (s1 * (1.0 + l1 * (1.0 - s1)))).astype(BF16)
        grads[:ch] += weighted(d1, x)

    def gradient_exchange(i):
        for stage, step in STAGE_STEPS:
            pl.when(i == tiles - 1 + step)(lambda stage=stage: gradient_stage(stage))

    def gradient_work(i):
        @pl.when(i < tiles)
        def _():
            gradient_tile(i)

            @pl.when(i == tiles - 1)
            def _():
                gradient_stage(0)

    mp[...] = jnp.zeros_like(mp)
    yr[...] = jnp.zeros_like(yr)
    zr[...] = jnp.zeros_like(zr)

    barrier = pltpu.get_barrier_semaphore()
    total = 0
    for _, peers in groups:
        for to, _ in peers:
            pl.semaphore_signal(barrier, inc=1, device_id=to, device_id_type=MESH)
            total += 1

    lane = lax.broadcasted_iota(jnp.int32, (ly, lz), 1)
    sub8 = lax.broadcasted_iota(jnp.int32, (8, lz), 0)

    def halo_copies(par):
        out = {}

        def add(axis, step, number, src, dst):
            copy = pltpu.make_async_remote_copy(
                src_ref=src,
                dst_ref=dst,
                send_sem=h_send.at[par, number],
                recv_sem=h_recv.at[par, number],
                device_id={**pos, axis: jnp.clip(pos[axis] + step, 0, sizes[axis] - 1)},
                device_id_type=MESH,
            )
            can_send = pos[axis] < sizes[axis] - 1 if step > 0 else pos[axis] > 0
            will_get = pos[axis] > 0 if step > 0 else pos[axis] < sizes[axis] - 1
            out.setdefault(axis, []).append((copy, can_send, will_get))

        rows = pl.ds(8, ly)
        if sizes["gx"] > 1:
            add("gx", 1, 0, mp.at[par, pl.ds(lx, 4), rows], mp.at[par, pl.ds(0, 4), rows])
            add("gx", -1, 1, mp.at[par, pl.ds(4, 4), rows], mp.at[par, pl.ds(lx + 4, 4), rows])
        if sizes["ga"] > 1:
            add("ga", 1, 2, yp.at[par, 0], yr.at[par, 0])
            add("ga", -1, 3, yp.at[par, 1], yr.at[par, 1])
        if sizes["gz"] > 1:
            add("gz", 1, 4, zp.at[par], zr.at[par, 0])
            add("gz", -1, 5, zp.at[par], zr.at[par, 1])
        return out

    def halo_start(par, *axes):
        copies = halo_copies(par)
        for axis in axes:
            for copy, can_send, _ in copies.get(axis, []):
                pl.when(can_send)(copy.start)

    def halo_wait(par, *axes):
        copies = halo_copies(par)
        for axis in axes:
            for copy, _, will_get in copies.get(axis, []):
                pl.when(will_get)(copy.wait_recv)

    def halo_sent(par):
        for copies in halo_copies(par).values():
            for copy, can_send, _ in copies:
                pl.when(can_send)(copy.wait_send)

    bases = []
    base = 0
    for axes in phases:
        bases.append(base)
        n = 1
        for a in axes:
            n *= sizes[a]
        base += n

    def sum_copies(phase):
        me, peers = groups[phase]
        out = []
        for k, (to, source) in enumerate(peers):
            slot = bases[phase]
            send = pltpu.make_async_remote_copy(
                src_ref=ar_src.at[phase],
                dst_ref=ar_dst.at[slot + me],
                send_sem=a_send.at[slot + k],
                recv_sem=a_recv.at[slot + me],
                device_id=to,
                device_id_type=MESH,
            )
            receive = pltpu.make_async_remote_copy(
                src_ref=ar_src.at[phase],
                dst_ref=ar_dst.at[slot + source],
                send_sem=a_send.at[slot + k],
                recv_sem=a_recv.at[slot + source],
                device_id=to,
                device_id_type=MESH,
            )
            out.append((send, receive))
        return out

    def sum_start(phase, row):
        ar_src[phase] = row
        ar_dst[bases[phase] + groups[phase][0]] = row
        for send, _ in sum_copies(phase):
            send.start()

    def sum_wait(phase):
        count = len(groups[phase][1]) + 1
        for _, receive in sum_copies(phase):
            receive.wait_recv()
        parts = [ar_dst[bases[phase] + j] for j in range(count)]
        parts = [(v, jnp.zeros_like(v)) for v in parts]
        while len(parts) > 1:
            joined = [pair_add(a, b) for a, b in zip(parts[::2], parts[1::2])]
            parts = joined + parts[2 * len(joined) :]
        return pair_add(parts[0], tuple(pltpu.roll(v, lz // 2, 1) for v in parts[0]))

    def packed_pair(v):
        first_half = lax.broadcasted_iota(jnp.int32, (1, lz), 1) < lz // 2
        return jnp.where(first_half, v[0], pltpu.roll(v[1], lz // 2, 1))

    def sums_sent():
        for phase in range(len(phases)):
            for send, _ in sum_copies(phase):
                send.wait_send()

    def stencil_local(par, keep, start, back, older):
        even = jnp.zeros((ly, lz), F32)
        for x in range(lx):
            v = mp[par, 4 + x, pl.ds(8, ly)]
            acc = None
            for k in range(1, 5):
                t = mp[par, 4 + x, pl.ds(8 + k, ly)] + mp[par, 4 + x, pl.ds(8 - k, ly)]
                if x + k < lx:
                    t = t + mp[par, 4 + x + k, pl.ds(8, ly)]
                if x - k >= 0:
                    t = t + mp[par, 4 + x - k, pl.ds(8, ly)]
                t = t + jnp.where(lane >= k, pltpu.roll(v, k, 1), 0.0)
                t = t + jnp.where(lane < lz - k, pltpu.roll(v, lz - k, 1), 0.0)
                t = taps[k - 1] * t
                acc = t if acc is None else acc + t
            nb[x] = keep * v - start * (inv[x] * acc) - back * basis[older, x]
            even = even + pre[x] * v * v
        return even

    def z_correction(par):
        h = jnp.where(lane % 8 < 4, zr[par, 0], zr[par, 1])
        acc = jnp.zeros((ly, lz), F32)
        place = lane % 8
        for k in range(1, 5):
            ahead = jnp.where((place >= 4) & (place - 4 < k), pltpu.roll(h, k, 1), 0.0)
            behind = jnp.where((place < 4) & (place >= 4 - k), pltpu.roll(h, lz - k, 1), 0.0)
            acc = acc + taps[k - 1] * (ahead + behind)
        return acc

    def side_part(par, x, zc):
        z = pltpu.roll(zc, (2 * lz - 8 * x - 4) % lz, 1)
        acc = jnp.where((lane < 4) | (lane >= lz - 4), z, 0.0)
        if x % 2 == 0:
            h = jnp.where(sub8 < 4, yr[par, 1, x // 2], yr[par, 0, x // 2])
        else:
            h = pltpu.roll(jnp.where(sub8 < 4, yr[par, 0, x // 2], yr[par, 1, x // 2]), 4, 0)
        low = jnp.zeros((8, lz), F32)
        high = jnp.zeros((8, lz), F32)
        for k in range(1, 5):
            low = low + taps[k - 1] * jnp.where(sub8 < k, pltpu.roll(h, k, 0), 0.0)
            high = high + taps[k - 1] * jnp.where(sub8 >= 8 - k, pltpu.roll(h, 8 - k, 0), 0.0)
        parts = [acc[:8] + low] + ([acc[8:-8]] if ly > 16 else []) + [acc[-8:] + high]
        return jnp.concatenate(parts, axis=0)

    def end_part(par, x):
        acc = None
        for k in range(1, 5):
            for at in (4 + x - k, 4 + x + k):
                if at < 4 or at >= lx + 4:
                    t = taps[k - 1] * mp[par, at, pl.ds(8, ly)]
                    acc = t if acc is None else acc + t
        return acc

    def publish(par, x, m, packed, edges):
        mp[par, 4 + x, pl.ds(8, ly)] = m
        if x % 2 == 0:
            edges = (m[:8], m[-8:])
        else:
            yp[par, 0, x // 2] = jnp.where(sub8 < 4, pltpu.roll(m[-8:], 4, 0), edges[1])
            yp[par, 1, x // 2] = jnp.where(sub8 < 4, edges[0], pltpu.roll(m[:8], 4, 0))
        turned = pltpu.roll(m, (8 * x + 4) % lz, 1)
        return jnp.where((lane >= 8 * x) & (lane < 8 * x + 8), turned, packed), edges

    ends = list(range(4)) + list(range(lx - 4, lx))
    inner = list(range(4, lx - 4))

    for copy in given[:4]:
        copy.wait()
    hidden = dot(w1[...], feats[...])
    hidden = (hidden * sigmoid(hidden)).astype(BF16)
    hidden = dot(w2[...], hidden)
    hidden = (hidden * sigmoid(hidden)).astype(BF16)
    predicted = dot(w3[...], hidden)
    trace = (predicted[0:1] + predicted[1:2] + predicted[2:3]) / 3.0
    ex, ey, ez = lx // EL, ly // EL, lz // EL
    spread = jnp.where(
        lax.broadcasted_iota(jnp.int32, (lz, lz), 0) == lax.broadcasted_iota(jnp.int32, (lz, lz), 1) // EL,
        1.0,
        0.0,
    )
    lines = jnp.concatenate(
        [trace if e == 0 else pltpu.roll(trace, (lz - e * ez) % lz, 1) for e in range(ex * ey)], axis=0
    )
    forcing = dot(lines, spread, precision=lax.Precision.HIGHEST)
    for copy in given[4:6]:
        copy.wait()
    pl.semaphore_wait(barrier, total)
    packed = jnp.zeros((ly, lz), F32)
    edges = None
    for n, x in enumerate(ends + inner):
        line = forcing[(x // EL) * ey : (x // EL) * ey + ey]
        block = jnp.concatenate([jnp.broadcast_to(line[j : j + 1], (EL, lz)) for j in range(ey)], axis=0)
        whole = diag[x] + center
        scale = 1.0 / whole
        pre[x] = whole
        inv[x] = scale * (2.0 / half)
        first_vector = (right[x] + block) * scale
        basis[0, x] = first_vector
        packed, edges = publish(0, x, first_vector, packed, edges)
        if n == 7:
            halo_start(0, "gx")
    zp[0] = packed
    halo_start(0, "ga", "gz")
    grads[...] = jnp.zeros_like(grads)
    small[...] = jnp.zeros_like(small)
    for copy in given[6:]:
        copy.wait()
    count_samples()

    def iteration(i, carry):
        par = lax.rem(i, 2)
        later = 1 - par
        start = jnp.where(i == 0, 0.5, 1.0)
        back = jnp.where(i == 0, 0.0, 1.0)
        keep = start * (2.0 / half - 2.0)
        gradient_exchange(i)
        even = stencil_local(par, keep, start, back, jnp.maximum(i - 1, 0))
        eta[2 * i] = jnp.sum(even.reshape(ly // 8, 8, lz), axis=0)
        gradient_work(i)
        halo_wait(par, "ga", "gz")
        zc = z_correction(par)
        more = i < ITERS - 1
        packed = jnp.zeros((ly, lz), F32)
        odd = jnp.zeros((ly, lz), F32)
        edges = None
        for x in ends:
            nb[x] = nb[x] - start * (inv[x] * side_part(par, x, zc))
        for x in inner:
            m = nb[x] - start * (inv[x] * side_part(par, x, zc))
            basis[i + 1, x] = m
            odd = odd + pre[x] * mp[par, 4 + x, pl.ds(8, ly)] * m
            packed, edges = publish(later, x, m, packed, edges)
        halo_wait(par, "gx")
        for x in ends:
            m = nb[x] - start * (inv[x] * end_part(par, x))
            basis[i + 1, x] = m
            odd = odd + pre[x] * mp[par, 4 + x, pl.ds(8, ly)] * m
            packed, edges = publish(later, x, m, packed, edges)
        pl.when(more)(lambda: halo_start(later, "gx"))
        zp[later] = packed
        pl.when(more)(lambda: halo_start(later, "ga", "gz"))
        eta[2 * i + 1] = jnp.sum(odd.reshape(ly // 8, 8, lz), axis=0)
        halo_sent(par)
        return carry

    lax.fori_loop(0, ITERS, iteration, 0)

    count = 2 * ITERS
    lanes = jnp.sum(eta[...], axis=1)
    coarse = jnp.max(jnp.abs(lanes), axis=1, keepdims=True) * (2.0 * lz)
    upper = (lanes + coarse) - coarse
    mine = lax.broadcasted_iota(jnp.int32, (count, lz), 0) == lax.broadcasted_iota(jnp.int32, (count, lz), 1)
    row = packed_pair(
        [
            jnp.sum(jnp.where(mine, jnp.sum(v, axis=1, keepdims=True), 0.0), axis=0, keepdims=True)
            for v in (upper, lanes - upper)
        ]
    )
    sum_start(0, row)
    for phase in range(1, len(phases)):
        sum_start(phase, packed_pair(sum_wait(phase - 1)))
    sums = sum_wait(len(phases) - 1)
    gradient_stage(8)
    sums = tuple(
        jnp.broadcast_to(jnp.sum(jnp.where(mine, v, 0.0), axis=1, keepdims=True), (count, lz)) for v in sums
    )
    in_x, in_r = krylov_coefficients(sums)
    along_x = [jnp.broadcast_to(in_x[j : j + 1], (ly, lz)) for j in range(ITERS)]
    along_r = [jnp.broadcast_to(in_r[j : j + 1], (ly, lz)) for j in range(ITERS + 1)]
    for x in range(lx):
        p = along_x[0] * basis[0, x]
        r = along_r[0] * basis[0, x]
        for j in range(1, ITERS):
            v = basis[j, x]
            p = p + along_x[j] * v
            r = r + along_r[j] * v
        press[x] = p
        resid[x] = pre[x] * (r + along_r[ITERS] * basis[ITERS, x])
    gradient_stage(9)
    total_grads[: 2 * ch] = full[...]
    total_grads[2 * ch :] = jnp.sum(small_third[...], axis=0)
    sums_sent()


def pressure_solve(right_side, diagonal, feats, bank, target, index, w1, w2, w3):
    sizes = {a: lax.axis_size(a) for a in AXES}
    lx, ly, lz = right_side.shape
    ch, columns = bank.shape
    slots = 0
    phases = phases_of(sizes)
    for axes in phases:
        n = 1
        for a in axes:
            n *= sizes[a]
        slots += n
    nx, nz, na = (sizes[a] for a in ("gx", "gz", "ga"))
    rows = w1.shape[0] + w2.shape[0]
    few = (w3.shape[0] + 7) // 8 * 8
    pair = 2 if nz % 2 == 0 else 1
    nh = nz // pair
    share = rows // nz
    piece = share // na
    tiles = columns // TILE
    copies = 3 + 3 * (nh - 1) + 3 * (na - 1) + 2 * (nx - 1)
    inputs = (right_side, diagonal, feats, bank, target, index.reshape(1, -1), w1, w2, w3)
    field = pltpu.VMEM((lx, ly, lz), F32)
    vmem = pl.BlockSpec(memory_space=pltpu.VMEM)
    return pl.pallas_call(
        functools.partial(solve_kernel, sizes),
        out_shape=[pltpu.VMEM((lx, ly, lz), F32)] * 2 + [pltpu.VMEM((rows + few, ch), F32)],
        in_specs=[pl.BlockSpec(memory_space=pl.ANY)] * 9,
        out_specs=[vmem] * 3,
        scratch_shapes=[pltpu.VMEM(v.shape, v.dtype) for v in inputs if v is not bank]
        + [
            pltpu.SemaphoreType.DMA((len(inputs) - 1,)),
            pltpu.VMEM((2, lx + 8, ly + 16, lz), F32),
            field,
            pltpu.VMEM((ITERS + 1, lx, ly, lz), F32),
            field, field,
            pltpu.VMEM((2, 2, lx // 2, 8, lz), F32),
            pltpu.VMEM((2, 2, lx // 2, 8, lz), F32),
            pltpu.VMEM((2, ly, lz), F32),
            pltpu.VMEM((2, 2, ly, lz), F32),
            pltpu.VMEM((2 * ITERS, 8, lz), F32),
            pltpu.VMEM((len(phases), 1, lz), F32),
            pltpu.VMEM((slots, 1, lz), F32),
            pltpu.VMEM((tiles, ch, TILE), BF16),
            pltpu.VMEM((columns // 128, 128), F32),
            pltpu.VMEM((rows, ch), F32),
            pltpu.VMEM((rows // pair, ch), F32),
            pltpu.VMEM((rows // pair, ch), F32),
            pltpu.VMEM((max(nh - 1, 1), share, ch), F32),
            pltpu.VMEM((share, ch), F32),
            pltpu.VMEM((max(na - 1, 1), piece, ch), F32),
            pltpu.VMEM((piece, ch), F32),
            pltpu.VMEM((nx, piece, ch), F32),
            pltpu.VMEM((rows, ch), F32),
            pltpu.VMEM((4, few, ch), F32),
            pltpu.VMEM((nh + na - 1, few, ch), F32),
            pltpu.VMEM((nx, few, ch), F32),
            pltpu.SemaphoreType.DMA((tiles,)),
            pltpu.SemaphoreType.DMA((copies,)),
            pltpu.SemaphoreType.DMA((copies,)),
            pltpu.SemaphoreType.DMA((2, 6)),
            pltpu.SemaphoreType.DMA((2, 6)),
            pltpu.SemaphoreType.DMA((slots,)),
            pltpu.SemaphoreType.DMA((slots,)),
        ],
        compiler_params=pltpu.CompilerParams(collective_id=0, has_side_effects=True),
        cost_estimate=pl.CostEstimate(
            flops=60_000_000, bytes_accessed=200_000_000, transcendentals=0
        ),
    )(*inputs)


def finish_kernel(press_in, resid_in, grads, press, resid, step1, step2, step3):
    press[...] = press_in[...]
    resid[...] = resid_in[...]
    ch = step1.shape[0]
    start = 0
    for out in (step1, step2, step3):
        count = out.shape[0]
        value = grads[start : start + count]
        squares = jnp.sum(jnp.sum(value * value, axis=0, keepdims=True), axis=1, keepdims=True)
        out[...] = value * lax.rsqrt(squares / (count * ch) + epsilon)
        start += count


def finish(press, resid, grads, weights):
    vmem = pl.BlockSpec(memory_space=pltpu.VMEM)
    return pl.pallas_call(
        finish_kernel,
        out_shape=[jax.ShapeDtypeStruct(press.shape, F32)] * 2
        + [jax.ShapeDtypeStruct(w.shape, F32) for w in weights],
        in_specs=[vmem] * 3,
        out_specs=[vmem] * 5,
        cost_estimate=pl.CostEstimate(flops=1_000_000, bytes_accessed=2_000_000, transcendentals=0),
    )(*(pltpu.with_memory_space_constraint(v, pltpu.VMEM) for v in (press, resid, grads)))


def body(
    right_side, diagonal, element_features, sample_bank, target_bank, patch_index, w_first, w_second, w_third
):
    weights = (w_first, w_second, w_third)
    solved = pressure_solve(
        right_side, diagonal, element_features, sample_bank, target_bank, patch_index, *weights
    )
    return tuple(finish(*solved, weights))


def solution(mesh):
    return jax.shard_map(
        body,
        mesh=mesh,
        in_specs=(
            P("gx", "ga", "gz"),
            P("gx", "ga", "gz"),
            P(None, ("gx", "gz", "ga")),
            P(None, ("gx", "gz", "ga")),
            P(None, ("gx", "gz", "ga")),
            P(("gx", "gz", "ga")),
            P(),
            P(),
            P(),
        ),
        out_specs=(P("gx", "ga", "gz"), P("gx", "ga", "gz"), P(), P(), P()),
        check_vma=False,
    )
```

```python
import functools

import jax
import jax.numpy as jnp
from jax import lax
from jax.experimental import pallas as pl
from jax.experimental.pallas import tpu as pltpu
from jax.sharding import PartitionSpec as P

EL = 8
ITERS = 12
TILE = 1024
AXES = ("gx", "gz", "ga")
ONE_PHASE = 64
STAGE_STEPS = ((1, 1), (2, 3), (3, 4), (4, 5), (5, 6), (6, 7), (7, 8))

taps = (1.6, -0.2, 8.0 / 315.0, -1.0 / 560.0)
center = 3.0 * 205.0 / 72.0
epsilon = 1e-06
half = 1.1
MESH = pl.DeviceIdType.MESH
F32 = jnp.float32
BF16 = jnp.bfloat16


def dot(a, b, dims=((1,), (0,)), precision=None):
    return lax.dot_general(a, b, (dims, ((), ())), preferred_element_type=F32, precision=precision)


def sigmoid(v):
    return 1.0 / (1.0 + jnp.exp(-v))


def phases_of(sizes):
    total = 1
    for a in AXES:
        total *= sizes[a]
    return (AXES,) if total <= ONE_PHASE else (("gx",), ("gz", "ga"))


def shift_offsets(sizes):
    combos = [()]
    for n in sizes:
        combos = [c + (k,) for c in combos for k in range(n)]
    return combos[1:]


def renormalized(s, e):
    r = s + e
    return r, e - (r - s)


def two_sum(a, b):
    s = a + b
    t = s - a
    return s, (a - (s - t)) + (b - t)


def pair_add(a, b):
    s, e = two_sum(a[0], b[0])
    return renormalized(s, e + (a[1] + b[1]))


def pair_scale(a, c):
    return a[0] * c, a[1] * c


def halves(v):
    t = v * 4097.0
    high = t - (t - v)
    return high, v - high


def product(a, b, parts):
    p = a * b
    (ah, al), (bh, bl) = parts, halves(b)
    return p, ((ah * bh - p) + ah * bl + al * bh) + al * bl


def pair_div(a, b, inverse):
    q = a[0] * inverse
    p, e = product(q, b[0], halves(q))
    return renormalized(q, (((a[0] - p) - e) + (a[1] - q * b[1])) * inverse)


def krylov_coefficients(eta):
    count, lanes = eta[0].shape
    low_row, rows = 0, count
    n = count // 2
    size = (n + 2 + 7) // 8 * 8
    row = lax.broadcasted_iota(jnp.int32, (count, lanes), 0)
    place = lax.broadcasted_iota(jnp.int32, (size, lanes), 0)

    def at(v, j):
        return tuple(jnp.broadcast_to(part[j - low_row : j - low_row + 1], (1, lanes)) for part in v)

    def wide(v):
        return tuple(jnp.broadcast_to(part, (rows, lanes)) for part in v)

    def plus_product(a, c, v):
        c0, c1 = wide(c)
        p, e = product(c0, v[0], wide(halves(c[0])))
        value, error = two_sum(a[0], p)
        return renormalized(value, error + (a[1] + (e + (c0 * v[1] + c1 * v[0]))))

    low = tuple(jnp.where(row % 2 == 0, e, o) for e, o in zip(wide(at(eta, 0)), wide(at(eta, 1))))
    moments = pair_add(pair_scale(eta, 2.0), pair_scale(low, -1.0))
    rho = tuple(jnp.where(row < 2, e, m) for e, m in zip(eta, moments))
    pi = rho
    r = jnp.where(place == 0, 1.0, 0.0)
    p, x = r, jnp.zeros_like(r)
    for k in range(n):
        keep = max(k - 1, 0) // 8 * 8
        end = min((2 * n - 1 - k) // 8 * 8 + 8, low_row + rows)
        if (keep, end - keep) != (low_row, rows):
            rho, pi = (tuple(part[keep - low_row : end - low_row] for part in v) for v in (rho, pi))
            low_row, rows = keep, end - keep
        above = tuple(pltpu.roll(v, rows - 1, 0) for v in pi)
        below = tuple(pltpu.roll(v, 1, 0) for v in pi)
        if k < 2:
            below = tuple(jnp.where(row == 0, u, v) for u, v in zip(above, below))
        near, rest = two_sum(above[0], below[0])
        value, error = two_sum(pi[0], 0.5 * near)
        tau = value, error + (pi[1] + 0.5 * (rest + (above[1] + below[1])))
        pivot = at(tau, k)
        inverse = 1.0 / pivot[0]
        alpha = pair_div(at(rho, k), pivot, inverse)
        step = jnp.broadcast_to(alpha[0], (size, lanes))
        x = x + step * p
        ahead = jnp.where(place < size - 1, pltpu.roll(p, size - 1, 0), 0.0)
        r = r - step * (p + 0.5 * (ahead + pltpu.roll(jnp.where(place == 0, 2.0 * p, p), 1, 0)))
        if k + 1 < n:
            new = plus_product(rho, pair_scale(alpha, -1.0), tau)
            beta = pair_scale(pair_div(at(new, k + 1), pivot, inverse), -1.0 if k == 0 else -0.5)
            p = r + jnp.broadcast_to(beta[0], (size, lanes)) * p
            pi = plus_product(new, beta, pi)
            rho = new
    return x * (1.0 / half), r


def solve_kernel(
    sizes, right_in, diag_in, feats_in, bank, target_in, index_in, w1_in, w2_in, w3_in, press, resid, step1, step2, step3,
    right, diag, feats, target, index, w1, w2, w3, in_sem,
    mp, nb, basis, pre, inv, yp, yr, zp, zr, eta, ar_src, ar_dst,
    bank_v, counts, grads, swapped, halved, first, held, second, owned, third, full,
    small, small_in, small_third,
    bank_sem, g_send, g_recv, h_send, h_recv, a_send, a_recv,
):
    given = ((feats_in, feats), (w1_in, w1), (w2_in, w2), (w3_in, w3), (diag_in, diag), (right_in, right),
             (index_in, index), (target_in, target))
    given = [pltpu.make_async_copy(src, dst, in_sem.at[n]) for n, (src, dst) in enumerate(given)]
    for copy in given:
        copy.start()

    lx, ly, lz = right.shape
    ch, columns = bank.shape
    stress = target.shape[0]
    tiles = columns // TILE
    pos = {a: lax.axis_index(a) for a in AXES}
    phases = phases_of(sizes)

    def tile_copy(t):
        return pltpu.make_async_copy(
            bank.at[:, pl.ds(t * TILE, TILE)], bank_v.at[t], bank_sem.at[t]
        )

    for t in range(tiles):
        tile_copy(t).start()

    def coords(axes, offs, sign):
        out = {}
        for a, k in zip(axes, offs):
            n = sizes[a]
            c = pos[a] + (k if sign > 0 else n - k) if k else pos[a]
            out[a] = lax.rem(c, n) if k else c
        return out

    def flat(axes, at):
        value = 0
        for a in axes:
            value = value * sizes[a] + at[a]
        return value

    groups = []
    for axes in phases:
        me = flat(axes, pos)
        peers = []
        for offs in shift_offsets([sizes[a] for a in axes]):
            to = {**pos, **coords(axes, offs, 1)}
            source = flat(axes, coords(axes, offs, -1))
            far = sum(min(k, sizes[a] - k) for a, k in zip(axes, offs))
            peers.append((far, to, source))
        peers = [(to, source) for far, to, source in sorted(peers, key=lambda peer: -peer[0])]
        groups.append((me, peers))

    nx, nz, na = sizes["gx"], sizes["gz"], sizes["ga"]
    pair = 2 if nz % 2 == 0 else 1
    nh = nz // pair
    side, spot = lax.rem(pos["gz"], pair), lax.div(pos["gz"], pair)
    half_rows = grads.shape[0] // pair
    share = half_rows // nh
    piece = share // na

    def half_of(b):
        return pl.ds(pl.multiple_of(b * half_rows, 8), half_rows)

    def share_of(h):
        return pl.ds(pl.multiple_of(h * share, 8), share)

    def block_of(h, ia=None):
        start = side * half_rows + h * share
        if ia is None:
            return pl.ds(pl.multiple_of(start, 8), share)
        return pl.ds(pl.multiple_of(start + ia * piece, 8), piece)

    def along(axis, k, sign):
        return coords((axis,), (k,), sign)[axis]

    def spot_along(k, sign):
        return lax.rem(spot + (k if sign > 0 else nh - k), nh)

    numbers = {}

    def gradient_copy(kind, k, src, dst, to):
        number = numbers.setdefault((kind, k), len(numbers))
        return pltpu.make_async_remote_copy(
            src_ref=src,
            dst_ref=dst,
            send_sem=g_send.at[number],
            recv_sem=g_recv.at[number],
            device_id={**pos, **to},
            device_id_type=MESH,
        )

    def to_pair():
        return {"gz": spot * pair + (pair - 1 - side)}

    def to_spot(k):
        return {"gz": spot_along(k, 1) * pair + side}

    def swap_pair():
        other = half_of(pair - 1 - side)
        return [
            gradient_copy("swap", 0, grads.at[other], swapped, to_pair()),
            gradient_copy("swap", 1, small.at[0], small_in.at[0], to_pair()),
        ]

    def scatter_gz(k):
        return [
            gradient_copy("gz", k, halved.at[share_of(spot_along(k, 1))], first.at[k - 1], to_spot(k)),
            gradient_copy("small gz", k, small.at[1], small_in.at[k], to_spot(k)),
        ]

    def scatter_ga(k):
        rows = pl.ds(pl.multiple_of(along("ga", k, 1) * piece, 8), piece)
        to = {"ga": along("ga", k, 1)}
        return [
            gradient_copy("ga", k, held.at[rows], second.at[k - 1], to),
            gradient_copy("small ga", k, small.at[2], small_in.at[nh + k - 1], to),
        ]

    def add_gx(k, sign=1):
        slot = pos["gx"] if sign > 0 else along("gx", k, -1)
        to = {"gx": along("gx", k, 1)}
        return [
            gradient_copy("gx", k, owned, third.at[slot], to),
            gradient_copy("small gx", k, small.at[3], small_third.at[slot], to),
        ]

    def gather_ga(k, sign=1):
        at = pos["ga"] if sign > 0 else along("ga", k, -1)
        rows = block_of(spot, at)
        return [gradient_copy("all ga", k, full.at[rows], full.at[rows], {"ga": along("ga", k, 1)})]

    def gather_gz(k, sign=1):
        rows = block_of(spot if sign > 0 else spot_along(k, -1))
        return [gradient_copy("all gz", k, full.at[rows], full.at[rows], to_spot(k))]

    def gather_pair(sign=1):
        rows = half_of(side if sign > 0 else pair - 1 - side)
        return [gradient_copy("all pair", 0, full.at[rows], full.at[rows], to_pair())]

    def start(copies):
        for copy in copies:
            copy.start()

    def arrived(copies):
        for copy in copies:
            copy.wait_recv()

    def sent(copies):
        for copy in copies:
            copy.wait_send()

    def gradient_stage(stage):
        if stage == 0:
            if pair > 1:
                start(swap_pair())
        elif stage == 1:
            total, few = grads[half_of(side), :], small[0]
            if pair > 1:
                arrived(swap_pair())
                total, few = total + swapped[...], few + small_in[0]
            halved[...] = total
            small[1] = few
            for k in range(1, nh):
                start(scatter_gz(k))
        elif stage == 2:
            total, few = halved[share_of(spot), :], small[1]
            for k in range(1, nh):
                arrived(scatter_gz(k))
                total, few = total + first[k - 1], few + small_in[k]
            held[...] = total
            small[2] = few
            for k in range(1, na, 2):
                start(scatter_ga(k))
        elif stage == 3:
            for k in range(2, na, 2):
                start(scatter_ga(k))
        elif stage == 4:
            total, few = held[pl.ds(pl.multiple_of(pos["ga"] * piece, 8), piece), :], small[2]
            for k in range(1, na):
                arrived(scatter_ga(k))
                total, few = total + second[k - 1], few + small_in[nh + k - 1]
            owned[...] = total
            third[pos["gx"]] = total
            small[3] = few
            small_third[pos["gx"]] = few
            for k in range(1, nx):
                start(add_gx(k))
        elif stage == 5:
            for k in range(1, nx):
                arrived(add_gx(k, -1))
            full[block_of(spot, pos["ga"]), :] = jnp.sum(third[...], axis=0)
            for k in range(1, na, 2):
                start(gather_ga(k))
        elif stage == 6:
            for k in range(2, na, 2):
                start(gather_ga(k))
        elif stage == 7:
            for k in range(1, na):
                arrived(gather_ga(k, -1))
            for k in range(1, nh):
                start(gather_gz(k))
        elif stage == 8:
            for k in range(1, nh):
                arrived(gather_gz(k, -1))
            if pair > 1:
                start(gather_pair())
        else:
            if pair > 1:
                arrived(gather_pair(-1))
                sent(swap_pair() + gather_pair())
            for k in range(1, nh):
                sent(scatter_gz(k) + gather_gz(k))
            for k in range(1, na):
                sent(scatter_ga(k) + gather_ga(k))
            for k in range(1, nx):
                sent(add_gx(k))

    def count_samples():
        samples = index.shape[1]
        ids = index[...]
        high = lax.broadcasted_iota(jnp.int32, (columns // 128, samples), 0) == (ids // 128)
        low = lax.broadcasted_iota(jnp.int32, (128, samples), 0) == (ids % 128)
        counts[...] = dot(
            jnp.where(high, 1.0, 0.0).astype(BF16),
            jnp.where(low, 1.0, 0.0).astype(BF16),
            ((1,), (1,)),
        )

    def gradient_tile(t):
        rows = TILE // 128
        tile_copy(t).wait()
        weight = jnp.concatenate([counts[pl.ds(t * rows + j, 1), :] for j in range(rows)], axis=1)
        x = bank_v[t]
        a1, a2, a3 = w1[...], w2[...], w3[...]
        l1 = dot(a1, x)
        s1 = sigmoid(l1)
        h1 = (l1 * s1).astype(BF16)
        l2 = dot(a2, h1)
        s2 = sigmoid(l2)
        h2 = (l2 * s2).astype(BF16)
        goal = target[:, pl.ds(pl.multiple_of(t * TILE, TILE), TILE)]
        error = (dot(a3, h2) - goal.astype(F32)).astype(BF16)

        def weighted(delta, right):
            scaled = delta.astype(F32) * weight
            upper = scaled.astype(BF16)
            lower = (scaled - upper.astype(F32)).astype(BF16)
            return dot(upper, right, ((1,), (1,))) + dot(lower, right, ((1,), (1,)))

        small[0, :stress] += weighted(error, h2)
        d2 = (dot(a3, error, ((0,), (0,))) * (s2 * (1.0 + l2 * (1.0 - s2)))).astype(BF16)
        grads[ch : 2 * ch] += weighted(d2, h1)
        d1 = (dot(a2, d2, ((0,), (0,))) * (s1 * (1.0 + l1 * (1.0 - s1)))).astype(BF16)
        grads[:ch] += weighted(d1, x)

    def gradient_exchange(i):
        for stage, step in STAGE_STEPS:
            pl.when(i == tiles - 1 + step)(lambda stage=stage: gradient_stage(stage))

    def gradient_work(i):
        @pl.when(i < tiles)
        def _():
            gradient_tile(i)

            @pl.when(i == tiles - 1)
            def _():
                gradient_stage(0)

    mp[...] = jnp.zeros_like(mp)
    yr[...] = jnp.zeros_like(yr)
    zr[...] = jnp.zeros_like(zr)

    barrier = pltpu.get_barrier_semaphore()
    total = 0
    for _, peers in groups:
        for to, _ in peers:
            pl.semaphore_signal(barrier, inc=1, device_id=to, device_id_type=MESH)
            total += 1

    lane = lax.broadcasted_iota(jnp.int32, (ly, lz), 1)
    sub8 = lax.broadcasted_iota(jnp.int32, (8, lz), 0)

    def halo_copies(par):
        out = {}

        def add(axis, step, number, src, dst):
            copy = pltpu.make_async_remote_copy(
                src_ref=src,
                dst_ref=dst,
                send_sem=h_send.at[par, number],
                recv_sem=h_recv.at[par, number],
                device_id={**pos, axis: jnp.clip(pos[axis] + step, 0, sizes[axis] - 1)},
                device_id_type=MESH,
            )
            can_send = pos[axis] < sizes[axis] - 1 if step > 0 else pos[axis] > 0
            will_get = pos[axis] > 0 if step > 0 else pos[axis] < sizes[axis] - 1
            out.setdefault(axis, []).append((copy, can_send, will_get))

        rows = pl.ds(8, ly)
        if sizes["gx"] > 1:
            add("gx", 1, 0, mp.at[par, pl.ds(lx, 4), rows], mp.at[par, pl.ds(0, 4), rows])
            add("gx", -1, 1, mp.at[par, pl.ds(4, 4), rows], mp.at[par, pl.ds(lx + 4, 4), rows])
        if sizes["ga"] > 1:
            add("ga", 1, 2, yp.at[par, 0], yr.at[par, 0])
            add("ga", -1, 3, yp.at[par, 1], yr.at[par, 1])
        if sizes["gz"] > 1:
            add("gz", 1, 4, zp.at[par], zr.at[par, 0])
            add("gz", -1, 5, zp.at[par], zr.at[par, 1])
        return out

    def halo_start(par, *axes):
        copies = halo_copies(par)
        for axis in axes:
            for copy, can_send, _ in copies.get(axis, []):
                pl.when(can_send)(copy.start)

    def halo_wait(par, *axes):
        copies = halo_copies(par)
        for axis in axes:
            for copy, _, will_get in copies.get(axis, []):
                pl.when(will_get)(copy.wait_recv)

    def halo_sent(par):
        for copies in halo_copies(par).values():
            for copy, can_send, _ in copies:
                pl.when(can_send)(copy.wait_send)

    bases = []
    base = 0
    for axes in phases:
        bases.append(base)
        n = 1
        for a in axes:
            n *= sizes[a]
        base += n

    def sum_copies(phase):
        me, peers = groups[phase]
        out = []
        for k, (to, source) in enumerate(peers):
            slot = bases[phase]
            send = pltpu.make_async_remote_copy(
                src_ref=ar_src.at[phase],
                dst_ref=ar_dst.at[slot + me],
                send_sem=a_send.at[slot + k],
                recv_sem=a_recv.at[slot + me],
                device_id=to,
                device_id_type=MESH,
            )
            receive = pltpu.make_async_remote_copy(
                src_ref=ar_src.at[phase],
                dst_ref=ar_dst.at[slot + source],
                send_sem=a_send.at[slot + k],
                recv_sem=a_recv.at[slot + source],
                device_id=to,
                device_id_type=MESH,
            )
            out.append((send, receive))
        return out

    def sum_start(phase, row):
        ar_src[phase] = row
        ar_dst[bases[phase] + groups[phase][0]] = row
        for send, _ in sum_copies(phase):
            send.start()

    def sum_wait(phase):
        count = len(groups[phase][1]) + 1
        for _, receive in sum_copies(phase):
            receive.wait_recv()
        parts = [ar_dst[bases[phase] + j] for j in range(count)]
        parts = [(v, jnp.zeros_like(v)) for v in parts]
        while len(parts) > 1:
            joined = [pair_add(a, b) for a, b in zip(parts[::2], parts[1::2])]
            parts = joined + parts[2 * len(joined) :]
        return pair_add(parts[0], tuple(pltpu.roll(v, lz // 2, 1) for v in parts[0]))

    def packed_pair(v):
        first_half = lax.broadcasted_iota(jnp.int32, (1, lz), 1) < lz // 2
        return jnp.where(first_half, v[0], pltpu.roll(v[1], lz // 2, 1))

    def sums_sent():
        for phase in range(len(phases)):
            for send, _ in sum_copies(phase):
                send.wait_send()

    def stencil_local(par, keep, start, back, older):
        even = jnp.zeros((ly, lz), F32)
        for x in range(lx):
            v = mp[par, 4 + x, pl.ds(8, ly)]
            acc = None
            for k in range(1, 5):
                t = mp[par, 4 + x, pl.ds(8 + k, ly)] + mp[par, 4 + x, pl.ds(8 - k, ly)]
                if x + k < lx:
                    t = t + mp[par, 4 + x + k, pl.ds(8, ly)]
                if x - k >= 0:
                    t = t + mp[par, 4 + x - k, pl.ds(8, ly)]
                t = t + jnp.where(lane >= k, pltpu.roll(v, k, 1), 0.0)
                t = t + jnp.where(lane < lz - k, pltpu.roll(v, lz - k, 1), 0.0)
                t = taps[k - 1] * t
                acc = t if acc is None else acc + t
            nb[x] = keep * v - start * (inv[x] * acc) - back * basis[older, x]
            even = even + pre[x] * v * v
        return even

    def z_correction(par, weights):
        h = jnp.where(lane % 8 < 4, zr[par, 0], zr[par, 1])
        acc = jnp.zeros((ly, lz), F32)
        place = lane % 8
        for k in range(1, 5):
            ahead = jnp.where((place >= 4) & (place - 4 < k), pltpu.roll(h, k, 1), 0.0)
            behind = jnp.where((place < 4) & (place >= 4 - k), pltpu.roll(h, lz - k, 1), 0.0)
            acc = acc + weights[k - 1] * (ahead + behind)
        return acc

    def side_part(par, x, zc, weights):
        z = pltpu.roll(zc, (2 * lz - 8 * x - 4) % lz, 1)
        acc = jnp.where((lane < 4) | (lane >= lz - 4), z, 0.0)
        if x % 2 == 0:
            h = jnp.where(sub8 < 4, yr[par, 1, x // 2], yr[par, 0, x // 2])
        else:
            h = pltpu.roll(jnp.where(sub8 < 4, yr[par, 0, x // 2], yr[par, 1, x // 2]), 4, 0)
        low = jnp.zeros((8, lz), F32)
        high = jnp.zeros((8, lz), F32)
        for k in range(1, 5):
            low = low + weights[k - 1] * jnp.where(sub8 < k, pltpu.roll(h, k, 0), 0.0)
            high = high + weights[k - 1] * jnp.where(sub8 >= 8 - k, pltpu.roll(h, 8 - k, 0), 0.0)
        parts = [acc[:8] + low] + ([acc[8:-8]] if ly > 16 else []) + [acc[-8:] + high]
        return jnp.concatenate(parts, axis=0)

    def end_part(par, x, weights):
        acc = None
        for k in range(1, 5):
            for at in (4 + x - k, 4 + x + k):
                if at < 4 or at >= lx + 4:
                    t = weights[k - 1] * mp[par, at, pl.ds(8, ly)]
                    acc = t if acc is None else acc + t
        return acc

    def publish(par, x, m, packed, edges, store=True):
        if store:
            mp[par, 4 + x, pl.ds(8, ly)] = m
        if x % 2 == 0:
            edges = (m[:8], m[-8:])
        else:
            yp[par, 0, x // 2] = jnp.where(sub8 < 4, pltpu.roll(m[-8:], 4, 0), edges[1])
            yp[par, 1, x // 2] = jnp.where(sub8 < 4, edges[0], pltpu.roll(m[:8], 4, 0))
        turned = pltpu.roll(m, (8 * x + 4) % lz, 1)
        return jnp.where((lane >= 8 * x) & (lane < 8 * x + 8), turned, packed), edges

    ends = list(range(4)) + list(range(lx - 4, lx))
    inner = list(range(4, lx - 4))

    for copy in given[:4]:
        copy.wait()
    hidden = dot(w1[...], feats[...])
    hidden = (hidden * sigmoid(hidden)).astype(BF16)
    hidden = dot(w2[...], hidden)
    hidden = (hidden * sigmoid(hidden)).astype(BF16)
    predicted = dot(w3[...], hidden)
    trace = (predicted[0:1] + predicted[1:2] + predicted[2:3]) / 3.0
    ex, ey, ez = lx // EL, ly // EL, lz // EL
    spread = jnp.where(
        lax.broadcasted_iota(jnp.int32, (lz, lz), 0) == lax.broadcasted_iota(jnp.int32, (lz, lz), 1) // EL,
        1.0,
        0.0,
    ).astype(BF16)
    lines = jnp.concatenate(
        [trace if e == 0 else pltpu.roll(trace, (lz - e * ez) % lz, 1) for e in range(ex * ey)], axis=0
    )
    parts, rest = [], lines
    for _ in range(3):
        parts.append(rest.astype(BF16))
        rest = rest - parts[-1].astype(F32)
    forcing = sum(dot(part, spread) for part in parts)
    for copy in given[4:6]:
        copy.wait()
    pl.semaphore_wait(barrier, total)
    packed = jnp.zeros((ly, lz), F32)
    edges = None
    for n, x in enumerate(ends + inner):
        line = forcing[(x // EL) * ey : (x // EL) * ey + ey]
        block = jnp.concatenate([jnp.broadcast_to(line[j : j + 1], (EL, lz)) for j in range(ey)], axis=0)
        whole = diag[x] + center
        scale = 1.0 / whole
        pre[x] = whole
        inv[x] = scale * (2.0 / half)
        first_vector = (right[x] + block) * scale
        basis[0, x] = first_vector
        packed, edges = publish(0, x, first_vector, packed, edges)
        if n == 7:
            halo_start(0, "gx")
    zp[0] = packed
    halo_start(0, "ga", "gz")
    grads[...] = jnp.zeros_like(grads)
    small[...] = jnp.zeros_like(small)
    for copy in given[6:]:
        copy.wait()
    count_samples()

    def iteration(i, carry):
        par = lax.rem(i, 2)
        later = 1 - par
        start = jnp.where(i == 0, 0.5, 1.0)
        back = jnp.where(i == 0, 0.0, 1.0)
        keep = start * (2.0 / half - 2.0)
        gradient_exchange(i)
        even = stencil_local(par, keep, start, back, jnp.maximum(i - 1, 0))
        eta[2 * i] = jnp.sum(even.reshape(ly // 8, 8, lz), axis=0)
        gradient_work(i)
        halo_wait(par, "ga", "gz")
        weights = [start * t for t in taps]
        zc = z_correction(par, weights)
        more = i < ITERS - 1
        packed = jnp.zeros((ly, lz), F32)
        odd = jnp.zeros((ly, lz), F32)
        edges = None
        for x in ends:
            nb[x] = nb[x] - inv[x] * side_part(par, x, zc, weights)
        for x in inner:
            m = nb[x] - inv[x] * side_part(par, x, zc, weights)
            basis[i + 1, x] = m
            odd = odd + pre[x] * mp[par, 4 + x, pl.ds(8, ly)] * m
            packed, edges = publish(later, x, m, packed, edges)
        halo_wait(par, "gx")
        for x in ends:
            mp[later, 4 + x, pl.ds(8, ly)] = nb[x] - inv[x] * end_part(par, x, weights)
        pl.when(more)(lambda: halo_start(later, "gx"))
        for x in ends:
            m = mp[later, 4 + x, pl.ds(8, ly)]
            basis[i + 1, x] = m
            odd = odd + pre[x] * mp[par, 4 + x, pl.ds(8, ly)] * m
            packed, edges = publish(later, x, m, packed, edges, False)
        zp[later] = packed
        pl.when(more)(lambda: halo_start(later, "ga", "gz"))
        eta[2 * i + 1] = jnp.sum(odd.reshape(ly // 8, 8, lz), axis=0)
        halo_sent(par)
        return carry

    lax.fori_loop(0, ITERS, iteration, 0)

    count = 2 * ITERS
    lanes = jnp.sum(eta[...], axis=1)
    coarse = jnp.max(jnp.abs(lanes), axis=1, keepdims=True) * (2.0 * lz)
    upper = (lanes + coarse) - coarse
    mine = lax.broadcasted_iota(jnp.int32, (count, lz), 0) == lax.broadcasted_iota(jnp.int32, (count, lz), 1)
    row = packed_pair(
        [
            jnp.sum(jnp.where(mine, jnp.sum(v, axis=1, keepdims=True), 0.0), axis=0, keepdims=True)
            for v in (upper, lanes - upper)
        ]
    )
    sum_start(0, row)
    gradient_stage(8)
    gradient_stage(9)
    last = jnp.sum(small_third[...], axis=0)[:stress]
    for out, value in ((step1, full[:ch]), (step2, full[ch:]), (step3, last)):
        squares = jnp.sum(jnp.sum(value * value, axis=0, keepdims=True), axis=1, keepdims=True)
        out[...] = value * lax.rsqrt(squares / (out.shape[0] * ch) + epsilon)
    for phase in range(1, len(phases)):
        sum_start(phase, packed_pair(sum_wait(phase - 1)))
    sums = sum_wait(len(phases) - 1)
    sums = tuple(
        jnp.broadcast_to(jnp.sum(jnp.where(mine, v, 0.0), axis=1, keepdims=True), (count, lz)) for v in sums
    )
    in_x, in_r = krylov_coefficients(sums)
    along_x = [jnp.broadcast_to(in_x[j : j + 1], (ly, lz)) for j in range(ITERS)]
    along_r = [jnp.broadcast_to(in_r[j : j + 1], (ly, lz)) for j in range(ITERS + 1)]
    for x in range(lx):
        p = along_x[0] * basis[0, x]
        r = along_r[0] * basis[0, x]
        for j in range(1, ITERS):
            v = basis[j, x]
            p = p + along_x[j] * v
            r = r + along_r[j] * v
        press[x] = p
        resid[x] = pre[x] * (r + along_r[ITERS] * basis[ITERS, x])
    sums_sent()


def pressure_solve(right_side, diagonal, feats, bank, target, index, w1, w2, w3):
    sizes = {a: lax.axis_size(a) for a in AXES}
    lx, ly, lz = right_side.shape
    ch, columns = bank.shape
    slots = 0
    phases = phases_of(sizes)
    for axes in phases:
        n = 1
        for a in axes:
            n *= sizes[a]
        slots += n
    nx, nz, na = (sizes[a] for a in ("gx", "gz", "ga"))
    rows = w1.shape[0] + w2.shape[0]
    few = (w3.shape[0] + 7) // 8 * 8
    pair = 2 if nz % 2 == 0 else 1
    nh = nz // pair
    share = rows // nz
    piece = share // na
    tiles = columns // TILE
    copies = 3 + 3 * (nh - 1) + 3 * (na - 1) + 2 * (nx - 1)
    inputs = (right_side, diagonal, feats, bank, target, index.reshape(1, -1), w1, w2, w3)
    field = pltpu.VMEM((lx, ly, lz), F32)
    vmem = pl.BlockSpec(memory_space=pltpu.VMEM)
    return pl.pallas_call(
        functools.partial(solve_kernel, sizes),
        out_shape=[pltpu.VMEM((lx, ly, lz), F32)] * 2 + [pltpu.VMEM(w.shape, F32) for w in (w1, w2, w3)],
        in_specs=[pl.BlockSpec(memory_space=pl.ANY)] * 9,
        out_specs=[vmem] * 5,
        scratch_shapes=[pltpu.VMEM(v.shape, v.dtype) for v in inputs if v is not bank]
        + [
            pltpu.SemaphoreType.DMA((len(inputs) - 1,)),
            pltpu.VMEM((2, lx + 8, ly + 16, lz), F32),
            field,
            pltpu.VMEM((ITERS + 1, lx, ly, lz), F32),
            field, field,
            pltpu.VMEM((2, 2, lx // 2, 8, lz), F32),
            pltpu.VMEM((2, 2, lx // 2, 8, lz), F32),
            pltpu.VMEM((2, ly, lz), F32),
            pltpu.VMEM((2, 2, ly, lz), F32),
            pltpu.VMEM((2 * ITERS, 8, lz), F32),
            pltpu.VMEM((len(phases), 1, lz), F32),
            pltpu.VMEM((slots, 1, lz), F32),
            pltpu.VMEM((tiles, ch, TILE), BF16),
            pltpu.VMEM((columns // 128, 128), F32),
            pltpu.VMEM((rows, ch), F32),
            pltpu.VMEM((rows // pair, ch), F32),
            pltpu.VMEM((rows // pair, ch), F32),
            pltpu.VMEM((max(nh - 1, 1), share, ch), F32),
            pltpu.VMEM((share, ch), F32),
            pltpu.VMEM((max(na - 1, 1), piece, ch), F32),
            pltpu.VMEM((piece, ch), F32),
            pltpu.VMEM((nx, piece, ch), F32),
            pltpu.VMEM((rows, ch), F32),
            pltpu.VMEM((4, few, ch), F32),
            pltpu.VMEM((nh + na - 1, few, ch), F32),
            pltpu.VMEM((nx, few, ch), F32),
            pltpu.SemaphoreType.DMA((tiles,)),
            pltpu.SemaphoreType.DMA((copies,)),
            pltpu.SemaphoreType.DMA((copies,)),
            pltpu.SemaphoreType.DMA((2, 6)),
            pltpu.SemaphoreType.DMA((2, 6)),
            pltpu.SemaphoreType.DMA((slots,)),
            pltpu.SemaphoreType.DMA((slots,)),
        ],
        compiler_params=pltpu.CompilerParams(collective_id=0, has_side_effects=True),
        cost_estimate=pl.CostEstimate(
            flops=60_000_000, bytes_accessed=200_000_000, transcendentals=0
        ),
    )(*inputs)


def finish_kernel(*refs):
    half_way = len(refs) // 2
    for src, dst in zip(refs[:half_way], refs[half_way:]):
        dst[...] = src[...]


def finish(values):
    vmem = pl.BlockSpec(memory_space=pltpu.VMEM)
    return pl.pallas_call(
        finish_kernel,
        out_shape=[jax.ShapeDtypeStruct(v.shape, v.dtype) for v in values],
        in_specs=[vmem] * len(values),
        out_specs=[vmem] * len(values),
        cost_estimate=pl.CostEstimate(flops=1_000_000, bytes_accessed=2_000_000, transcendentals=0),
    )(*(pltpu.with_memory_space_constraint(v, pltpu.VMEM) for v in values))


def body(
    right_side, diagonal, element_features, sample_bank, target_bank, patch_index, w_first, w_second, w_third
):
    weights = (w_first, w_second, w_third)
    solved = pressure_solve(
        right_side, diagonal, element_features, sample_bank, target_bank, patch_index, *weights
    )
    return tuple(finish(solved))


def solution(mesh):
    return jax.shard_map(
        body,
        mesh=mesh,
        in_specs=(
            P("gx", "ga", "gz"),
            P("gx", "ga", "gz"),
            P(None, ("gx", "gz", "ga")),
            P(None, ("gx", "gz", "ga")),
            P(None, ("gx", "gz", "ga")),
            P(("gx", "gz", "ga")),
            P(),
            P(),
            P(),
        ),
        out_specs=(P("gx", "ga", "gz"), P("gx", "ga", "gz"), P(), P(), P()),
        check_vma=False,
    )
```

```python
import functools

import jax
import jax.numpy as jnp
from jax import lax
from jax.experimental import pallas as pl
from jax.experimental.pallas import tpu as pltpu
from jax.sharding import PartitionSpec as P

EL = 8
ITERS = 12
TILE = 1024
AXES = ("gx", "gz", "ga")
ONE_PHASE = 64
PLAIN = 3
STAGE_STEPS = ((1, 1), (2, 3), (3, 4), (4, 5), (5, 6), (6, 7), (7, 8))

taps = (1.6, -0.2, 8.0 / 315.0, -1.0 / 560.0)
center = 3.0 * 205.0 / 72.0
epsilon = 1e-06
half = 1.1
MESH = pl.DeviceIdType.MESH
F32 = jnp.float32
BF16 = jnp.bfloat16


def dot(a, b, dims=((1,), (0,)), precision=None):
    return lax.dot_general(a, b, (dims, ((), ())), preferred_element_type=F32, precision=precision)


def sigmoid(v):
    return 1.0 / (1.0 + jnp.exp(-v))


def phases_of(sizes):
    total = 1
    for a in AXES:
        total *= sizes[a]
    return (AXES,) if total <= ONE_PHASE else (("gx",), ("gz", "ga"))


def shift_offsets(sizes):
    combos = [()]
    for n in sizes:
        combos = [c + (k,) for c in combos for k in range(n)]
    return combos[1:]


def renormalized(s, e):
    r = s + e
    return r, e - (r - s)


def two_sum(a, b):
    s = a + b
    t = s - a
    return s, (a - (s - t)) + (b - t)


def pair_add(a, b):
    s, e = two_sum(a[0], b[0])
    return renormalized(s, e + (a[1] + b[1]))


def pair_scale(a, c):
    return a[0] * c, a[1] * c


def halves(v):
    t = v * 4097.0
    high = t - (t - v)
    return high, v - high


def product(a, b, parts):
    p = a * b
    (ah, al), (bh, bl) = parts, halves(b)
    return p, ((ah * bh - p) + ah * bl + al * bh) + al * bl


def pair_div(a, b, inverse):
    q = a[0] * inverse
    p, e = product(q, b[0], halves(q))
    return renormalized(q, (((a[0] - p) - e) + (a[1] - q * b[1])) * inverse)


def pair_sum(a, b, c):
    near, rest = two_sum(b[0], c[0])
    value, error = two_sum(a[0], 0.5 * near)
    return value, error + (a[1] + 0.5 * (rest + (b[1] + c[1])))


def krylov_coefficients(eta):
    count, lanes = eta[0].shape
    low_row, rows = 0, count
    n = count // 2
    size = (n + 2 + 7) // 8 * 8
    row = lax.broadcasted_iota(jnp.int32, (count, lanes), 0)
    place = lax.broadcasted_iota(jnp.int32, (size, lanes), 0)

    def at(v, j):
        return tuple(jnp.broadcast_to(part[j - low_row : j - low_row + 1], (1, lanes)) for part in v)

    def wide(v):
        return tuple(jnp.broadcast_to(part, (rows, lanes)) for part in v)

    def plus_product(a, c, v):
        c0, c1 = wide(c)
        p, e = product(c0, v[0], wide(halves(c[0])))
        value, error = two_sum(a[0], p)
        return renormalized(value, error + (a[1] + (e + (c0 * v[1] + c1 * v[0]))))

    low = tuple(jnp.where(row % 2 == 0, e, o) for e, o in zip(wide(at(eta, 0)), wide(at(eta, 1))))
    moments = pair_add(pair_scale(eta, 2.0), pair_scale(low, -1.0))
    rho = tuple(jnp.where(row < 2, e, m) for e, m in zip(eta, moments))
    pi = rho
    r = jnp.where(place == 0, 1.0, 0.0)
    p, x = r, jnp.zeros_like(r)
    for k in range(n):
        keep = max(k - 1, 0) // 8 * 8
        end = min((2 * n - 1 - k) // 8 * 8 + 8, low_row + rows)
        if (keep, end - keep) != (low_row, rows):
            rho, pi = (tuple(part[keep - low_row : end - low_row] for part in v) for v in (rho, pi))
            low_row, rows = keep, end - keep
        above = tuple(pltpu.roll(v, rows - 1, 0) for v in pi)
        below = tuple(pltpu.roll(v, 1, 0) for v in pi)
        if k < 2:
            below = tuple(jnp.where(row == 0, u, v) for u, v in zip(above, below))
        if k >= n - PLAIN:
            tau = (pi[0] + 0.5 * (above[0] + below[0]), None)
        else:
            tau = pair_sum(pi, above, below)
        plain = tau[1] is None
        if plain:
            tau, rho, pi = tau[:1], rho[:1], pi[:1]
        pivot = at(tau, k)
        inverse = 1.0 / pivot[0]
        alpha = (at(rho, k)[0] * inverse,) if plain else pair_div(at(rho, k), pivot, inverse)
        step = jnp.broadcast_to(alpha[0], (size, lanes))
        x = x + step * p
        ahead = jnp.where(place < size - 1, pltpu.roll(p, size - 1, 0), 0.0)
        r = r - step * (p + 0.5 * (ahead + pltpu.roll(jnp.where(place == 0, 2.0 * p, p), 1, 0)))
        if k + 1 < n:
            if plain:
                new = (rho[0] - wide(alpha)[0] * tau[0],)
                beta = (at(new, k + 1)[0] * inverse * -0.5,)
            else:
                new = plus_product(rho, pair_scale(alpha, -1.0), tau)
                beta = pair_scale(pair_div(at(new, k + 1), pivot, inverse), -1.0 if k == 0 else -0.5)
            p = r + jnp.broadcast_to(beta[0], (size, lanes)) * p
            pi = (new[0] + wide(beta)[0] * pi[0],) if plain else plus_product(new, beta, pi)
            rho = new
    return x * (1.0 / half), r


def solve_kernel(
    sizes, right_in, diag_in, feats_in, bank, target_in, index_in, w1_in, w2_in, w3_in, press, resid, step1, step2, step3,
    right, diag, feats, target, index, w1, w2, w3, in_sem,
    mp, nb, basis, pre, inv, yp, yr, zp, zr, eta, ar_src, ar_dst,
    bank_v, counts, grads, swapped, halved, first, held, second, owned, third, full,
    small, small_in, small_third,
    bank_sem, g_send, g_recv, h_send, h_recv, a_send, a_recv,
):
    given = ((feats_in, feats), (w1_in, w1), (w2_in, w2), (w3_in, w3), (diag_in, diag), (right_in, right),
             (index_in, index), (target_in, target))
    given = [pltpu.make_async_copy(src, dst, in_sem.at[n]) for n, (src, dst) in enumerate(given)]
    for copy in given:
        copy.start()

    lx, ly, lz = right.shape
    ch, columns = bank.shape
    stress = target.shape[0]
    tiles = columns // TILE
    pos = {a: lax.axis_index(a) for a in AXES}
    phases = phases_of(sizes)

    def tile_copy(t):
        return pltpu.make_async_copy(
            bank.at[:, pl.ds(t * TILE, TILE)], bank_v.at[t], bank_sem.at[t]
        )

    for t in range(tiles):
        tile_copy(t).start()

    def coords(axes, offs, sign):
        out = {}
        for a, k in zip(axes, offs):
            n = sizes[a]
            c = pos[a] + (k if sign > 0 else n - k) if k else pos[a]
            out[a] = lax.rem(c, n) if k else c
        return out

    def flat(axes, at):
        value = 0
        for a in axes:
            value = value * sizes[a] + at[a]
        return value

    groups = []
    for axes in phases:
        me = flat(axes, pos)
        peers = []
        for offs in shift_offsets([sizes[a] for a in axes]):
            to = {**pos, **coords(axes, offs, 1)}
            source = flat(axes, coords(axes, offs, -1))
            far = sum(min(k, sizes[a] - k) for a, k in zip(axes, offs))
            peers.append((far, to, source))
        peers = [(to, source) for far, to, source in sorted(peers, key=lambda peer: -peer[0])]
        groups.append((me, peers))

    nx, nz, na = sizes["gx"], sizes["gz"], sizes["ga"]
    pair = 2 if nz % 2 == 0 else 1
    nh = nz // pair
    side, spot = lax.rem(pos["gz"], pair), lax.div(pos["gz"], pair)
    half_rows = grads.shape[0] // pair
    share = half_rows // nh
    piece = share // na

    def half_of(b):
        return pl.ds(pl.multiple_of(b * half_rows, 8), half_rows)

    def share_of(h):
        return pl.ds(pl.multiple_of(h * share, 8), share)

    def block_of(h, ia=None):
        start = side * half_rows + h * share
        if ia is None:
            return pl.ds(pl.multiple_of(start, 8), share)
        return pl.ds(pl.multiple_of(start + ia * piece, 8), piece)

    def along(axis, k, sign):
        return coords((axis,), (k,), sign)[axis]

    def spot_along(k, sign):
        return lax.rem(spot + (k if sign > 0 else nh - k), nh)

    numbers = {}

    def gradient_copy(kind, k, src, dst, to):
        number = numbers.setdefault((kind, k), len(numbers))
        return pltpu.make_async_remote_copy(
            src_ref=src,
            dst_ref=dst,
            send_sem=g_send.at[number],
            recv_sem=g_recv.at[number],
            device_id={**pos, **to},
            device_id_type=MESH,
        )

    def to_pair():
        return {"gz": spot * pair + (pair - 1 - side)}

    def to_spot(k):
        return {"gz": spot_along(k, 1) * pair + side}

    def swap_pair():
        other = half_of(pair - 1 - side)
        return [
            gradient_copy("swap", 0, grads.at[other], swapped, to_pair()),
            gradient_copy("swap", 1, small.at[0], small_in.at[0], to_pair()),
        ]

    def scatter_gz(k):
        return [
            gradient_copy("gz", k, halved.at[share_of(spot_along(k, 1))], first.at[k - 1], to_spot(k)),
            gradient_copy("small gz", k, small.at[1], small_in.at[k], to_spot(k)),
        ]

    def scatter_ga(k):
        rows = pl.ds(pl.multiple_of(along("ga", k, 1) * piece, 8), piece)
        to = {"ga": along("ga", k, 1)}
        return [
            gradient_copy("ga", k, held.at[rows], second.at[k - 1], to),
            gradient_copy("small ga", k, small.at[2], small_in.at[nh + k - 1], to),
        ]

    def add_gx(k, sign=1):
        slot = pos["gx"] if sign > 0 else along("gx", k, -1)
        to = {"gx": along("gx", k, 1)}
        return [
            gradient_copy("gx", k, owned, third.at[slot], to),
            gradient_copy("small gx", k, small.at[3], small_third.at[slot], to),
        ]

    def gather_ga(k, sign=1):
        at = pos["ga"] if sign > 0 else along("ga", k, -1)
        rows = block_of(spot, at)
        return [gradient_copy("all ga", k, full.at[rows], full.at[rows], {"ga": along("ga", k, 1)})]

    def gather_gz(k, sign=1):
        rows = block_of(spot if sign > 0 else spot_along(k, -1))
        return [gradient_copy("all gz", k, full.at[rows], full.at[rows], to_spot(k))]

    def gather_pair(sign=1):
        rows = half_of(side if sign > 0 else pair - 1 - side)
        return [gradient_copy("all pair", 0, full.at[rows], full.at[rows], to_pair())]

    def start(copies):
        for copy in copies:
            copy.start()

    def arrived(copies):
        for copy in copies:
            copy.wait_recv()

    def sent(copies):
        for copy in copies:
            copy.wait_send()

    def gradient_stage(stage):
        if stage == 0:
            if pair > 1:
                start(swap_pair())
        elif stage == 1:
            total, few = grads[half_of(side), :], small[0]
            if pair > 1:
                arrived(swap_pair())
                total, few = total + swapped[...], few + small_in[0]
            halved[...] = total
            small[1] = few
            for k in range(1, nh):
                start(scatter_gz(k))
        elif stage == 2:
            total, few = halved[share_of(spot), :], small[1]
            for k in range(1, nh):
                arrived(scatter_gz(k))
                total, few = total + first[k - 1], few + small_in[k]
            held[...] = total
            small[2] = few
            for k in range(1, na, 2):
                start(scatter_ga(k))
        elif stage == 3:
            for k in range(2, na, 2):
                start(scatter_ga(k))
        elif stage == 4:
            total, few = held[pl.ds(pl.multiple_of(pos["ga"] * piece, 8), piece), :], small[2]
            for k in range(1, na):
                arrived(scatter_ga(k))
                total, few = total + second[k - 1], few + small_in[nh + k - 1]
            owned[...] = total
            third[pos["gx"]] = total
            small[3] = few
            small_third[pos["gx"]] = few
            for k in range(1, nx):
                start(add_gx(k))
        elif stage == 5:
            for k in range(1, nx):
                arrived(add_gx(k, -1))
            full[block_of(spot, pos["ga"]), :] = jnp.sum(third[...], axis=0)
            for k in range(1, na, 2):
                start(gather_ga(k))
        elif stage == 6:
            for k in range(2, na, 2):
                start(gather_ga(k))
        elif stage == 7:
            for k in range(1, na):
                arrived(gather_ga(k, -1))
            for k in range(1, nh):
                start(gather_gz(k))
        elif stage == 8:
            for k in range(1, nh):
                arrived(gather_gz(k, -1))
            if pair > 1:
                start(gather_pair())
        else:
            if pair > 1:
                arrived(gather_pair(-1))
                sent(swap_pair() + gather_pair())
            for k in range(1, nh):
                sent(scatter_gz(k) + gather_gz(k))
            for k in range(1, na):
                sent(scatter_ga(k) + gather_ga(k))
            for k in range(1, nx):
                sent(add_gx(k))

    def count_samples():
        samples = index.shape[1]
        ids = index[...]
        high = lax.broadcasted_iota(jnp.int32, (columns // 128, samples), 0) == (ids // 128)
        low = lax.broadcasted_iota(jnp.int32, (128, samples), 0) == (ids % 128)
        counts[...] = dot(
            jnp.where(high, 1.0, 0.0).astype(BF16),
            jnp.where(low, 1.0, 0.0).astype(BF16),
            ((1,), (1,)),
        )

    def gradient_tile(t):
        rows = TILE // 128
        tile_copy(t).wait()
        weight = jnp.concatenate([counts[pl.ds(t * rows + j, 1), :] for j in range(rows)], axis=1)
        x = bank_v[t]
        a1, a2, a3 = w1[...], w2[...], w3[...]
        l1 = dot(a1, x)
        s1 = sigmoid(l1)
        h1 = (l1 * s1).astype(BF16)
        l2 = dot(a2, h1)
        s2 = sigmoid(l2)
        h2 = (l2 * s2).astype(BF16)
        goal = target[:, pl.ds(pl.multiple_of(t * TILE, TILE), TILE)]
        error = (dot(a3, h2) - goal.astype(F32)).astype(BF16)

        def weighted(delta, right):
            scaled = delta.astype(F32) * weight
            upper = scaled.astype(BF16)
            lower = (scaled - upper.astype(F32)).astype(BF16)
            return dot(upper, right, ((1,), (1,))) + dot(lower, right, ((1,), (1,)))

        small[0, :stress] += weighted(error, h2)
        d2 = (dot(a3, error, ((0,), (0,))) * (s2 * (1.0 + l2 * (1.0 - s2)))).astype(BF16)
        grads[ch : 2 * ch] += weighted(d2, h1)
        d1 = (dot(a2, d2, ((0,), (0,))) * (s1 * (1.0 + l1 * (1.0 - s1)))).astype(BF16)
        grads[:ch] += weighted(d1, x)

    def gradient_exchange(i):
        for stage, step in STAGE_STEPS:
            pl.when(i == tiles - 1 + step)(lambda stage=stage: gradient_stage(stage))

    def gradient_work(i):
        @pl.when(i < tiles)
        def _():
            gradient_tile(i)

            @pl.when(i == tiles - 1)
            def _():
                gradient_stage(0)

    mp[...] = jnp.zeros_like(mp)
    yr[...] = jnp.zeros_like(yr)
    zr[...] = jnp.zeros_like(zr)

    barrier = pltpu.get_barrier_semaphore()
    total = 0
    for _, peers in groups:
        for to, _ in peers:
            pl.semaphore_signal(barrier, inc=1, device_id=to, device_id_type=MESH)
            total += 1

    lane = lax.broadcasted_iota(jnp.int32, (ly, lz), 1)
    sub8 = lax.broadcasted_iota(jnp.int32, (8, lz), 0)

    def halo_copies(par):
        out = {}

        def add(axis, step, number, src, dst):
            copy = pltpu.make_async_remote_copy(
                src_ref=src,
                dst_ref=dst,
                send_sem=h_send.at[par, number],
                recv_sem=h_recv.at[par, number],
                device_id={**pos, axis: jnp.clip(pos[axis] + step, 0, sizes[axis] - 1)},
                device_id_type=MESH,
            )
            can_send = pos[axis] < sizes[axis] - 1 if step > 0 else pos[axis] > 0
            will_get = pos[axis] > 0 if step > 0 else pos[axis] < sizes[axis] - 1
            out.setdefault(axis, []).append((copy, can_send, will_get))

        rows = pl.ds(8, ly)
        if sizes["gx"] > 1:
            add("gx", 1, 0, mp.at[par, pl.ds(lx, 4), rows], mp.at[par, pl.ds(0, 4), rows])
            add("gx", -1, 1, mp.at[par, pl.ds(4, 4), rows], mp.at[par, pl.ds(lx + 4, 4), rows])
        if sizes["ga"] > 1:
            add("ga", 1, 2, yp.at[par, 0], yr.at[par, 0])
            add("ga", -1, 3, yp.at[par, 1], yr.at[par, 1])
        if sizes["gz"] > 1:
            add("gz", 1, 4, zp.at[par], zr.at[par, 0])
            add("gz", -1, 5, zp.at[par], zr.at[par, 1])
        return out

    def halo_start(par, *axes):
        copies = halo_copies(par)
        for axis in axes:
            for copy, can_send, _ in copies.get(axis, []):
                pl.when(can_send)(copy.start)

    def halo_wait(par, *axes):
        copies = halo_copies(par)
        for axis in axes:
            for copy, _, will_get in copies.get(axis, []):
                pl.when(will_get)(copy.wait_recv)

    def halo_sent(par):
        for copies in halo_copies(par).values():
            for copy, can_send, _ in copies:
                pl.when(can_send)(copy.wait_send)

    bases = []
    base = 0
    for axes in phases:
        bases.append(base)
        n = 1
        for a in axes:
            n *= sizes[a]
        base += n

    def sum_copies(phase):
        me, peers = groups[phase]
        out = []
        for k, (to, source) in enumerate(peers):
            slot = bases[phase]
            send = pltpu.make_async_remote_copy(
                src_ref=ar_src.at[phase],
                dst_ref=ar_dst.at[slot + me],
                send_sem=a_send.at[slot + k],
                recv_sem=a_recv.at[slot + me],
                device_id=to,
                device_id_type=MESH,
            )
            receive = pltpu.make_async_remote_copy(
                src_ref=ar_src.at[phase],
                dst_ref=ar_dst.at[slot + source],
                send_sem=a_send.at[slot + k],
                recv_sem=a_recv.at[slot + source],
                device_id=to,
                device_id_type=MESH,
            )
            out.append((send, receive))
        return out

    def sum_start(phase, row):
        ar_src[phase] = row
        ar_dst[bases[phase] + groups[phase][0]] = row
        for send, _ in sum_copies(phase):
            send.start()

    def sum_wait(phase):
        count = len(groups[phase][1]) + 1
        for _, receive in sum_copies(phase):
            receive.wait_recv()
        parts = [ar_dst[bases[phase] + j] for j in range(count)]
        parts = [(v, jnp.zeros_like(v)) for v in parts]
        while len(parts) > 1:
            joined = [pair_add(a, b) for a, b in zip(parts[::2], parts[1::2])]
            parts = joined + parts[2 * len(joined) :]
        return pair_add(parts[0], tuple(pltpu.roll(v, lz // 2, 1) for v in parts[0]))

    def packed_pair(v):
        first_half = lax.broadcasted_iota(jnp.int32, (1, lz), 1) < lz // 2
        return jnp.where(first_half, v[0], pltpu.roll(v[1], lz // 2, 1))

    def sums_sent():
        for phase in range(len(phases)):
            for send, _ in sum_copies(phase):
                send.wait_send()

    def stencil_local(par, keep, start, back, older):
        even = jnp.zeros((ly, lz), F32)
        for x in range(lx):
            v = mp[par, 4 + x, pl.ds(8, ly)]
            acc = None
            for k in range(1, 5):
                t = mp[par, 4 + x, pl.ds(8 + k, ly)] + mp[par, 4 + x, pl.ds(8 - k, ly)]
                if x + k < lx:
                    t = t + mp[par, 4 + x + k, pl.ds(8, ly)]
                if x - k >= 0:
                    t = t + mp[par, 4 + x - k, pl.ds(8, ly)]
                t = t + jnp.where(lane >= k, pltpu.roll(v, k, 1), 0.0)
                t = t + jnp.where(lane < lz - k, pltpu.roll(v, lz - k, 1), 0.0)
                t = taps[k - 1] * t
                acc = t if acc is None else acc + t
            nb[x] = keep * v - start * (inv[x] * acc) - back * basis[older, x]
            even = even + pre[x] * v * v
        return even

    def z_correction(par, weights):
        h = jnp.where(lane % 8 < 4, zr[par, 0], zr[par, 1])
        acc = jnp.zeros((ly, lz), F32)
        place = lane % 8
        for k in range(1, 5):
            ahead = jnp.where((place >= 4) & (place - 4 < k), pltpu.roll(h, k, 1), 0.0)
            behind = jnp.where((place < 4) & (place >= 4 - k), pltpu.roll(h, lz - k, 1), 0.0)
            acc = acc + weights[k - 1] * (ahead + behind)
        return acc

    def side_part(par, x, zc, weights):
        z = pltpu.roll(zc, (2 * lz - 8 * x - 4) % lz, 1)
        acc = jnp.where((lane < 4) | (lane >= lz - 4), z, 0.0)
        if x % 2 == 0:
            h = jnp.where(sub8 < 4, yr[par, 1, x // 2], yr[par, 0, x // 2])
        else:
            h = pltpu.roll(jnp.where(sub8 < 4, yr[par, 0, x // 2], yr[par, 1, x // 2]), 4, 0)
        low = jnp.zeros((8, lz), F32)
        high = jnp.zeros((8, lz), F32)
        for k in range(1, 5):
            low = low + weights[k - 1] * jnp.where(sub8 < k, pltpu.roll(h, k, 0), 0.0)
            high = high + weights[k - 1] * jnp.where(sub8 >= 8 - k, pltpu.roll(h, 8 - k, 0), 0.0)
        parts = [acc[:8] + low] + ([acc[8:-8]] if ly > 16 else []) + [acc[-8:] + high]
        return jnp.concatenate(parts, axis=0)

    def end_part(par, x, weights):
        acc = None
        for k in range(1, 5):
            for at in (4 + x - k, 4 + x + k):
                if at < 4 or at >= lx + 4:
                    t = weights[k - 1] * mp[par, at, pl.ds(8, ly)]
                    acc = t if acc is None else acc + t
        return acc

    def publish(par, x, m, packed, edges, store=True):
        if store:
            mp[par, 4 + x, pl.ds(8, ly)] = m
        if x % 2 == 0:
            edges = (m[:8], m[-8:])
        else:
            yp[par, 0, x // 2] = jnp.where(sub8 < 4, pltpu.roll(m[-8:], 4, 0), edges[1])
            yp[par, 1, x // 2] = jnp.where(sub8 < 4, edges[0], pltpu.roll(m[:8], 4, 0))
        turned = pltpu.roll(m, (8 * x + 4) % lz, 1)
        return jnp.where((lane >= 8 * x) & (lane < 8 * x + 8), turned, packed), edges

    ends = list(range(4)) + list(range(lx - 4, lx))
    inner = list(range(4, lx - 4))

    for copy in given[:4]:
        copy.wait()
    hidden = dot(w1[...], feats[...])
    hidden = (hidden * sigmoid(hidden)).astype(BF16)
    hidden = dot(w2[...], hidden)
    hidden = (hidden * sigmoid(hidden)).astype(BF16)
    predicted = dot(w3[...], hidden)
    trace = (predicted[0:1] + predicted[1:2] + predicted[2:3]) / 3.0
    ex, ey, ez = lx // EL, ly // EL, lz // EL
    spread = jnp.where(
        lax.broadcasted_iota(jnp.int32, (lz, lz), 0) == lax.broadcasted_iota(jnp.int32, (lz, lz), 1) // EL,
        1.0,
        0.0,
    ).astype(BF16)
    lines = jnp.concatenate(
        [trace if e == 0 else pltpu.roll(trace, (lz - e * ez) % lz, 1) for e in range(ex * ey)], axis=0
    )
    parts, rest = [], lines
    for _ in range(3):
        parts.append(rest.astype(BF16))
        rest = rest - parts[-1].astype(F32)
    forcing = sum(dot(part, spread) for part in parts)
    for copy in given[4:6]:
        copy.wait()
    pl.semaphore_wait(barrier, total)
    packed = jnp.zeros((ly, lz), F32)
    edges = None
    for n, x in enumerate(ends + inner):
        line = forcing[(x // EL) * ey : (x // EL) * ey + ey]
        block = jnp.concatenate([jnp.broadcast_to(line[j : j + 1], (EL, lz)) for j in range(ey)], axis=0)
        whole = diag[x] + center
        scale = 1.0 / whole
        pre[x] = whole
        inv[x] = scale * (2.0 / half)
        first_vector = (right[x] + block) * scale
        basis[0, x] = first_vector
        packed, edges = publish(0, x, first_vector, packed, edges)
        if n == 7:
            halo_start(0, "gx")
    zp[0] = packed
    halo_start(0, "ga", "gz")
    grads[...] = jnp.zeros_like(grads)
    small[...] = jnp.zeros_like(small)
    for copy in given[6:]:
        copy.wait()
    count_samples()

    def iteration(i, carry):
        par = lax.rem(i, 2)
        later = 1 - par
        start = jnp.where(i == 0, 0.5, 1.0)
        back = jnp.where(i == 0, 0.0, 1.0)
        keep = start * (2.0 / half - 2.0)
        gradient_exchange(i)
        even = stencil_local(par, keep, start, back, jnp.maximum(i - 1, 0))
        eta[2 * i] = jnp.sum(even.reshape(ly // 8, 8, lz), axis=0)
        gradient_work(i)
        halo_wait(par, "ga", "gz")
        weights = [start * t for t in taps]
        zc = z_correction(par, weights)
        more = i < ITERS - 1
        packed = jnp.zeros((ly, lz), F32)
        odd = jnp.zeros((ly, lz), F32)
        edges = None
        for x in ends:
            nb[x] = nb[x] - inv[x] * side_part(par, x, zc, weights)
        for x in inner:
            m = nb[x] - inv[x] * side_part(par, x, zc, weights)
            basis[i + 1, x] = m
            odd = odd + pre[x] * mp[par, 4 + x, pl.ds(8, ly)] * m
            packed, edges = publish(later, x, m, packed, edges)
        halo_wait(par, "gx")
        for x in ends:
            mp[later, 4 + x, pl.ds(8, ly)] = nb[x] - inv[x] * end_part(par, x, weights)
        pl.when(more)(lambda: halo_start(later, "gx"))
        for x in ends:
            m = mp[later, 4 + x, pl.ds(8, ly)]
            basis[i + 1, x] = m
            odd = odd + pre[x] * mp[par, 4 + x, pl.ds(8, ly)] * m
            packed, edges = publish(later, x, m, packed, edges, False)
        zp[later] = packed
        pl.when(more)(lambda: halo_start(later, "ga", "gz"))
        eta[2 * i + 1] = jnp.sum(odd.reshape(ly // 8, 8, lz), axis=0)
        halo_sent(par)
        return carry

    lax.fori_loop(0, ITERS, iteration, 0)

    count = 2 * ITERS
    lanes = jnp.sum(eta[...], axis=1)
    coarse = jnp.max(jnp.abs(lanes), axis=1, keepdims=True) * (2.0 * lz)
    upper = (lanes + coarse) - coarse
    mine = lax.broadcasted_iota(jnp.int32, (count, lz), 0) == lax.broadcasted_iota(jnp.int32, (count, lz), 1)
    row = packed_pair(
        [
            jnp.sum(jnp.where(mine, jnp.sum(v, axis=1, keepdims=True), 0.0), axis=0, keepdims=True)
            for v in (upper, lanes - upper)
        ]
    )
    sum_start(0, row)
    gradient_stage(8)
    gradient_stage(9)
    last = jnp.sum(small_third[...], axis=0)[:stress]
    for out, value in ((step1, full[:ch]), (step2, full[ch:]), (step3, last)):
        squares = jnp.sum(jnp.sum(value * value, axis=0, keepdims=True), axis=1, keepdims=True)
        out[...] = value * lax.rsqrt(squares / (out.shape[0] * ch) + epsilon)
    for phase in range(1, len(phases)):
        sum_start(phase, packed_pair(sum_wait(phase - 1)))
    sums = sum_wait(len(phases) - 1)
    sums = tuple(
        jnp.broadcast_to(jnp.sum(jnp.where(mine, v, 0.0), axis=1, keepdims=True), (count, lz)) for v in sums
    )
    in_x, in_r = krylov_coefficients(sums)
    along_x = [jnp.broadcast_to(in_x[j : j + 1], (ly, lz)) for j in range(ITERS)]
    along_r = [jnp.broadcast_to(in_r[j : j + 1], (ly, lz)) for j in range(ITERS + 1)]
    for x in range(lx):
        p = along_x[0] * basis[0, x]
        r = along_r[0] * basis[0, x]
        for j in range(1, ITERS):
            v = basis[j, x]
            p = p + along_x[j] * v
            r = r + along_r[j] * v
        press[x] = p
        resid[x] = pre[x] * (r + along_r[ITERS] * basis[ITERS, x])
    sums_sent()


def pressure_solve(right_side, diagonal, feats, bank, target, index, w1, w2, w3):
    sizes = {a: lax.axis_size(a) for a in AXES}
    lx, ly, lz = right_side.shape
    ch, columns = bank.shape
    slots = 0
    phases = phases_of(sizes)
    for axes in phases:
        n = 1
        for a in axes:
            n *= sizes[a]
        slots += n
    nx, nz, na = (sizes[a] for a in ("gx", "gz", "ga"))
    rows = w1.shape[0] + w2.shape[0]
    few = (w3.shape[0] + 7) // 8 * 8
    pair = 2 if nz % 2 == 0 else 1
    nh = nz // pair
    share = rows // nz
    piece = share // na
    tiles = columns // TILE
    copies = 3 + 3 * (nh - 1) + 3 * (na - 1) + 2 * (nx - 1)
    inputs = (right_side, diagonal, feats, bank, target, index.reshape(1, -1), w1, w2, w3)
    field = pltpu.VMEM((lx, ly, lz), F32)
    vmem = pl.BlockSpec(memory_space=pltpu.VMEM)
    return pl.pallas_call(
        functools.partial(solve_kernel, sizes),
        out_shape=[pltpu.VMEM((lx, ly, lz), F32)] * 2 + [pltpu.VMEM(w.shape, F32) for w in (w1, w2, w3)],
        in_specs=[pl.BlockSpec(memory_space=pl.ANY)] * 9,
        out_specs=[vmem] * 5,
        scratch_shapes=[pltpu.VMEM(v.shape, v.dtype) for v in inputs if v is not bank]
        + [
            pltpu.SemaphoreType.DMA((len(inputs) - 1,)),
            pltpu.VMEM((2, lx + 8, ly + 16, lz), F32),
            field,
            pltpu.VMEM((ITERS + 1, lx, ly, lz), F32),
            field, field,
            pltpu.VMEM((2, 2, lx // 2, 8, lz), F32),
            pltpu.VMEM((2, 2, lx // 2, 8, lz), F32),
            pltpu.VMEM((2, ly, lz), F32),
            pltpu.VMEM((2, 2, ly, lz), F32),
            pltpu.VMEM((2 * ITERS, 8, lz), F32),
            pltpu.VMEM((len(phases), 1, lz), F32),
            pltpu.VMEM((slots, 1, lz), F32),
            pltpu.VMEM((tiles, ch, TILE), BF16),
            pltpu.VMEM((columns // 128, 128), F32),
            pltpu.VMEM((rows, ch), F32),
            pltpu.VMEM((rows // pair, ch), F32),
            pltpu.VMEM((rows // pair, ch), F32),
            pltpu.VMEM((max(nh - 1, 1), share, ch), F32),
            pltpu.VMEM((share, ch), F32),
            pltpu.VMEM((max(na - 1, 1), piece, ch), F32),
            pltpu.VMEM((piece, ch), F32),
            pltpu.VMEM((nx, piece, ch), F32),
            pltpu.VMEM((rows, ch), F32),
            pltpu.VMEM((4, few, ch), F32),
            pltpu.VMEM((nh + na - 1, few, ch), F32),
            pltpu.VMEM((nx, few, ch), F32),
            pltpu.SemaphoreType.DMA((tiles,)),
            pltpu.SemaphoreType.DMA((copies,)),
            pltpu.SemaphoreType.DMA((copies,)),
            pltpu.SemaphoreType.DMA((2, 6)),
            pltpu.SemaphoreType.DMA((2, 6)),
            pltpu.SemaphoreType.DMA((slots,)),
            pltpu.SemaphoreType.DMA((slots,)),
        ],
        compiler_params=pltpu.CompilerParams(collective_id=0, has_side_effects=True),
        cost_estimate=pl.CostEstimate(
            flops=60_000_000, bytes_accessed=200_000_000, transcendentals=0
        ),
    )(*inputs)


def finish_kernel(*refs):
    half_way = len(refs) // 2
    for src, dst in zip(refs[:half_way], refs[half_way:]):
        dst[...] = src[...]


def finish(values):
    vmem = pl.BlockSpec(memory_space=pltpu.VMEM)
    return pl.pallas_call(
        finish_kernel,
        out_shape=[jax.ShapeDtypeStruct(v.shape, v.dtype) for v in values],
        in_specs=[vmem] * len(values),
        out_specs=[vmem] * len(values),
        cost_estimate=pl.CostEstimate(flops=1_000_000, bytes_accessed=2_000_000, transcendentals=0),
    )(*(pltpu.with_memory_space_constraint(v, pltpu.VMEM) for v in values))


def body(
    right_side, diagonal, element_features, sample_bank, target_bank, patch_index, w_first, w_second, w_third
):
    weights = (w_first, w_second, w_third)
    solved = pressure_solve(
        right_side, diagonal, element_features, sample_bank, target_bank, patch_index, *weights
    )
    return tuple(finish(solved))


def solution(mesh):
    return jax.shard_map(
        body,
        mesh=mesh,
        in_specs=(
            P("gx", "ga", "gz"),
            P("gx", "ga", "gz"),
            P(None, ("gx", "gz", "ga")),
            P(None, ("gx", "gz", "ga")),
            P(None, ("gx", "gz", "ga")),
            P(("gx", "gz", "ga")),
            P(),
            P(),
            P(),
        ),
        out_specs=(P("gx", "ga", "gz"), P("gx", "ga", "gz"), P(), P(), P()),
        check_vma=False,
    )
```
